512 devices in a mesh: rows: 128 (over x, z_lo, y), cols: 4 (over z_hi, core).
Axes of the slice: x: 4, y: 4, z: 16 (z_hi: 2, z_lo: 8; z = z_hi * 8 + z_lo), core: 2. Of those that a mesh axis runs over, the one named last changes fastest.
Arguments:
- coords: int32 [8, 262144], P(None, ('rows', 'cols')), may hold values from 0 to 4095
- probes: float32 [64, 262144], P(None, ('rows', 'cols')), may hold values from -6 to 6
- lengthscales: float32 [8], replicated, may hold values from 0.15 to 0.25
- amplitude: float32 [1], replicated, may hold values from 0.1 to 0.3
- landmarks: float32 [254, 8, 128], replicated, may hold values from 0 to 1
- coupling: float32 [128, 128], replicated, may hold values from -0.5 to 0.5
Outputs:
- products: float32 [2, 64, 262144], P(None, None, ('rows', 'cols'))
The draws below stay inside these ranges and needn't reach their ends.
All inputs are finite; a program needn't handle non-finite values.
Results may differ from the reference program's by a relative error of at most 0.0025.
Values may be sent and summed in bfloat16 or wider, within the bound.
No kernel may reach another device: no remote copies, remote signals or barrier semaphores. Data moves between devices by JAX's collectives and lax.ppermute only.
A program may use at most 64 MiB of HBM per device.

```python
import math
import jax
import jax.numpy as jnp
from jax import lax

DIMS = 8
RANK = 128
PROBES = 64
LEAF = 2048
POINTS = 262144
LEVELS = 7
N_ROWS = 128


def radius_at(depth):
    return max(32, 768 >> depth - 1)


def tree_centres(key):
    centres = jnp.full((DIMS, 1), 2048, jnp.int32)
    listing = []
    for depth in range(1, LEVELS + 1):
        radius = radius_at(depth)
        count = 1 << depth
        offsets = jax.random.randint(jax.random.fold_in(key, 1000 + depth), (DIMS, count), -radius, radius + 1, jnp.int32)
        centres = jnp.repeat(centres, 2, axis=1) + offsets
        listing.append(centres)
    return listing


def draw_coords(key, part):
    leaf_centres = tree_centres(key)[-1]
    spread = jax.random.randint(jax.random.fold_in(key, 77), (DIMS, POINTS), -1024, 1025, jnp.int32)
    placed = jnp.clip(jnp.repeat(leaf_centres, LEAF, axis=1) + spread, 0, 4095)
    chosen = jax.random.randint(jax.random.fold_in(key, 78), (2,), 0, POINTS, jnp.int32)
    placed = placed.at[0, chosen[0]].set(4095)
    placed = placed.at[1, chosen[1]].set(0)
    return placed


def draw_landmarks(key, part):
    listing = tree_centres(key)
    blocks = []
    for depth in range(1, LEVELS + 1):
        deeper = sum((radius_at(lower) * radius_at(lower) for lower in range(depth + 1, LEVELS + 1)))
        half_width = math.sqrt(deeper + 1048576.0)
        count = 1 << depth
        centres = listing[depth - 1].astype(jnp.float32)
        jitter = jax.random.uniform(jax.random.fold_in(key, 2000 + depth), (count, DIMS, RANK), jnp.float32, -1.0, 1.0)
        placed = (jnp.transpose(centres)[:, :, None] + half_width * jitter) / 4096.0
        blocks.append(jnp.clip(placed, 0.0, 1.0))
    return jnp.concatenate(blocks, axis=0)


def block_levels(key, dims, cuts, low, high):
    factor_of = 1.0
    for axis_at, blocks in cuts:
        draws = jax.random.uniform(jax.random.fold_in(jax.random.fold_in(key, 6), axis_at), (blocks,), jnp.float32, low / len(cuts), high / len(cuts))
        factor_of = factor_of * jnp.repeat(jnp.exp(draws), dims[axis_at] // blocks).reshape((-1,) + (1,) * (len(dims) - 1 - axis_at))
    return factor_of


def normal_values(stream_key, dims, scale, most, pieces=(), held_as=jnp.bfloat16):
    array = jax.random.normal(stream_key, dims, jnp.float32) * scale
    if len(pieces) > 0:
        array = block_levels(stream_key, dims, pieces, -0.22, 0.18) * array
    return jnp.clip(array, min=-most, max=most).astype(held_as)


def setup_inputs(seed: int = 0) -> dict:
    seeds = jax.random.split(jax.random.key(seed), 7)
    coords = draw_coords(jax.random.fold_in(seeds[6], 71), 0)
    probes = normal_values(seeds[1], (PROBES, POINTS), 1.0, 6.0, ((1, 512),), jnp.float32)
    lengthscales = jnp.clip(jnp.exp(jax.random.uniform(seeds[2], (DIMS,), jnp.float32, math.log(0.15), math.log(0.25))), 0.15, 0.25)
    amplitude = jnp.clip(jnp.exp(jax.random.uniform(seeds[3], (1,), jnp.float32, math.log(0.1), math.log(0.3))), 0.1, 0.3)
    landmarks = draw_landmarks(jax.random.fold_in(seeds[6], 71), 0)
    coupling = normal_values(seeds[5], (RANK, RANK), RANK ** -0.5, 0.5, (), jnp.float32)
    return {"coords": coords, "probes": probes, "lengthscales": lengthscales, "amplitude": amplitude, "landmarks": landmarks, "coupling": coupling}


def pair_squares(left_points, right_points):
    squared = jnp.zeros((left_points.shape[1], right_points.shape[1]), jnp.float32)
    for component in range(left_points.shape[0]):
        offset = left_points[component][:, None] - right_points[component][None, :]
        squared = squared + offset * offset
    return squared


def reference(coords, probes, lengthscales, amplitude, landmarks, coupling):
    highest = lax.Precision.HIGHEST
    inverse_scale = 1.0 / lengthscales
    scaled = coords.astype(jnp.float32) * (1.0 / 4096.0) * inverse_scale[:, None]
    anchors = landmarks * inverse_scale[None, :, None]
    strength = amplitude[0]
    signs = probes
    signs_half = signs.astype(jnp.bfloat16)

    leaf_points = jnp.transpose(scaled.reshape(DIMS, N_ROWS, LEAF), (1, 0, 2))
    leaf_signs = jnp.transpose(signs_half.reshape(PROBES, N_ROWS, LEAF), (1, 0, 2))

    def leaf_block(items):
        points, sign_rows = items
        squared = pair_squares(points, points)
        kernel = strength * jnp.exp(-0.5 * squared)
        kernel_half = kernel.astype(jnp.bfloat16)
        slope_half = (kernel * squared).astype(jnp.bfloat16)
        return jnp.stack([jnp.dot(sign_rows, kernel_half, preferred_element_type=jnp.float32),
                          jnp.dot(sign_rows, slope_half, preferred_element_type=jnp.float32)])

    diagonal = lax.map(leaf_block, (leaf_points, leaf_signs))
    result = jnp.transpose(diagonal, (1, 2, 0, 3)).reshape(2, PROBES, POINTS)

    cores = jnp.stack([coupling.T, coupling])
    for depth in range(1, LEVELS + 1):
        count = 2 ** depth
        members = POINTS // count
        node_points = scaled.reshape(DIMS, count, members)
        node_anchors = anchors[count - 2:2 * count - 2]
        squared = jnp.zeros((count, members, RANK), jnp.float32)
        for component in range(DIMS):
            offset = node_points[component][:, :, None] - node_anchors[:, component, None, :]
            squared = squared + offset * offset
        factor = strength * jnp.exp(-0.5 * squared)
        dfactor = factor * squared
        node_signs = signs.reshape(PROBES, count, members)
        project = jnp.einsum('pnm,nmr->npr', node_signs, factor, precision=highest)
        dproject = jnp.einsum('pnm,nmr->npr', node_signs, dfactor, precision=highest)
        sib_project = project.reshape(count // 2, 2, PROBES, RANK)[:, ::-1].reshape(count, PROBES, RANK)
        sib_dproject = dproject.reshape(count // 2, 2, PROBES, RANK)[:, ::-1].reshape(count, PROBES, RANK)
        node_cores = jnp.tile(cores, (count // 2, 1, 1))
        first = jnp.einsum('npr,nrs->nps', sib_project, node_cores, precision=highest)
        second = jnp.einsum('npr,nrs->nps', sib_dproject, node_cores, precision=highest)
        value = jnp.einsum('nps,nms->pnm', first, factor, precision=highest)
        slope = jnp.einsum('nps,nms->pnm', first, dfactor, precision=highest) + jnp.einsum('nps,nms->pnm', second, factor, precision=highest)
        result = result + jnp.stack([value.reshape(PROBES, POINTS), slope.reshape(PROBES, POINTS)])
    return result
```

```python
import functools
import math

import jax
import jax.numpy as jnp
from jax import lax
from jax.experimental import pallas as pl
from jax.experimental.pallas import tpu as pltpu
from jax.sharding import Mesh, PartitionSpec as P

LEVELS = 7
PROBES = 64
RANK = 128
HALF = RANK // 2
QUARTER = PROBES // 4
SPAN = 128
WIDTH = 512
TRANSFER = 80
LANES = 1024
BLOCK = 256
ROOT = math.sqrt(math.log2(math.e))
TWO_LN2 = 2.0 * math.log(2.0)
F32 = jnp.float32
BF16 = jnp.bfloat16
VMEM = pl.BlockSpec(memory_space=pltpu.VMEM)
SMEM = pl.BlockSpec(memory_space=pltpu.SMEM)


def cost(flops, moved):
    return pl.CostEstimate(flops=flops, bytes_accessed=moved, transcendentals=0)


def split3(value):
    first = value.astype(BF16).astype(F32)
    rest = value - first
    second = rest.astype(BF16).astype(F32)
    third = (rest - second).astype(BF16).astype(F32)
    return first, second, third


def inverse_scales(scales_ref):
    row = lax.broadcasted_iota(jnp.int32, (8, 128), 0)
    held = jnp.full((8, 128), scales_ref[0], F32)
    for k in range(1, 8):
        held = jnp.where(row == k, scales_ref[k], held)
    return (ROOT / held)[:, :1]


def norms(value):
    return -0.5 * jnp.sum(value * value, axis=0, keepdims=True)


def stacked(parts, rows):
    width = parts[0].shape[1]
    index = lax.broadcasted_iota(jnp.int32, (8, width), 0)
    held = jnp.zeros((8, width), F32)
    for k, row in enumerate(rows):
        held = jnp.where(index == k, row, held)
    zeros = jnp.zeros((SPAN - 56, width), F32)
    return jnp.concatenate(list(parts) + [held, zeros], axis=0)


def left_form(value, extra):
    one, two, three = split3(value)
    n1, n2, n3 = split3(norms(value) + extra)
    return stacked((one, one, two, one, three, two), (1.0, 1.0, 1.0, n1, n2, n3))


def right_form(value, extra):
    one, two, three = split3(value)
    n1, n2, n3 = split3(norms(value) + extra)
    return stacked((one, two, one, three, one, two), (n1, n2, n3, 1.0, 1.0, 1.0))


def points_of(message, inverse):
    high = message[PROBES : PROBES + 8, :].astype(F32)
    low = message[PROBES + 8 : PROBES + 16, :].astype(F32)
    return ((high * 64.0 + low) * (1.0 / 4096.0) - 0.5) * inverse


def kernel_pair(exponent, log_strength):
    kern = jnp.exp2(exponent)
    return kern, kern * (TWO_LN2 * log_strength - TWO_LN2 * exponent)


def halved(value):
    top = value.astype(BF16)
    return top, (value - top.astype(F32)).astype(BF16)


def log2_strength(strength_ref):
    return jnp.log(jnp.full((1, 128), strength_ref[0], F32))[:, :1] * math.log2(math.e)


def prepare_kernel(coords_ref, probes_ref, out_ref):
    coords = coords_ref[...]
    high = jnp.right_shift(coords, 6)
    low = coords - high * 64
    out_ref[0:PROBES, :] = probes_ref[...].astype(BF16)
    both = jnp.concatenate([high.astype(F32), low.astype(F32)], axis=0)
    out_ref[PROBES:TRANSFER, :] = both.astype(BF16)


def accumulate(message_ref, inverse, right, log_strength, held_k, held_s, fresh):
    message = message_ref[...]
    left = left_form(points_of(message, inverse), 0.0).T.astype(BF16)
    for block in range(WIDTH // BLOCK):
        rows = left[block * BLOCK : (block + 1) * BLOCK, :]
        signs = message[0:PROBES, block * BLOCK : (block + 1) * BLOCK]
        for at in range(0, LANES, BLOCK):
            exponent = jnp.dot(rows, right[:, at : at + BLOCK], preferred_element_type=F32)
            sums = []
            for value in kernel_pair(exponent, log_strength):
                top, rest = halved(value)
                total = jnp.dot(signs, top, preferred_element_type=F32)
                if at >= WIDTH:
                    total = total + jnp.dot(signs, rest, preferred_element_type=F32)
                sums.append(total)
            add_k, add_s = sums
            if fresh and block == 0:
                held_k[:, at : at + BLOCK] = add_k
                held_s[:, at : at + BLOCK] = add_s
            else:
                held_k[:, at : at + BLOCK] += add_k
                held_s[:, at : at + BLOCK] += add_s


def near_kernel(
    own_ref, other_ref, scales_ref, strength_ref, marks_ref,
    held_ref, right_ref, factor_ref, marks_buf, sem,
):
    row = lax.axis_index("x") * 32 + lax.axis_index("z") * 4 + lax.axis_index("y")
    core = lax.axis_index("c")
    copies = []
    for level in range(LEVELS):
        node = 2 ** (LEVELS - level) - 2 + jnp.right_shift(row, level)
        copies.append(pltpu.make_async_copy(marks_ref.at[node], marks_buf.at[level], sem.at[level]))
    for copy in copies:
        copy.start()
    inverse = inverse_scales(scales_ref)
    log_strength = log2_strength(strength_ref)
    own = points_of(own_ref[...], inverse)
    for copy in copies:
        copy.wait()
    marks = [(marks_buf[level] - 0.5) * inverse for level in range(LEVELS)]
    halves = [jnp.where(core == 0, mark[:, :HALF], mark[:, HALF:]) for mark in marks]
    halves.append(jnp.zeros((8, HALF), F32))
    columns = jnp.concatenate([own] + halves, axis=1)
    right = right_form(columns, log_strength).astype(BF16)
    right_ref[...] = right
    accumulate(own_ref, inverse, right, log_strength, held_ref.at[0], held_ref.at[1], True)
    accumulate(other_ref, inverse, right, log_strength, held_ref.at[0], held_ref.at[1], False)
    own_right = right[:, :WIDTH]
    for level in range(LEVELS):
        turned = left_form(marks[level], 0.0).T.astype(BF16)
        exponent = jnp.dot(turned, own_right, preferred_element_type=F32)
        kern, slope = kernel_pair(exponent, log_strength)
        factor_ref[0, level * RANK : (level + 1) * RANK, :] = kern.astype(BF16)
        factor_ref[1, level * RANK : (level + 1) * RANK, :] = slope.astype(BF16)


def far_kernel(
    far_ref, cross_ref, scales_ref, strength_ref, held_ref, right_ref,
    diagonal_ref, plane_ref, low_ref, sums,
):
    x = lax.axis_index("x")
    y = lax.axis_index("y")
    inverse = inverse_scales(scales_ref)
    log_strength = log2_strength(strength_ref)
    right = right_ref[...]
    sums[...] = held_ref[...]
    accumulate(far_ref, inverse, right, log_strength, sums.at[0], sums.at[1], False)
    accumulate(cross_ref, inverse, right, log_strength, sums.at[0], sums.at[1], False)
    diagonal_ref[...] = sums[:, :, :WIDTH]
    units = []
    for level in range(LEVELS):
        at = WIDTH + level * HALF
        pair = [sums[0, :, at : at + HALF], sums[1, :, at : at + HALF]]
        units.append(jnp.concatenate(pair, axis=1))
    blank = jnp.zeros((2 * QUARTER, 128), F32)
    for at in range(4):
        part = slice(at * QUARTER, (at + 1) * QUARTER)
        mine = jnp.concatenate([units[2][part], units[3][part], units[4][part]], axis=0)
        plane_ref[x * 4 + at] = mine
        for apart, level in ((1, 5), (2, 6), (3, 6)):
            plane_ref[jnp.bitwise_xor(x, apart) * 4 + at] = jnp.concatenate([units[level][part], blank], axis=0)
    low_ref[y] = jnp.zeros((PROBES, 128), F32)
    for apart, level in ((1, 0), (2, 1), (3, 1)):
        low_ref[jnp.bitwise_xor(y, apart)] = units[level]


def plane_kernel(got_ref, out_ref):
    x = lax.axis_index("x")
    z = lax.axis_index("z")

    def total(apart, rows):
        start = jnp.bitwise_xor(x, apart) * 4
        parts = [got_ref[start + at, rows] for at in range(4)]
        return (parts[0] + parts[1]) + (parts[2] + parts[3])

    low, middle, high = slice(0, 16), slice(16, 32), slice(32, 48)
    sums = [total(0, low), total(0, middle), total(0, high)]
    five = total(1, low)
    six = total(2, low) + total(3, low)
    chosen = [jnp.zeros((QUARTER, 128), F32)] + sums
    for apart in range(8):
        which = apart.bit_length()
        out_ref[jnp.bitwise_xor(z, apart)] = jnp.concatenate([chosen[which], five, six], axis=0)


def depth_kernel(got_ref, low_ref, out_ref):
    z = lax.axis_index("z")

    def piece(apart, start):
        return got_ref[jnp.bitwise_xor(z, apart), start : start + QUARTER]

    two = piece(1, 0)
    three = piece(2, 0) + piece(3, 0)
    four = (piece(4, 0) + piece(5, 0)) + (piece(6, 0) + piece(7, 0))
    found = [two, three, four]
    for start in (QUARTER, 2 * QUARTER):
        parts = [piece(apart, start) for apart in range(8)]
        while len(parts) > 1:
            parts = [a + b for a, b in zip(parts[::2], parts[1::2])]
        found.append(parts[0])
    packed = jnp.concatenate(found, axis=0)
    for at in range(4):
        for core in range(2):
            out_ref[2 * at + core, 0:PROBES] = low_ref[at]
            out_ref[2 * at + core, PROBES:] = packed


def final_kernel(got_ref, factor_ref, coupling_ref, diagonal_ref, out_ref, sibling):
    y = lax.axis_index("y")
    row = lax.axis_index("x") * 32 + lax.axis_index("z") * 4 + y
    for core in range(2):
        lanes = slice(core * 128, core * 128 + 128)
        sibling[0:PROBES, lanes] = got_ref[jnp.bitwise_xor(y, 1) * 2 + core, 0:PROBES]
        pair = got_ref[jnp.bitwise_xor(y, 2) * 2 + core, 0:PROBES]
        pair = pair + got_ref[jnp.bitwise_xor(y, 3) * 2 + core, 0:PROBES]
        sibling[PROBES : 2 * PROBES, lanes] = pair
        for level in range(2, LEVELS):
            for at in range(4):
                start = level * PROBES + at * QUARTER
                source = PROBES + (level - 2) * QUARTER
                sibling[start : start + QUARTER, lanes] = got_ref[2 * at + core, source : source + QUARTER]
    coupling = coupling_ref[...]
    blank = jnp.zeros((HALF, RANK), F32)

    def spread(core_matrix):
        rows = []
        for core in range(2):
            part = core_matrix[core * HALF : (core + 1) * HALF, :]
            rows.append(jnp.concatenate([part, blank], axis=1))
            rows.append(jnp.concatenate([blank, part], axis=1))
        whole = jnp.concatenate(rows, axis=0)
        return halved(whole)

    values, remainders = halved(sibling[...])
    results = []
    for matrix in (coupling.T, coupling):
        top, rest = spread(matrix)
        results.append(
            jnp.dot(values, top, preferred_element_type=F32)
            + jnp.dot(values, rest, preferred_element_type=F32)
            + jnp.dot(remainders, top, preferred_element_type=F32)
        )
    heads = []
    for level in range(LEVELS):
        rows = slice(level * PROBES, (level + 1) * PROBES)
        left = jnp.bitwise_and(jnp.right_shift(row, level), 1) == 0
        heads.append(jnp.where(left, results[0][rows], results[1][rows]))
    firsts = jnp.concatenate([head[:, :RANK] for head in heads], axis=1)
    seconds = jnp.concatenate([head[:, RANK:] for head in heads], axis=1)
    top, rest = halved(jnp.concatenate([firsts, seconds], axis=0))
    stack = jnp.concatenate([top, rest], axis=0)
    on_kern = jnp.dot(stack, factor_ref[0], preferred_element_type=F32)
    pair = jnp.concatenate([top[:PROBES], rest[:PROBES]], axis=0)
    on_slope = jnp.dot(pair, factor_ref[1], preferred_element_type=F32)
    on_kern = on_kern[: 2 * PROBES] + on_kern[2 * PROBES :]
    on_slope = on_slope[:PROBES] + on_slope[PROBES:]
    out_ref[0] = diagonal_ref[0] + on_kern[:PROBES]
    out_ref[1] = diagonal_ref[1] + (on_kern[PROBES:] + on_slope)


def swap(value, axis):
    return lax.ppermute(value, axis, [(0, 1), (1, 0)])


def exchange(value, axes):
    return lax.all_to_all(value, axes, 0, 0, tiled=True)


def on_device(coords, probes, lengthscales, amplitude, landmarks, coupling):
    message = pl.pallas_call(
        prepare_kernel,
        out_shape=jax.ShapeDtypeStruct((TRANSFER, WIDTH), BF16),
        in_specs=[VMEM, VMEM],
        out_specs=VMEM,
        cost_estimate=cost(10**5, 2 * 10**5),
        name="prepare",
    )(coords, probes)
    far = swap(message, "h")
    other = swap(message, "c")
    held, right, factor = pl.pallas_call(
        near_kernel,
        out_shape=(
            jax.ShapeDtypeStruct((2, PROBES, LANES), F32),
            jax.ShapeDtypeStruct((SPAN, LANES), BF16),
            jax.ShapeDtypeStruct((2, LEVELS * RANK, WIDTH), BF16),
        ),
        in_specs=[VMEM, VMEM, SMEM, SMEM, pl.BlockSpec(memory_space=pl.ANY)],
        out_specs=(VMEM, VMEM, VMEM),
        scratch_shapes=[pltpu.VMEM((LEVELS, 8, RANK), F32), pltpu.SemaphoreType.DMA((LEVELS,))],
        cost_estimate=cost(2 * 10**9, 3 * 10**6),
        name="near",
    )(message, other, lengthscales, amplitude, landmarks)
    cross = swap(far, "c")
    diagonal, plane, low = pl.pallas_call(
        far_kernel,
        out_shape=(
            jax.ShapeDtypeStruct((2, PROBES, WIDTH), F32),
            jax.ShapeDtypeStruct((16, 3 * QUARTER, 128), F32),
            jax.ShapeDtypeStruct((4, PROBES, 128), F32),
        ),
        in_specs=[VMEM, VMEM, SMEM, SMEM, VMEM, VMEM],
        out_specs=(VMEM, VMEM, VMEM),
        scratch_shapes=[pltpu.VMEM((2, PROBES, LANES), F32)],
        cost_estimate=cost(10**9, 2 * 10**6),
        name="far",
    )(far, cross, lengthscales, amplitude, held, right)
    plane = exchange(plane, ("x", "y"))
    deep = pl.pallas_call(
        plane_kernel,
        out_shape=jax.ShapeDtypeStruct((8, 3 * QUARTER, 128), F32),
        in_specs=[VMEM],
        out_specs=VMEM,
        cost_estimate=cost(10**5, 3 * 10**5),
        name="plane",
    )(plane)
    deep = exchange(deep, "z")
    wide = pl.pallas_call(
        depth_kernel,
        out_shape=jax.ShapeDtypeStruct((8, PROBES + 5 * QUARTER, 128), F32),
        in_specs=[VMEM, VMEM],
        out_specs=VMEM,
        cost_estimate=cost(10**5, 5 * 10**5),
        name="depth",
    )(deep, low)
    wide = exchange(wide, ("y", "c"))
    return pl.pallas_call(
        final_kernel,
        out_shape=jax.ShapeDtypeStruct((2, PROBES, WIDTH), F32),
        in_specs=[VMEM] * 4,
        out_specs=VMEM,
        scratch_shapes=[pltpu.VMEM((LEVELS * PROBES, 2 * RANK), F32)],
        cost_estimate=cost(10**9, 3 * 10**6),
        name="final",
    )(wide, factor, coupling, diagonal)


def solution(mesh):
    fine = Mesh(mesh.devices.reshape(4, 8, 4, 2, 2), ("x", "z", "y", "h", "c"))
    every = ("x", "z", "y", "h", "c")
    in_specs = (P(None, every), P(None, every), P(), P(), P(), P())
    return jax.shard_map(
        on_device, mesh=fine, in_specs=in_specs, out_specs=P(None, None, every), check_vma=False
    )
```

```python
import math

import jax
import jax.numpy as jnp
from jax import lax
from jax.experimental import pallas as pl
from jax.experimental.pallas import tpu as pltpu
from jax.sharding import Mesh, PartitionSpec as P


LEVELS = 7
PROBES = 64
RANK = 128
HALF = RANK // 2
QUARTER = PROBES // 4
SPAN = 128
WIDTH = 512
TRANSFER = 80
LANES = 1024
BLOCK = 256
ROOT = math.sqrt(math.log2(math.e))
TWO_LN2 = 2.0 * math.log(2.0)
F32 = jnp.float32
BF16 = jnp.bfloat16
VMEM = pl.BlockSpec(memory_space=pltpu.VMEM)
ROOM = pltpu.CompilerParams(vmem_limit_bytes=16 * 2**20)
SMEM = pl.BlockSpec(memory_space=pltpu.SMEM)


def cost(flops, moved):
    return pl.CostEstimate(flops=flops, bytes_accessed=moved, transcendentals=0)


def split3(value):
    first = value.astype(BF16).astype(F32)
    rest = value - first
    second = rest.astype(BF16).astype(F32)
    third = (rest - second).astype(BF16).astype(F32)
    return first, second, third


def inverse_scales(scales_ref):
    row = lax.broadcasted_iota(jnp.int32, (8, 128), 0)
    held = jnp.full((8, 128), scales_ref[0], F32)
    for k in range(1, 8):
        held = jnp.where(row == k, scales_ref[k], held)
    return (ROOT / held)[:, :1]


def norms(value):
    return -0.5 * jnp.sum(value * value, axis=0, keepdims=True)


def stacked(parts, rows):
    width = parts[0].shape[1]
    index = lax.broadcasted_iota(jnp.int32, (8, width), 0)
    held = jnp.zeros((8, width), F32)
    for k, row in enumerate(rows):
        held = jnp.where(index == k, row, held)
    zeros = jnp.zeros((SPAN - 56, width), F32)
    return jnp.concatenate(list(parts) + [held, zeros], axis=0)


def left_form(value, extra):
    one, two, three = split3(value)
    n1, n2, n3 = split3(norms(value) + extra)
    return stacked((one, one, two, one, three, two), (1.0, 1.0, 1.0, n1, n2, n3))


def right_form(value, extra):
    one, two, three = split3(value)
    n1, n2, n3 = split3(norms(value) + extra)
    return stacked((one, two, one, three, one, two), (n1, n2, n3, 1.0, 1.0, 1.0))


def points_of(message, inverse):
    high = message[PROBES : PROBES + 8, :].astype(F32)
    low = message[PROBES + 8 : PROBES + 16, :].astype(F32)
    return ((high * 64.0 + low) * (1.0 / 4096.0) - 0.5) * inverse


def kernel_pair(exponent, log_strength):
    kern = jnp.exp2(exponent)
    return kern, kern * (TWO_LN2 * log_strength - TWO_LN2 * exponent)


def halved(value):
    top = value.astype(BF16)
    return top, (value - top.astype(F32)).astype(BF16)


def log2_strength(strength_ref):
    return jnp.log(jnp.full((1, 128), strength_ref[0], F32))[:, :1] * math.log2(math.e)


def prepare_kernel(coords_ref, probes_ref, out_ref):
    coords = coords_ref[...]
    high = jnp.right_shift(coords, 6)
    low = coords - high * 64
    out_ref[0:PROBES, :] = probes_ref[...].astype(BF16)
    both = jnp.concatenate([high.astype(F32), low.astype(F32)], axis=0)
    out_ref[PROBES:TRANSFER, :] = both.astype(BF16)


def accumulate(message_ref, inverse, right, log_strength, held_k, held_s, fresh):
    message = message_ref[...]
    left = left_form(points_of(message, inverse), 0.0).T.astype(BF16)
    for block in range(WIDTH // BLOCK):
        rows = left[block * BLOCK : (block + 1) * BLOCK, :]
        signs = message[0:PROBES, block * BLOCK : (block + 1) * BLOCK]
        for at in range(0, LANES, BLOCK):
            exponent = jnp.dot(rows, right[:, at : at + BLOCK], preferred_element_type=F32)
            sums = []
            for value in kernel_pair(exponent, log_strength):
                top, rest = halved(value)
                total = jnp.dot(signs, top, preferred_element_type=F32)
                if at >= WIDTH:
                    total = total + jnp.dot(signs, rest, preferred_element_type=F32)
                sums.append(total)
            add_k, add_s = sums
            if fresh and block == 0:
                held_k[:, at : at + BLOCK] = add_k
                held_s[:, at : at + BLOCK] = add_s
            else:
                held_k[:, at : at + BLOCK] += add_k
                held_s[:, at : at + BLOCK] += add_s


def near_kernel(
    own_ref, other_ref, scales_ref, strength_ref, marks_ref,
    held_ref, right_ref, factor_ref,
):
    row = lax.axis_index("x") * 32 + lax.axis_index("z") * 4 + lax.axis_index("y")
    core = lax.axis_index("c")
    inverse = inverse_scales(scales_ref)
    log_strength = log2_strength(strength_ref)
    own = points_of(own_ref[...], inverse)
    marks = []
    for level in range(LEVELS):
        node = 2 ** (LEVELS - level) - 2 + jnp.right_shift(row, level)
        marks.append((marks_ref[node] - 0.5) * inverse)
    halves = [jnp.where(core == 0, mark[:, :HALF], mark[:, HALF:]) for mark in marks]
    halves.append(jnp.zeros((8, HALF), F32))
    columns = jnp.concatenate([own] + halves, axis=1)
    right = right_form(columns, log_strength).astype(BF16)
    right_ref[...] = right
    accumulate(own_ref, inverse, right, log_strength, held_ref.at[0], held_ref.at[1], True)
    accumulate(other_ref, inverse, right, log_strength, held_ref.at[0], held_ref.at[1], False)
    own_right = right[:, :WIDTH]
    for level in range(LEVELS):
        turned = left_form(marks[level], 0.0).T.astype(BF16)
        exponent = jnp.dot(turned, own_right, preferred_element_type=F32)
        kern, slope = kernel_pair(exponent, log_strength)
        factor_ref[0, level * RANK : (level + 1) * RANK, :] = kern.astype(BF16)
        factor_ref[1, level * RANK : (level + 1) * RANK, :] = slope.astype(BF16)


def far_kernel(
    far_ref, cross_ref, scales_ref, strength_ref, held_ref, right_ref,
    diagonal_ref, plane_ref, low_ref, sums,
):
    x = lax.axis_index("x")
    y = lax.axis_index("y")
    inverse = inverse_scales(scales_ref)
    log_strength = log2_strength(strength_ref)
    right = right_ref[...]
    sums[...] = held_ref[...]
    accumulate(far_ref, inverse, right, log_strength, sums.at[0], sums.at[1], False)
    accumulate(cross_ref, inverse, right, log_strength, sums.at[0], sums.at[1], False)
    diagonal_ref[...] = sums[:, :, :WIDTH]
    units = []
    for level in range(LEVELS):
        at = WIDTH + level * HALF
        pair = [sums[0, :, at : at + HALF], sums[1, :, at : at + HALF]]
        units.append(jnp.concatenate(pair, axis=1))
    blank = jnp.zeros((2 * QUARTER, 128), F32)
    for at in range(4):
        part = slice(at * QUARTER, (at + 1) * QUARTER)
        mine = jnp.concatenate([units[2][part], units[3][part], units[4][part]], axis=0)
        plane_ref[x * 4 + at] = mine
        for apart, level in ((1, 5), (2, 6), (3, 6)):
            plane_ref[jnp.bitwise_xor(x, apart) * 4 + at] = jnp.concatenate([units[level][part], blank], axis=0)
    low_ref[y] = jnp.zeros((PROBES, 128), F32)
    for apart, level in ((1, 0), (2, 1), (3, 1)):
        low_ref[jnp.bitwise_xor(y, apart)] = units[level]


def plane_kernel(got_ref, out_ref):
    x = lax.axis_index("x")
    z = lax.axis_index("z")

    def total(apart, rows):
        start = jnp.bitwise_xor(x, apart) * 4
        parts = [got_ref[start + at, rows] for at in range(4)]
        return (parts[0] + parts[1]) + (parts[2] + parts[3])

    low, middle, high = slice(0, 16), slice(16, 32), slice(32, 48)
    sums = [total(0, low), total(0, middle), total(0, high)]
    five = total(1, low)
    six = total(2, low) + total(3, low)
    chosen = [jnp.zeros((QUARTER, 128), F32)] + sums
    for apart in range(8):
        which = apart.bit_length()
        out_ref[jnp.bitwise_xor(z, apart)] = jnp.concatenate([chosen[which], five, six], axis=0)


def depth_kernel(got_ref, low_ref, out_ref):
    z = lax.axis_index("z")

    def piece(apart, start):
        return got_ref[jnp.bitwise_xor(z, apart), start : start + QUARTER]

    two = piece(1, 0)
    three = piece(2, 0) + piece(3, 0)
    four = (piece(4, 0) + piece(5, 0)) + (piece(6, 0) + piece(7, 0))
    found = [two, three, four]
    for start in (QUARTER, 2 * QUARTER):
        parts = [piece(apart, start) for apart in range(8)]
        while len(parts) > 1:
            parts = [a + b for a, b in zip(parts[::2], parts[1::2])]
        found.append(parts[0])
    packed = jnp.concatenate(found, axis=0)
    for at in range(4):
        for core in range(2):
            out_ref[2 * at + core, 0:PROBES] = low_ref[at]
            out_ref[2 * at + core, PROBES:] = packed


def final_kernel(got_ref, factor_ref, coupling_ref, diagonal_ref, out_ref, sibling):
    y = lax.axis_index("y")
    row = lax.axis_index("x") * 32 + lax.axis_index("z") * 4 + y
    for core in range(2):
        lanes = slice(core * 128, core * 128 + 128)
        sibling[0:PROBES, lanes] = got_ref[jnp.bitwise_xor(y, 1) * 2 + core, 0:PROBES]
        pair = got_ref[jnp.bitwise_xor(y, 2) * 2 + core, 0:PROBES]
        pair = pair + got_ref[jnp.bitwise_xor(y, 3) * 2 + core, 0:PROBES]
        sibling[PROBES : 2 * PROBES, lanes] = pair
        for level in range(2, LEVELS):
            for at in range(4):
                start = level * PROBES + at * QUARTER
                source = PROBES + (level - 2) * QUARTER
                sibling[start : start + QUARTER, lanes] = got_ref[2 * at + core, source : source + QUARTER]
    coupling = coupling_ref[...]
    blank = jnp.zeros((HALF, RANK), F32)

    def spread(core_matrix):
        rows = []
        for core in range(2):
            part = core_matrix[core * HALF : (core + 1) * HALF, :]
            rows.append(jnp.concatenate([part, blank], axis=1))
            rows.append(jnp.concatenate([blank, part], axis=1))
        whole = jnp.concatenate(rows, axis=0)
        return halved(whole)

    values, remainders = halved(sibling[...])
    results = []
    for matrix in (coupling.T, coupling):
        top, rest = spread(matrix)
        results.append(
            jnp.dot(values, top, preferred_element_type=F32)
            + jnp.dot(values, rest, preferred_element_type=F32)
            + jnp.dot(remainders, top, preferred_element_type=F32)
        )
    heads = []
    for level in range(LEVELS):
        rows = slice(level * PROBES, (level + 1) * PROBES)
        left = jnp.bitwise_and(jnp.right_shift(row, level), 1) == 0
        heads.append(jnp.where(left, results[0][rows], results[1][rows]))
    firsts = jnp.concatenate([head[:, :RANK] for head in heads], axis=1)
    seconds = jnp.concatenate([head[:, RANK:] for head in heads], axis=1)
    top, rest = halved(jnp.concatenate([firsts, seconds], axis=0))
    stack = jnp.concatenate([top, rest], axis=0)
    on_kern = jnp.dot(stack, factor_ref[0], preferred_element_type=F32)
    pair = jnp.concatenate([top[:PROBES], rest[:PROBES]], axis=0)
    on_slope = jnp.dot(pair, factor_ref[1], preferred_element_type=F32)
    on_kern = on_kern[: 2 * PROBES] + on_kern[2 * PROBES :]
    on_slope = on_slope[:PROBES] + on_slope[PROBES:]
    out_ref[0] = diagonal_ref[0] + on_kern[:PROBES]
    out_ref[1] = diagonal_ref[1] + (on_kern[PROBES:] + on_slope)


def swap(value, axis):
    return lax.ppermute(value, axis, [(0, 1), (1, 0)])


def exchange(value, axes):
    return lax.all_to_all(value, axes, 0, 0, tiled=True)


def on_device(coords, probes, lengthscales, amplitude, landmarks, coupling):
    message = pl.pallas_call(
        prepare_kernel,
        out_shape=jax.ShapeDtypeStruct((TRANSFER, WIDTH), BF16),
        in_specs=[VMEM, VMEM],
        out_specs=VMEM,
        compiler_params=ROOM,
        cost_estimate=cost(10**5, 2 * 10**5),
        name="prepare",
    )(coords, probes)
    far = swap(message, "h")
    other = swap(message, "c")
    held, right, factor = pl.pallas_call(
        near_kernel,
        out_shape=(
            jax.ShapeDtypeStruct((2, PROBES, LANES), F32),
            jax.ShapeDtypeStruct((SPAN, LANES), BF16),
            jax.ShapeDtypeStruct((2, LEVELS * RANK, WIDTH), BF16),
        ),
        in_specs=[VMEM, VMEM, SMEM, SMEM, VMEM],
        out_specs=(VMEM, VMEM, VMEM),
        compiler_params=ROOM,
        cost_estimate=cost(2 * 10**9, 3 * 10**6),
        name="near",
    )(message, other, lengthscales, amplitude, landmarks)
    far, held, right = lax.optimization_barrier((far, held, right))
    cross = swap(far, "c")
    diagonal, plane, low = pl.pallas_call(
        far_kernel,
        out_shape=(
            jax.ShapeDtypeStruct((2, PROBES, WIDTH), F32),
            jax.ShapeDtypeStruct((16, 3 * QUARTER, 128), F32),
            jax.ShapeDtypeStruct((4, PROBES, 128), F32),
        ),
        in_specs=[VMEM, VMEM, SMEM, SMEM, VMEM, VMEM],
        out_specs=(VMEM, VMEM, VMEM),
        scratch_shapes=[pltpu.VMEM((2, PROBES, LANES), F32)],
        compiler_params=ROOM,
        cost_estimate=cost(10**9, 2 * 10**6),
        name="far",
    )(far, cross, lengthscales, amplitude, held, right)
    plane = exchange(plane, ("x", "y"))
    deep = pl.pallas_call(
        plane_kernel,
        out_shape=jax.ShapeDtypeStruct((8, 3 * QUARTER, 128), F32),
        in_specs=[VMEM],
        out_specs=VMEM,
        compiler_params=ROOM,
        cost_estimate=cost(10**5, 3 * 10**5),
        name="plane",
    )(plane)
    deep = exchange(deep, "z")
    wide = pl.pallas_call(
        depth_kernel,
        out_shape=jax.ShapeDtypeStruct((8, PROBES + 5 * QUARTER, 128), F32),
        in_specs=[VMEM, VMEM],
        out_specs=VMEM,
        compiler_params=ROOM,
        cost_estimate=cost(10**5, 5 * 10**5),
        name="depth",
    )(deep, low)
    wide = exchange(wide, ("y", "c"))
    return pl.pallas_call(
        final_kernel,
        out_shape=jax.ShapeDtypeStruct((2, PROBES, WIDTH), F32),
        in_specs=[VMEM] * 4,
        out_specs=VMEM,
        scratch_shapes=[pltpu.VMEM((LEVELS * PROBES, 2 * RANK), F32)],
        compiler_params=ROOM,
        cost_estimate=cost(10**9, 3 * 10**6),
        name="final",
    )(wide, factor, coupling, diagonal)


def solution(mesh):
    fine = Mesh(mesh.devices.reshape(4, 8, 4, 2, 2), ("x", "z", "y", "h", "c"))
    every = ("x", "z", "y", "h", "c")
    in_specs = (P(None, every), P(None, every), P(), P(), P(), P())
    return jax.shard_map(
        on_device, mesh=fine, in_specs=in_specs, out_specs=P(None, None, every), check_vma=False
    )
```

```python
import math

import jax
import jax.numpy as jnp
from jax import lax
from jax.experimental import pallas as pl
from jax.experimental.pallas import tpu as pltpu
from jax.sharding import Mesh, PartitionSpec as P


LEVELS = 7
PROBES = 64
RANK = 128
HALF = RANK // 2
QUARTER = PROBES // 4
SPAN = 128
WIDTH = 512
TRANSFER = 80
LANES = 1024
BLOCK = 256
ROOT = math.sqrt(math.log2(math.e))
TWO_LN2 = 2.0 * math.log(2.0)
F32 = jnp.float32
BF16 = jnp.bfloat16
I16 = jnp.int16
FINE = 2.0**26
OCTAVES = 44.0
VMEM = pl.BlockSpec(memory_space=pltpu.VMEM)
ROOM = pltpu.CompilerParams(vmem_limit_bytes=16 * 2**20)
SMEM = pl.BlockSpec(memory_space=pltpu.SMEM)


def cost(flops, moved):
    return pl.CostEstimate(flops=flops, bytes_accessed=moved, transcendentals=0)


def split3(value):
    first = value.astype(BF16).astype(F32)
    rest = value - first
    second = rest.astype(BF16).astype(F32)
    third = (rest - second).astype(BF16).astype(F32)
    return first, second, third


def norms(value):
    return -0.5 * jnp.sum(value * value, axis=0, keepdims=True)


def stacked(parts, rows):
    width = parts[0].shape[1]
    index = lax.broadcasted_iota(jnp.int32, (8, width), 0)
    held = jnp.zeros((8, width), F32)
    for k, row in enumerate(rows):
        held = jnp.where(index == k, row, held)
    zeros = jnp.zeros((SPAN - 56, width), F32)
    return jnp.concatenate(list(parts) + [held, zeros], axis=0)


def left_form(value, extra):
    one, two, three = split3(value)
    n1, n2, n3 = split3(norms(value) + extra)
    return stacked((one, one, two, one, three, two), (1.0, 1.0, 1.0, n1, n2, n3))


def right_form(value, extra):
    one, two, three = split3(value)
    n1, n2, n3 = split3(norms(value) + extra)
    return stacked((one, two, one, three, one, two), (n1, n2, n3, 1.0, 1.0, 1.0))


def points_of(message, inverse):
    high = message[PROBES : PROBES + 8, :].astype(F32)
    low = message[PROBES + 8 : PROBES + 16, :].astype(F32)
    return ((high * 64.0 + low) * (1.0 / 4096.0) - 0.5) * inverse


def kernel_pair(exponent, log_strength):
    kern = jnp.exp2(exponent)
    return kern, kern * (TWO_LN2 * log_strength - TWO_LN2 * exponent)


def halved(value):
    top = value.astype(BF16)
    return top, (value - top.astype(F32)).astype(BF16)


def encode(value):
    grade = jnp.log(1.0 + jnp.abs(value) * FINE) * (32767.0 / (OCTAVES * math.log(2.0))) + 0.5
    return jnp.where(value < 0.0, -grade, grade).astype(jnp.int32).astype(jnp.int16)


def decode(code):
    grade = code.astype(jnp.int32).astype(F32)
    size = (jnp.exp2(jnp.abs(grade) * (OCTAVES / 32767.0)) - 1.0) * (1.0 / FINE)
    return jnp.where(grade < 0.0, -size, size)


def prepare_kernel(
    coords_ref, probes_ref, marks_ref, scales_ref, strength_ref,
    out_ref, picked_ref, facts_ref, coords_buf, probes_buf, scales_buf, sem,
):
    row = lax.axis_index("x") * 32 + lax.axis_index("z") * 4 + lax.axis_index("y")
    copies = [
        pltpu.make_async_copy(probes_ref, probes_buf, sem.at[0]),
        pltpu.make_async_copy(coords_ref, coords_buf, sem.at[1]),
        pltpu.make_async_copy(scales_ref, scales_buf, sem.at[2 + LEVELS]),
    ]
    for level in range(LEVELS):
        node = 2 ** (LEVELS - level) - 2 + jnp.right_shift(row, level)
        copies.append(pltpu.make_async_copy(marks_ref.at[node], picked_ref.at[level], sem.at[2 + level]))
    for copy in copies:
        copy.start()
    for copy in copies:
        copy.wait()
    coords = coords_buf[...]
    high = jnp.right_shift(coords, 6)
    low = coords - high * 64
    out_ref[0:PROBES, :] = probes_buf[...].astype(BF16)
    both = jnp.concatenate([high.astype(F32), low.astype(F32)], axis=0)
    out_ref[PROBES:TRANSFER, :] = both.astype(BF16)
    place = lax.broadcasted_iota(jnp.int32, (8, 128), 0)
    held = jnp.full((8, 128), scales_buf[0], F32)
    for k in range(1, 8):
        held = jnp.where(place == k, scales_buf[k], held)
    facts_ref[0:8, :] = ROOT / held
    facts_ref[8:16, :] = jnp.log(jnp.full((8, 128), strength_ref[0], F32)) * math.log2(math.e)


def accumulate(message_ref, inverse, right, log_strength, held_k, held_s, fresh):
    message = message_ref[...]
    left = left_form(points_of(message, inverse), 0.0).T.astype(BF16)
    for block in range(WIDTH // BLOCK):
        rows = left[block * BLOCK : (block + 1) * BLOCK, :]
        signs = message[0:PROBES, block * BLOCK : (block + 1) * BLOCK]
        for at in range(0, LANES, BLOCK):
            exponent = jnp.dot(rows, right[:, at : at + BLOCK], preferred_element_type=F32)
            sums = []
            for value in kernel_pair(exponent, log_strength):
                top, rest = halved(value)
                total = jnp.dot(signs, top, preferred_element_type=F32)
                if at >= WIDTH:
                    total = total + jnp.dot(signs, rest, preferred_element_type=F32)
                sums.append(total)
            add_k, add_s = sums
            if fresh and block == 0:
                held_k[:, at : at + BLOCK] = add_k
                held_s[:, at : at + BLOCK] = add_s
            else:
                held_k[:, at : at + BLOCK] += add_k
                held_s[:, at : at + BLOCK] += add_s


def near_kernel(
    own_ref, other_ref, facts_ref, marks_ref,
    held_ref, right_ref, factor_ref,
):
    core = lax.axis_index("c")
    inverse = facts_ref[0:8, 0:1]
    log_strength = facts_ref[8:9, 0:1]
    own = points_of(own_ref[...], inverse)
    marks = [(marks_ref[level] - 0.5) * inverse for level in range(LEVELS)]
    halves = [jnp.where(core == 0, mark[:, :HALF], mark[:, HALF:]) for mark in marks]
    halves.append(jnp.zeros((8, HALF), F32))
    columns = jnp.concatenate([own] + halves, axis=1)
    right = right_form(columns, log_strength).astype(BF16)
    right_ref[...] = right
    accumulate(own_ref, inverse, right, log_strength, held_ref.at[0], held_ref.at[1], True)
    accumulate(other_ref, inverse, right, log_strength, held_ref.at[0], held_ref.at[1], False)
    own_right = right[:, :WIDTH]
    for level in range(LEVELS):
        turned = left_form(marks[level], 0.0).T.astype(BF16)
        exponent = jnp.dot(turned, own_right, preferred_element_type=F32)
        kern, slope = kernel_pair(exponent, log_strength)
        factor_ref[0, level * RANK : (level + 1) * RANK, :] = kern.astype(BF16)
        factor_ref[1, level * RANK : (level + 1) * RANK, :] = slope.astype(BF16)


def far_kernel(
    far_ref, cross_ref, facts_ref, held_ref, right_ref,
    diagonal_ref, plane_ref, low_ref, sums,
):
    x = lax.axis_index("x")
    y = lax.axis_index("y")
    inverse = facts_ref[0:8, 0:1]
    log_strength = facts_ref[8:9, 0:1]
    right = right_ref[...]
    sums[...] = held_ref[...]
    accumulate(far_ref, inverse, right, log_strength, sums.at[0], sums.at[1], False)
    accumulate(cross_ref, inverse, right, log_strength, sums.at[0], sums.at[1], False)
    diagonal_ref[...] = sums[:, :, :WIDTH]
    units = []
    for level in range(LEVELS):
        at = WIDTH + level * HALF
        pair = [sums[0, :, at : at + HALF], sums[1, :, at : at + HALF]]
        units.append(encode(jnp.concatenate(pair, axis=1)))
    blank = jnp.zeros((2 * QUARTER, 128), I16)
    for at in range(4):
        part = slice(at * QUARTER, (at + 1) * QUARTER)
        mine = jnp.concatenate([units[2][part], units[3][part], units[4][part]], axis=0)
        plane_ref[x * 4 + at] = mine
        for apart, level in ((1, 5), (2, 6), (3, 6)):
            plane_ref[jnp.bitwise_xor(x, apart) * 4 + at] = jnp.concatenate([units[level][part], blank], axis=0)
    low_ref[y] = jnp.zeros((PROBES, 128), I16)
    for apart, level in ((1, 0), (2, 1), (3, 1)):
        low_ref[jnp.bitwise_xor(y, apart)] = units[level]


def plane_kernel(got_ref, out_ref):
    x = lax.axis_index("x")
    z = lax.axis_index("z")

    def total(apart, rows):
        start = jnp.bitwise_xor(x, apart) * 4
        parts = [decode(got_ref[start + at, rows]) for at in range(4)]
        return (parts[0] + parts[1]) + (parts[2] + parts[3])

    low, middle, high = slice(0, 16), slice(16, 32), slice(32, 48)
    sums = [total(0, low), total(0, middle), total(0, high)]
    five = encode(total(1, low))
    six = encode(total(2, low) + total(3, low))
    chosen = [jnp.zeros((QUARTER, 128), I16)] + [encode(value) for value in sums]
    for apart in range(8):
        which = apart.bit_length()
        out_ref[jnp.bitwise_xor(z, apart)] = jnp.concatenate([chosen[which], five, six], axis=0)


def depth_kernel(got_ref, low_ref, out_ref):
    z = lax.axis_index("z")

    def piece(apart, start):
        return decode(got_ref[jnp.bitwise_xor(z, apart), start : start + QUARTER])

    two = piece(1, 0)
    three = piece(2, 0) + piece(3, 0)
    four = (piece(4, 0) + piece(5, 0)) + (piece(6, 0) + piece(7, 0))
    found = [two, three, four]
    for start in (QUARTER, 2 * QUARTER):
        parts = [piece(apart, start) for apart in range(8)]
        while len(parts) > 1:
            parts = [a + b for a, b in zip(parts[::2], parts[1::2])]
        found.append(parts[0])
    packed = jnp.concatenate([encode(value) for value in found], axis=0)
    for at in range(4):
        for core in range(2):
            out_ref[2 * at + core, 0:PROBES] = low_ref[at]
            out_ref[2 * at + core, PROBES:] = packed


def final_kernel(got_ref, factor_ref, coupling_ref, diagonal_ref, out_ref, sibling):
    y = lax.axis_index("y")
    row = lax.axis_index("x") * 32 + lax.axis_index("z") * 4 + y
    for core in range(2):
        lanes = slice(core * 128, core * 128 + 128)
        sibling[0:PROBES, lanes] = decode(got_ref[jnp.bitwise_xor(y, 1) * 2 + core, 0:PROBES])
        pair = decode(got_ref[jnp.bitwise_xor(y, 2) * 2 + core, 0:PROBES])
        pair = pair + decode(got_ref[jnp.bitwise_xor(y, 3) * 2 + core, 0:PROBES])
        sibling[PROBES : 2 * PROBES, lanes] = pair
        for level in range(2, LEVELS):
            for at in range(4):
                start = level * PROBES + at * QUARTER
                source = PROBES + (level - 2) * QUARTER
                sibling[start : start + QUARTER, lanes] = decode(got_ref[2 * at + core, source : source + QUARTER])
    coupling = coupling_ref[...]
    blank = jnp.zeros((HALF, RANK), F32)

    def spread(core_matrix):
        rows = []
        for core in range(2):
            part = core_matrix[core * HALF : (core + 1) * HALF, :]
            rows.append(jnp.concatenate([part, blank], axis=1))
            rows.append(jnp.concatenate([blank, part], axis=1))
        whole = jnp.concatenate(rows, axis=0)
        return halved(whole)

    values, remainders = halved(sibling[...])
    results = []
    for matrix in (coupling.T, coupling):
        top, rest = spread(matrix)
        results.append(
            jnp.dot(values, top, preferred_element_type=F32)
            + jnp.dot(values, rest, preferred_element_type=F32)
            + jnp.dot(remainders, top, preferred_element_type=F32)
        )
    heads = []
    for level in range(LEVELS):
        rows = slice(level * PROBES, (level + 1) * PROBES)
        left = jnp.bitwise_and(jnp.right_shift(row, level), 1) == 0
        heads.append(jnp.where(left, results[0][rows], results[1][rows]))
    firsts = jnp.concatenate([head[:, :RANK] for head in heads], axis=1)
    seconds = jnp.concatenate([head[:, RANK:] for head in heads], axis=1)
    top, rest = halved(jnp.concatenate([firsts, seconds], axis=0))
    stack = jnp.concatenate([top, rest], axis=0)
    on_kern = jnp.dot(stack, factor_ref[0], preferred_element_type=F32)
    pair = jnp.concatenate([top[:PROBES], rest[:PROBES]], axis=0)
    on_slope = jnp.dot(pair, factor_ref[1], preferred_element_type=F32)
    on_kern = on_kern[: 2 * PROBES] + on_kern[2 * PROBES :]
    on_slope = on_slope[:PROBES] + on_slope[PROBES:]
    out_ref[0] = diagonal_ref[0] + on_kern[:PROBES]
    out_ref[1] = diagonal_ref[1] + (on_kern[PROBES:] + on_slope)


def stay(array):
    return pltpu.with_memory_space_constraint(array, pltpu.HBM)


def swap(value, axis):
    return lax.ppermute(value, axis, [(0, 1), (1, 0)])


def exchange(value, axes):
    return lax.all_to_all(value, axes, 0, 0, tiled=True)


def on_device(coords, probes, lengthscales, amplitude, landmarks, coupling):
    message, marks, facts = pl.pallas_call(
        prepare_kernel,
        out_shape=(
            jax.ShapeDtypeStruct((TRANSFER, WIDTH), BF16),
            jax.ShapeDtypeStruct((LEVELS, 8, RANK), F32),
            jax.ShapeDtypeStruct((16, 128), F32),
        ),
        in_specs=[pl.BlockSpec(memory_space=pltpu.HBM)] * 4 + [SMEM],
        out_specs=(VMEM, VMEM, VMEM),
        scratch_shapes=[
            pltpu.VMEM((8, WIDTH), jnp.int32),
            pltpu.VMEM((PROBES, WIDTH), F32),
            pltpu.SMEM((8,), F32),
            pltpu.SemaphoreType.DMA((3 + LEVELS,)),
        ],
        compiler_params=ROOM,
        cost_estimate=cost(10**5, 2 * 10**5),
        name="prepare",
    )(*[stay(array) for array in (coords, probes, landmarks, lengthscales)], amplitude)
    far = swap(message, "h")
    other = swap(message, "c")
    held, right, factor = pl.pallas_call(
        near_kernel,
        out_shape=(
            jax.ShapeDtypeStruct((2, PROBES, LANES), F32),
            jax.ShapeDtypeStruct((SPAN, LANES), BF16),
            jax.ShapeDtypeStruct((2, LEVELS * RANK, WIDTH), BF16),
        ),
        in_specs=[VMEM] * 4,
        out_specs=(VMEM, VMEM, VMEM),
        compiler_params=ROOM,
        cost_estimate=cost(2 * 10**9, 3 * 10**6),
        name="near",
    )(message, other, facts, marks)
    far, held, right = lax.optimization_barrier((far, held, right))
    cross = swap(far, "c")
    diagonal, plane, low = pl.pallas_call(
        far_kernel,
        out_shape=(
            jax.ShapeDtypeStruct((2, PROBES, WIDTH), F32),
            jax.ShapeDtypeStruct((16, 3 * QUARTER, 128), I16),
            jax.ShapeDtypeStruct((4, PROBES, 128), I16),
        ),
        in_specs=[VMEM] * 5,
        out_specs=(VMEM, VMEM, VMEM),
        scratch_shapes=[pltpu.VMEM((2, PROBES, LANES), F32)],
        compiler_params=ROOM,
        cost_estimate=cost(10**9, 2 * 10**6),
        name="far",
    )(far, cross, facts, held, right)
    plane = exchange(plane, ("x", "y"))
    deep = pl.pallas_call(
        plane_kernel,
        out_shape=jax.ShapeDtypeStruct((8, 3 * QUARTER, 128), I16),
        in_specs=[VMEM],
        out_specs=VMEM,
        compiler_params=ROOM,
        cost_estimate=cost(10**5, 3 * 10**5),
        name="plane",
    )(plane)
    deep = exchange(deep, "z")
    wide = pl.pallas_call(
        depth_kernel,
        out_shape=jax.ShapeDtypeStruct((8, PROBES + 5 * QUARTER, 128), I16),
        in_specs=[VMEM, VMEM],
        out_specs=VMEM,
        compiler_params=ROOM,
        cost_estimate=cost(10**5, 5 * 10**5),
        name="depth",
    )(deep, low)
    wide = exchange(wide, ("y", "c"))
    return pl.pallas_call(
        final_kernel,
        out_shape=jax.ShapeDtypeStruct((2, PROBES, WIDTH), F32),
        in_specs=[VMEM] * 4,
        out_specs=VMEM,
        scratch_shapes=[pltpu.VMEM((LEVELS * PROBES, 2 * RANK), F32)],
        compiler_params=ROOM,
        cost_estimate=cost(10**9, 3 * 10**6),
        name="final",
    )(wide, factor, coupling, diagonal)


def solution(mesh):
    fine = Mesh(mesh.devices.reshape(4, 8, 4, 2, 2), ("x", "z", "y", "h", "c"))
    every = ("x", "z", "y", "h", "c")
    in_specs = (P(None, every), P(None, every), P(), P(), P(), P())
    return jax.shard_map(
        on_device, mesh=fine, in_specs=in_specs, out_specs=P(None, None, every), check_vma=False
    )
```

```python
import math

import jax
import jax.numpy as jnp
from jax import lax
from jax.experimental import pallas as pl
from jax.experimental.pallas import tpu as pltpu
from jax.sharding import Mesh, PartitionSpec as P


LEVELS = 7
PROBES = 64
RANK = 128
HALF = RANK // 2
QUARTER = PROBES // 4
SPAN = 128
WIDTH = 512
TRANSFER = 80
LANES = 1024
BLOCK = 256
ROOT = math.sqrt(math.log2(math.e))
TWO_LN2 = 2.0 * math.log(2.0)
F32 = jnp.float32
BF16 = jnp.bfloat16
I16 = jnp.int16
FINE = 2.0**26
OCTAVES = 44.0
VMEM = pl.BlockSpec(memory_space=pltpu.VMEM)
ROOM = pltpu.CompilerParams(vmem_limit_bytes=16 * 2**20)
SMEM = pl.BlockSpec(memory_space=pltpu.SMEM)


def cost(flops, moved):
    return pl.CostEstimate(flops=flops, bytes_accessed=moved, transcendentals=0)


def split3(value):
    first = value.astype(BF16).astype(F32)
    rest = value - first
    second = rest.astype(BF16).astype(F32)
    third = (rest - second).astype(BF16).astype(F32)
    return first, second, third


def norms(value):
    return -0.5 * jnp.sum(value * value, axis=0, keepdims=True)


def stacked(parts, rows):
    width = parts[0].shape[1]
    index = lax.broadcasted_iota(jnp.int32, (8, width), 0)
    held = jnp.zeros((8, width), F32)
    for k, row in enumerate(rows):
        held = jnp.where(index == k, row, held)
    zeros = jnp.zeros((SPAN - 56, width), F32)
    return jnp.concatenate(list(parts) + [held, zeros], axis=0)


def left_form(value, extra):
    one, two, three = split3(value)
    n1, n2, n3 = split3(norms(value) + extra)
    return stacked((one, one, two, one, three, two), (1.0, 1.0, 1.0, n1, n2, n3))


def right_form(value, extra):
    one, two, three = split3(value)
    n1, n2, n3 = split3(norms(value) + extra)
    return stacked((one, two, one, three, one, two), (n1, n2, n3, 1.0, 1.0, 1.0))


def points_of(message, inverse):
    high = message[PROBES : PROBES + 8, :].astype(F32)
    low = message[PROBES + 8 : PROBES + 16, :].astype(F32)
    return ((high * 64.0 + low) * (1.0 / 4096.0) - 0.5) * inverse


def kernel_pair(exponent, log_strength):
    kern = jnp.exp2(exponent)
    return kern, kern * (TWO_LN2 * log_strength - TWO_LN2 * exponent)


def halved(value):
    top = value.astype(BF16)
    return top, (value - top.astype(F32)).astype(BF16)


def encode(value):
    grade = jnp.log(1.0 + jnp.abs(value) * FINE) * (32767.0 / (OCTAVES * math.log(2.0))) + 0.5
    return jnp.where(value < 0.0, -grade, grade).astype(jnp.int32).astype(jnp.int16)


def decode(code):
    grade = code.astype(jnp.int32).astype(F32)
    size = (jnp.exp2(jnp.abs(grade) * (OCTAVES / 32767.0)) - 1.0) * (1.0 / FINE)
    return jnp.where(grade < 0.0, -size, size)


def prepare_kernel(
    coords_ref, probes_ref, marks_ref, scales_ref, strength_ref,
    out_ref, picked_ref, facts_ref, coords_buf, probes_buf, scales_buf, sem,
):
    row = lax.axis_index("x") * 32 + lax.axis_index("z") * 4 + lax.axis_index("y")
    copies = [
        pltpu.make_async_copy(probes_ref, probes_buf, sem.at[0]),
        pltpu.make_async_copy(coords_ref, coords_buf, sem.at[1]),
        pltpu.make_async_copy(scales_ref, scales_buf, sem.at[2 + LEVELS]),
    ]
    for level in range(LEVELS):
        node = 2 ** (LEVELS - level) - 2 + jnp.right_shift(row, level)
        copies.append(pltpu.make_async_copy(marks_ref.at[node], picked_ref.at[level], sem.at[2 + level]))
    for copy in copies:
        copy.start()
    for copy in copies:
        copy.wait()
    coords = coords_buf[...]
    high = jnp.right_shift(coords, 6)
    low = coords - high * 64
    out_ref[0:PROBES, :] = probes_buf[...].astype(BF16)
    both = jnp.concatenate([high.astype(F32), low.astype(F32)], axis=0)
    out_ref[PROBES:TRANSFER, :] = both.astype(BF16)
    place = lax.broadcasted_iota(jnp.int32, (8, 128), 0)
    held = jnp.full((8, 128), scales_buf[0], F32)
    for k in range(1, 8):
        held = jnp.where(place == k, scales_buf[k], held)
    facts_ref[0:8, :] = ROOT / held
    facts_ref[8:16, :] = jnp.log(jnp.full((8, 128), strength_ref[0], F32)) * math.log2(math.e)


def accumulate(message_ref, inverse, right, log_strength, held_k, held_s, fresh):
    message = message_ref[...]
    left = left_form(points_of(message, inverse), 0.0).T.astype(BF16)
    for block in range(WIDTH // BLOCK):
        rows = left[block * BLOCK : (block + 1) * BLOCK, :]
        signs = message[0:PROBES, block * BLOCK : (block + 1) * BLOCK]
        for at in range(0, LANES, BLOCK):
            exponent = jnp.dot(rows, right[:, at : at + BLOCK], preferred_element_type=F32)
            sums = []
            for value in kernel_pair(exponent, log_strength):
                top, rest = halved(value)
                total = jnp.dot(signs, top, preferred_element_type=F32)
                if at >= WIDTH:
                    total = total + jnp.dot(signs, rest, preferred_element_type=F32)
                sums.append(total)
            add_k, add_s = sums
            if fresh and block == 0:
                held_k[:, at : at + BLOCK] = add_k
                held_s[:, at : at + BLOCK] = add_s
            else:
                held_k[:, at : at + BLOCK] += add_k
                held_s[:, at : at + BLOCK] += add_s


def near_kernel(
    own_ref, other_ref, facts_ref, marks_ref,
    held_ref, right_ref, factor_ref,
):
    core = lax.axis_index("c")
    inverse = facts_ref[0:8, 0:1]
    log_strength = facts_ref[8:9, 0:1]
    own = points_of(own_ref[...], inverse)
    marks = [(marks_ref[level] - 0.5) * inverse for level in range(LEVELS)]
    halves = [jnp.where(core == 0, mark[:, :HALF], mark[:, HALF:]) for mark in marks]
    halves.append(jnp.zeros((8, HALF), F32))
    columns = jnp.concatenate([own] + halves, axis=1)
    right = right_form(columns, log_strength).astype(BF16)
    right_ref[...] = right
    accumulate(own_ref, inverse, right, log_strength, held_ref.at[0], held_ref.at[1], True)
    accumulate(other_ref, inverse, right, log_strength, held_ref.at[0], held_ref.at[1], False)
    own_right = right[:, :WIDTH]
    for level in range(LEVELS):
        turned = left_form(marks[level], 0.0).T.astype(BF16)
        exponent = jnp.dot(turned, own_right, preferred_element_type=F32)
        kern, slope = kernel_pair(exponent, log_strength)
        factor_ref[0, level * RANK : (level + 1) * RANK, :] = kern.astype(BF16)
        factor_ref[1, level * RANK : (level + 1) * RANK, :] = slope.astype(BF16)


def far_kernel(
    far_ref, cross_ref, facts_ref, held_ref, right_ref,
    diagonal_ref, line_ref, low_ref, sums,
):
    y = lax.axis_index("y")
    inverse = facts_ref[0:8, 0:1]
    log_strength = facts_ref[8:9, 0:1]
    right = right_ref[...]
    sums[...] = held_ref[...]
    accumulate(far_ref, inverse, right, log_strength, sums.at[0], sums.at[1], False)
    accumulate(cross_ref, inverse, right, log_strength, sums.at[0], sums.at[1], False)
    diagonal_ref[...] = sums[:, :, :WIDTH]
    units = []
    for level in range(LEVELS):
        at = WIDTH + level * HALF
        pair = [sums[0, :, at : at + HALF], sums[1, :, at : at + HALF]]
        units.append(encode(jnp.concatenate(pair, axis=1)))
    for at in range(4):
        part = slice(at * QUARTER, (at + 1) * QUARTER)
        line_ref[at] = jnp.concatenate([units[level][part] for level in range(2, LEVELS)], axis=0)
    low_ref[y] = jnp.zeros((PROBES, 128), I16)
    for apart, level in ((1, 0), (2, 1), (3, 1)):
        low_ref[jnp.bitwise_xor(y, apart)] = units[level]


def line_kernel(got_ref, out_ref):
    x = lax.axis_index("x")
    z = lax.axis_index("z")
    total = (decode(got_ref[0]) + decode(got_ref[1])) + (decode(got_ref[2]) + decode(got_ref[3]))
    packed = encode(total)
    parts = [packed[at * QUARTER : (at + 1) * QUARTER] for at in range(LEVELS - 2)]
    for aside in range(4):
        for apart in range(8):
            place = jnp.bitwise_xor(x, aside) * 8 + jnp.bitwise_xor(z, apart)
            if aside > 0:
                out_ref[place] = parts[2 + aside.bit_length()]
            elif apart > 0:
                out_ref[place] = parts[apart.bit_length() - 1]
            else:
                out_ref[place] = jnp.zeros((QUARTER, 128), I16)


def added(parts):
    while len(parts) > 1:
        parts = [a + b for a, b in zip(parts[::2], parts[1::2])]
    return parts[0]


def depth_kernel(got_ref, low_ref, out_ref):
    x = lax.axis_index("x")
    z = lax.axis_index("z")

    def total(asides, aparts):
        return added([
            decode(got_ref[jnp.bitwise_xor(x, aside) * 8 + jnp.bitwise_xor(z, apart)])
            for aside in asides for apart in aparts
        ])

    found = [
        total((0,), (1,)),
        total((0,), (2, 3)),
        total((0,), (4, 5, 6, 7)),
        total((1,), range(8)),
        total((2, 3), range(8)),
    ]
    packed = encode(jnp.concatenate(found, axis=0))
    for at in range(4):
        for core in range(2):
            out_ref[2 * at + core, 0:PROBES] = low_ref[at]
            out_ref[2 * at + core, PROBES:] = packed


def final_kernel(got_ref, factor_ref, coupling_ref, diagonal_ref, out_ref, sibling):
    y = lax.axis_index("y")
    row = lax.axis_index("x") * 32 + lax.axis_index("z") * 4 + y
    for core in range(2):
        lanes = slice(core * 128, core * 128 + 128)
        sibling[0:PROBES, lanes] = decode(got_ref[jnp.bitwise_xor(y, 1) * 2 + core, 0:PROBES])
        pair = decode(got_ref[jnp.bitwise_xor(y, 2) * 2 + core, 0:PROBES])
        pair = pair + decode(got_ref[jnp.bitwise_xor(y, 3) * 2 + core, 0:PROBES])
        sibling[PROBES : 2 * PROBES, lanes] = pair
        for level in range(2, LEVELS):
            for at in range(4):
                start = level * PROBES + at * QUARTER
                source = PROBES + (level - 2) * QUARTER
                sibling[start : start + QUARTER, lanes] = decode(got_ref[2 * at + core, source : source + QUARTER])
    coupling = coupling_ref[...]
    blank = jnp.zeros((HALF, RANK), F32)

    def spread(core_matrix):
        rows = []
        for core in range(2):
            part = core_matrix[core * HALF : (core + 1) * HALF, :]
            rows.append(jnp.concatenate([part, blank], axis=1))
            rows.append(jnp.concatenate([blank, part], axis=1))
        whole = jnp.concatenate(rows, axis=0)
        return halved(whole)

    values, remainders = halved(sibling[...])
    results = []
    for matrix in (coupling.T, coupling):
        top, rest = spread(matrix)
        results.append(
            jnp.dot(values, top, preferred_element_type=F32)
            + jnp.dot(values, rest, preferred_element_type=F32)
            + jnp.dot(remainders, top, preferred_element_type=F32)
        )
    heads = []
    for level in range(LEVELS):
        rows = slice(level * PROBES, (level + 1) * PROBES)
        left = jnp.bitwise_and(jnp.right_shift(row, level), 1) == 0
        heads.append(jnp.where(left, results[0][rows], results[1][rows]))
    firsts = jnp.concatenate([head[:, :RANK] for head in heads], axis=1)
    seconds = jnp.concatenate([head[:, RANK:] for head in heads], axis=1)
    top, rest = halved(jnp.concatenate([firsts, seconds], axis=0))
    stack = jnp.concatenate([top, rest], axis=0)
    on_kern = jnp.dot(stack, factor_ref[0], preferred_element_type=F32)
    pair = jnp.concatenate([top[:PROBES], rest[:PROBES]], axis=0)
    on_slope = jnp.dot(pair, factor_ref[1], preferred_element_type=F32)
    on_kern = on_kern[: 2 * PROBES] + on_kern[2 * PROBES :]
    on_slope = on_slope[:PROBES] + on_slope[PROBES:]
    out_ref[0] = diagonal_ref[0] + on_kern[:PROBES]
    out_ref[1] = diagonal_ref[1] + (on_kern[PROBES:] + on_slope)


def stay(array):
    return pltpu.with_memory_space_constraint(array, pltpu.HBM)


def swap(value, axis):
    return lax.ppermute(value, axis, [(0, 1), (1, 0)])


def exchange(value, axes):
    return lax.all_to_all(value, axes, 0, 0, tiled=True)


def on_device(coords, probes, lengthscales, amplitude, landmarks, coupling):
    message, marks, facts = pl.pallas_call(
        prepare_kernel,
        out_shape=(
            jax.ShapeDtypeStruct((TRANSFER, WIDTH), BF16),
            jax.ShapeDtypeStruct((LEVELS, 8, RANK), F32),
            jax.ShapeDtypeStruct((16, 128), F32),
        ),
        in_specs=[pl.BlockSpec(memory_space=pltpu.HBM)] * 4 + [SMEM],
        out_specs=(VMEM, VMEM, VMEM),
        scratch_shapes=[
            pltpu.VMEM((8, WIDTH), jnp.int32),
            pltpu.VMEM((PROBES, WIDTH), F32),
            pltpu.SMEM((8,), F32),
            pltpu.SemaphoreType.DMA((3 + LEVELS,)),
        ],
        compiler_params=ROOM,
        cost_estimate=cost(10**5, 2 * 10**5),
        name="prepare",
    )(*[stay(array) for array in (coords, probes, landmarks, lengthscales)], amplitude)
    far = swap(message, "h")
    other = swap(message, "c")
    held, right, factor = pl.pallas_call(
        near_kernel,
        out_shape=(
            jax.ShapeDtypeStruct((2, PROBES, LANES), F32),
            jax.ShapeDtypeStruct((SPAN, LANES), BF16),
            jax.ShapeDtypeStruct((2, LEVELS * RANK, WIDTH), BF16),
        ),
        in_specs=[VMEM] * 4,
        out_specs=(VMEM, VMEM, VMEM),
        compiler_params=ROOM,
        cost_estimate=cost(2 * 10**9, 3 * 10**6),
        name="near",
    )(message, other, facts, marks)
    far, held, right = lax.optimization_barrier((far, held, right))
    cross = swap(far, "c")
    diagonal, line, low = pl.pallas_call(
        far_kernel,
        out_shape=(
            jax.ShapeDtypeStruct((2, PROBES, WIDTH), F32),
            jax.ShapeDtypeStruct((4, 5 * QUARTER, 128), I16),
            jax.ShapeDtypeStruct((4, PROBES, 128), I16),
        ),
        in_specs=[VMEM] * 5,
        out_specs=(VMEM, VMEM, VMEM),
        scratch_shapes=[pltpu.VMEM((2, PROBES, LANES), F32)],
        compiler_params=ROOM,
        cost_estimate=cost(10**9, 2 * 10**6),
        name="far",
    )(far, cross, facts, held, right)
    line = exchange(line, "y")
    deep = pl.pallas_call(
        line_kernel,
        out_shape=jax.ShapeDtypeStruct((32, QUARTER, 128), I16),
        in_specs=[VMEM],
        out_specs=VMEM,
        compiler_params=ROOM,
        cost_estimate=cost(10**5, 3 * 10**5),
        name="line",
    )(line)
    deep = exchange(deep, ("x", "z"))
    wide = pl.pallas_call(
        depth_kernel,
        out_shape=jax.ShapeDtypeStruct((8, PROBES + 5 * QUARTER, 128), I16),
        in_specs=[VMEM, VMEM],
        out_specs=VMEM,
        compiler_params=ROOM,
        cost_estimate=cost(10**5, 5 * 10**5),
        name="depth",
    )(deep, low)
    wide = exchange(wide, ("y", "c"))
    return pl.pallas_call(
        final_kernel,
        out_shape=jax.ShapeDtypeStruct((2, PROBES, WIDTH), F32),
        in_specs=[VMEM] * 4,
        out_specs=VMEM,
        scratch_shapes=[pltpu.VMEM((LEVELS * PROBES, 2 * RANK), F32)],
        compiler_params=ROOM,
        cost_estimate=cost(10**9, 3 * 10**6),
        name="final",
    )(wide, factor, coupling, diagonal)


def solution(mesh):
    fine = Mesh(mesh.devices.reshape(4, 8, 4, 2, 2), ("x", "z", "y", "h", "c"))
    every = ("x", "z", "y", "h", "c")
    in_specs = (P(None, every), P(None, every), P(), P(), P(), P())
    return jax.shard_map(
        on_device, mesh=fine, in_specs=in_specs, out_specs=P(None, None, every), check_vma=False
    )
```

```python
import math

import jax
import jax.numpy as jnp
from jax import lax
from jax.experimental import pallas as pl
from jax.experimental.pallas import tpu as pltpu
from jax.sharding import Mesh, PartitionSpec as P


LEVELS = 7
PROBES = 64
RANK = 128
HALF = RANK // 2
QUARTER = PROBES // 4
SPAN = 128
WIDTH = 512
TRANSFER = 80
LANES = 1024
BLOCK = 256
KEPT = WIDTH + RANK
ALL_SPANS = ((0, 256), (256, 512), (512, 768), (768, 1024))
LATE_SPANS = ((0, 256), (256, 512), (512, 640))
ROOT = math.sqrt(math.log2(math.e))
TWO_LN2 = 2.0 * math.log(2.0)
F32 = jnp.float32
BF16 = jnp.bfloat16
I16 = jnp.int16
FINE = 2.0**26
OCTAVES = 44.0
VMEM = pl.BlockSpec(memory_space=pltpu.VMEM)
ROOM = pltpu.CompilerParams(vmem_limit_bytes=16 * 2**20)
SMEM = pl.BlockSpec(memory_space=pltpu.SMEM)


def cost(flops, moved):
    return pl.CostEstimate(flops=flops, bytes_accessed=moved, transcendentals=0)


def split3(value):
    first = value.astype(BF16).astype(F32)
    rest = value - first
    second = rest.astype(BF16).astype(F32)
    third = (rest - second).astype(BF16).astype(F32)
    return first, second, third


def norms(value):
    return -0.5 * jnp.sum(value * value, axis=0, keepdims=True)


def stacked(parts, rows):
    width = parts[0].shape[1]
    index = lax.broadcasted_iota(jnp.int32, (8, width), 0)
    held = jnp.zeros((8, width), F32)
    for k, row in enumerate(rows):
        held = jnp.where(index == k, row, held)
    zeros = jnp.zeros((SPAN - 56, width), F32)
    return jnp.concatenate(list(parts) + [held, zeros], axis=0)


def left_form(value, extra):
    one, two, three = split3(value)
    n1, n2, n3 = split3(norms(value) + extra)
    return stacked((one, one, two, one, three, two), (1.0, 1.0, 1.0, n1, n2, n3))


def right_form(value, extra):
    one, two, three = split3(value)
    n1, n2, n3 = split3(norms(value) + extra)
    return stacked((one, two, one, three, one, two), (n1, n2, n3, 1.0, 1.0, 1.0))


def points_of(message, inverse):
    high = message[PROBES : PROBES + 8, :].astype(F32)
    low = message[PROBES + 8 : PROBES + 16, :].astype(F32)
    return ((high * 64.0 + low) * (1.0 / 4096.0) - 0.5) * inverse


def kernel_pair(exponent, log_strength):
    kern = jnp.exp2(exponent)
    return kern, kern * (TWO_LN2 * log_strength - TWO_LN2 * exponent)


def halved(value):
    top = value.astype(BF16)
    return top, (value - top.astype(F32)).astype(BF16)


def encode(value):
    grade = jnp.log(1.0 + jnp.abs(value) * FINE) * (32767.0 / (OCTAVES * math.log(2.0))) + 0.5
    return jnp.where(value < 0.0, -grade, grade).astype(jnp.int32).astype(jnp.int16)


def decode(code):
    grade = code.astype(jnp.int32).astype(F32)
    size = (jnp.exp2(jnp.abs(grade) * (OCTAVES / 32767.0)) - 1.0) * (1.0 / FINE)
    return jnp.where(grade < 0.0, -size, size)


def prepare_kernel(
    coords_ref, probes_ref, marks_ref, scales_ref, strength_ref,
    out_ref, picked_ref, facts_ref, coords_buf, probes_buf, scales_buf, sem,
):
    row = lax.axis_index("x") * 32 + lax.axis_index("z") * 4 + lax.axis_index("y")
    copies = [
        pltpu.make_async_copy(probes_ref, probes_buf, sem.at[0]),
        pltpu.make_async_copy(coords_ref, coords_buf, sem.at[1]),
        pltpu.make_async_copy(scales_ref, scales_buf, sem.at[2 + LEVELS]),
    ]
    for level in range(LEVELS):
        node = 2 ** (LEVELS - level) - 2 + jnp.right_shift(row, level)
        copies.append(pltpu.make_async_copy(marks_ref.at[node], picked_ref.at[level], sem.at[2 + level]))
    for copy in copies:
        copy.start()
    for copy in copies:
        copy.wait()
    coords = coords_buf[...]
    high = jnp.right_shift(coords, 6)
    low = coords - high * 64
    out_ref[0:PROBES, :] = probes_buf[...].astype(BF16)
    both = jnp.concatenate([high.astype(F32), low.astype(F32)], axis=0)
    out_ref[PROBES:TRANSFER, :] = both.astype(BF16)
    place = lax.broadcasted_iota(jnp.int32, (8, 128), 0)
    held = jnp.full((8, 128), scales_buf[0], F32)
    for k in range(1, 8):
        held = jnp.where(place == k, scales_buf[k], held)
    facts_ref[0:8, :] = ROOT / held
    facts_ref[8:16, :] = jnp.log(jnp.full((8, 128), strength_ref[0], F32)) * math.log2(math.e)


def accumulate(message_ref, facts_ref, right_ref, sums, spans, fresh):
    message = message_ref[...]
    inverse = facts_ref[0:8, 0:1]
    log_strength = facts_ref[8:9, 0:1]
    left = left_form(points_of(message, inverse), 0.0).T.astype(BF16)
    for block in range(WIDTH // BLOCK):
        rows = left[block * BLOCK : (block + 1) * BLOCK, :]
        signs = message[0:PROBES, block * BLOCK : (block + 1) * BLOCK]
        for start, stop in spans:
            exponent = jnp.dot(rows, right_ref[:, start:stop], preferred_element_type=F32)
            for which, value in enumerate(kernel_pair(exponent, log_strength)):
                top, rest = halved(value)
                total = jnp.dot(signs, top, preferred_element_type=F32)
                if start >= WIDTH:
                    total = total + jnp.dot(signs, rest, preferred_element_type=F32)
                if fresh and block == 0:
                    sums[which, :, start:stop] = total
                else:
                    sums[which, :, start:stop] += total


def unit_of(sums, level):
    at = WIDTH + level * HALF
    return encode(jnp.concatenate([sums[0, :, at : at + HALF], sums[1, :, at : at + HALF]], axis=1))


def own_kernel(own_ref, facts_ref, marks_ref, held_ref, right_ref, factor_ref):
    core = lax.axis_index("c")
    inverse = facts_ref[0:8, 0:1]
    log_strength = facts_ref[8:9, 0:1]
    own = points_of(own_ref[...], inverse)
    marks = [(marks_ref[level] - 0.5) * inverse for level in range(LEVELS)]
    halves = [jnp.where(core == 0, mark[:, :HALF], mark[:, HALF:]) for mark in marks]
    halves.append(jnp.zeros((8, HALF), F32))
    columns = jnp.concatenate([own] + halves, axis=1)
    right_ref[...] = right_form(columns, log_strength).astype(BF16)
    accumulate(own_ref, facts_ref, right_ref, held_ref, ALL_SPANS, True)
    own_right = right_ref[:, :WIDTH]
    for level in range(LEVELS):
        turned = left_form(marks[level], 0.0).T.astype(BF16)
        exponent = jnp.dot(turned, own_right, preferred_element_type=F32)
        kern, slope = kernel_pair(exponent, log_strength)
        factor_ref[0, level * RANK : (level + 1) * RANK, :] = kern.astype(BF16)
        factor_ref[1, level * RANK : (level + 1) * RANK, :] = slope.astype(BF16)


def near_kernel(other_ref, facts_ref, held_ref, right_ref, kept_ref, plane_ref, sums):
    x = lax.axis_index("x")
    sums[...] = held_ref[...]
    accumulate(other_ref, facts_ref, right_ref, sums, ALL_SPANS, False)
    kept_ref[...] = sums[:, :, :KEPT]
    units = [unit_of(sums, level) for level in range(2, LEVELS)]
    blank = jnp.zeros((2 * QUARTER, 128), I16)
    for at in range(4):
        part = slice(at * QUARTER, (at + 1) * QUARTER)
        plane_ref[x * 4 + at] = jnp.concatenate([unit[part] for unit in units[:3]], axis=0)
        for apart, which in ((1, 3), (2, 4), (3, 4)):
            plane_ref[jnp.bitwise_xor(x, apart) * 4 + at] = jnp.concatenate([units[which][part], blank], axis=0)


def plane_kernel(got_ref, out_ref):
    x = lax.axis_index("x")
    z = lax.axis_index("z")

    def total(apart, rows):
        start = jnp.bitwise_xor(x, apart) * 4
        return added([decode(got_ref[start + at, rows]) for at in range(4)])

    low = slice(0, QUARTER)
    chosen = [jnp.zeros((QUARTER, 128), I16)]
    chosen += [encode(total(0, slice(at * QUARTER, (at + 1) * QUARTER))) for at in range(3)]
    five = encode(total(1, low))
    six = encode(total(2, low) + total(3, low))
    for apart in range(8):
        piece = jnp.concatenate([chosen[apart.bit_length()], five, six], axis=0)
        for half in range(2):
            out_ref[half * 8 + jnp.bitwise_xor(z, apart)] = piece


def added(parts):
    while len(parts) > 1:
        parts = [a + b for a, b in zip(parts[::2], parts[1::2])]
    return parts[0]


def late_kernel(
    far_ref, cross_ref, facts_ref, kept_ref, right_ref, got_ref,
    diagonal_ref, out_ref, sums,
):
    y = lax.axis_index("y")
    z = lax.axis_index("z")
    sums[...] = kept_ref[...]
    accumulate(far_ref, facts_ref, right_ref, sums, LATE_SPANS, False)
    accumulate(cross_ref, facts_ref, right_ref, sums, LATE_SPANS, False)
    diagonal_ref[...] = sums[:, :, :WIDTH]

    def total(aparts, start):
        return added([
            decode(got_ref[half * 8 + jnp.bitwise_xor(z, apart), start : start + QUARTER])
            for half in range(2) for apart in aparts
        ])

    found = [
        total((1,), 0),
        total((2, 3), 0),
        total((4, 5, 6, 7), 0),
        total(range(8), QUARTER),
        total(range(8), 2 * QUARTER),
    ]
    packed = encode(jnp.concatenate(found, axis=0))
    for core in range(2):
        out_ref[2 * y + core, 0:PROBES] = jnp.zeros((PROBES, 128), I16)
    units = [unit_of(sums, level) for level in range(2)]
    for apart, level in ((1, 0), (2, 1), (3, 1)):
        for core in range(2):
            out_ref[2 * jnp.bitwise_xor(y, apart) + core, 0:PROBES] = units[level]
    for place in range(8):
        out_ref[place, PROBES:] = packed


def final_kernel(got_ref, factor_ref, coupling_ref, diagonal_ref, out_ref, sibling):
    y = lax.axis_index("y")
    row = lax.axis_index("x") * 32 + lax.axis_index("z") * 4 + y
    for core in range(2):
        lanes = slice(core * 128, core * 128 + 128)
        sibling[0:PROBES, lanes] = decode(got_ref[jnp.bitwise_xor(y, 1) * 2 + core, 0:PROBES])
        pair = decode(got_ref[jnp.bitwise_xor(y, 2) * 2 + core, 0:PROBES])
        pair = pair + decode(got_ref[jnp.bitwise_xor(y, 3) * 2 + core, 0:PROBES])
        sibling[PROBES : 2 * PROBES, lanes] = pair
        for level in range(2, LEVELS):
            for at in range(4):
                start = level * PROBES + at * QUARTER
                source = PROBES + (level - 2) * QUARTER
                sibling[start : start + QUARTER, lanes] = decode(got_ref[2 * at + core, source : source + QUARTER])
    coupling = coupling_ref[...]
    blank = jnp.zeros((HALF, RANK), F32)

    def spread(core_matrix):
        rows = []
        for core in range(2):
            part = core_matrix[core * HALF : (core + 1) * HALF, :]
            rows.append(jnp.concatenate([part, blank], axis=1))
            rows.append(jnp.concatenate([blank, part], axis=1))
        whole = jnp.concatenate(rows, axis=0)
        return halved(whole)

    values, remainders = halved(sibling[...])
    results = []
    for matrix in (coupling.T, coupling):
        top, rest = spread(matrix)
        results.append(
            jnp.dot(values, top, preferred_element_type=F32)
            + jnp.dot(values, rest, preferred_element_type=F32)
            + jnp.dot(remainders, top, preferred_element_type=F32)
        )
    heads = []
    for level in range(LEVELS):
        rows = slice(level * PROBES, (level + 1) * PROBES)
        left = jnp.bitwise_and(jnp.right_shift(row, level), 1) == 0
        heads.append(jnp.where(left, results[0][rows], results[1][rows]))
    firsts = jnp.concatenate([head[:, :RANK] for head in heads], axis=1)
    seconds = jnp.concatenate([head[:, RANK:] for head in heads], axis=1)
    top, rest = halved(jnp.concatenate([firsts, seconds], axis=0))
    stack = jnp.concatenate([top, rest], axis=0)
    on_kern = jnp.dot(stack, factor_ref[0], preferred_element_type=F32)
    pair = jnp.concatenate([top[:PROBES], rest[:PROBES]], axis=0)
    on_slope = jnp.dot(pair, factor_ref[1], preferred_element_type=F32)
    on_kern = on_kern[: 2 * PROBES] + on_kern[2 * PROBES :]
    on_slope = on_slope[:PROBES] + on_slope[PROBES:]
    out_ref[0] = diagonal_ref[0] + on_kern[:PROBES]
    out_ref[1] = diagonal_ref[1] + (on_kern[PROBES:] + on_slope)


def stay(array):
    return pltpu.with_memory_space_constraint(array, pltpu.HBM)


def swap(value, axis):
    return lax.ppermute(value, axis, [(0, 1), (1, 0)])


def exchange(value, axes):
    return lax.all_to_all(value, axes, 0, 0, tiled=True)


def on_device(coords, probes, lengthscales, amplitude, landmarks, coupling):
    message, marks, facts = pl.pallas_call(
        prepare_kernel,
        out_shape=(
            jax.ShapeDtypeStruct((TRANSFER, WIDTH), BF16),
            jax.ShapeDtypeStruct((LEVELS, 8, RANK), F32),
            jax.ShapeDtypeStruct((16, 128), F32),
        ),
        in_specs=[pl.BlockSpec(memory_space=pltpu.HBM)] * 4 + [SMEM],
        out_specs=(VMEM, VMEM, VMEM),
        scratch_shapes=[
            pltpu.VMEM((8, WIDTH), jnp.int32),
            pltpu.VMEM((PROBES, WIDTH), F32),
            pltpu.SMEM((8,), F32),
            pltpu.SemaphoreType.DMA((3 + LEVELS,)),
        ],
        compiler_params=ROOM,
        cost_estimate=cost(10**5, 2 * 10**5),
        name="prepare",
    )(*[stay(array) for array in (coords, probes, landmarks, lengthscales)], amplitude)
    far = swap(message, "h")
    cross = lax.ppermute(message, ("h", "c"), [(0, 3), (1, 2), (2, 1), (3, 0)])
    other = swap(message, "c")
    held, right, factor = pl.pallas_call(
        own_kernel,
        out_shape=(
            jax.ShapeDtypeStruct((2, PROBES, LANES), F32),
            jax.ShapeDtypeStruct((SPAN, LANES), BF16),
            jax.ShapeDtypeStruct((2, LEVELS * RANK, WIDTH), BF16),
        ),
        in_specs=[VMEM] * 3,
        out_specs=(VMEM, VMEM, VMEM),
        compiler_params=ROOM,
        cost_estimate=cost(2 * 10**9, 3 * 10**6),
        name="own",
    )(message, facts, marks)
    kept, plane = pl.pallas_call(
        near_kernel,
        out_shape=(
            jax.ShapeDtypeStruct((2, PROBES, KEPT), F32),
            jax.ShapeDtypeStruct((16, 3 * QUARTER, 128), I16),
        ),
        in_specs=[VMEM] * 4,
        out_specs=(VMEM, VMEM),
        scratch_shapes=[pltpu.VMEM((2, PROBES, LANES), F32)],
        compiler_params=ROOM,
        cost_estimate=cost(10**9, 2 * 10**6),
        name="near",
    )(other, facts, held, right)
    plane = exchange(plane, ("x", "y"))
    deep = pl.pallas_call(
        plane_kernel,
        out_shape=jax.ShapeDtypeStruct((16, 3 * QUARTER, 128), I16),
        in_specs=[VMEM],
        out_specs=VMEM,
        compiler_params=ROOM,
        cost_estimate=cost(10**5, 3 * 10**5),
        name="plane",
    )(plane)
    deep = exchange(deep, ("h", "z"))
    diagonal, wide = pl.pallas_call(
        late_kernel,
        out_shape=(
            jax.ShapeDtypeStruct((2, PROBES, WIDTH), F32),
            jax.ShapeDtypeStruct((8, PROBES + 5 * QUARTER, 128), I16),
        ),
        in_specs=[VMEM] * 6,
        out_specs=(VMEM, VMEM),
        scratch_shapes=[pltpu.VMEM((2, PROBES, KEPT), F32)],
        compiler_params=ROOM,
        cost_estimate=cost(10**9, 2 * 10**6),
        name="late",
    )(far, cross, facts, kept, right, deep)
    wide = exchange(wide, ("y", "c"))
    return pl.pallas_call(
        final_kernel,
        out_shape=jax.ShapeDtypeStruct((2, PROBES, WIDTH), F32),
        in_specs=[VMEM] * 4,
        out_specs=VMEM,
        scratch_shapes=[pltpu.VMEM((LEVELS * PROBES, 2 * RANK), F32)],
        compiler_params=ROOM,
        cost_estimate=cost(10**9, 3 * 10**6),
        name="final",
    )(wide, factor, coupling, diagonal)


def solution(mesh):
    fine = Mesh(mesh.devices.reshape(4, 8, 4, 2, 2), ("x", "z", "y", "h", "c"))
    every = ("x", "z", "y", "h", "c")
    in_specs = (P(None, every), P(None, every), P(), P(), P(), P())
    return jax.shard_map(
        on_device, mesh=fine, in_specs=in_specs, out_specs=P(None, None, every), check_vma=False
    )
```

```python
import math

import jax
import jax.numpy as jnp
from jax import lax
from jax.experimental import pallas as pl
from jax.experimental.pallas import tpu as pltpu
from jax.sharding import Mesh, PartitionSpec as P


LEVELS = 7
PROBES = 64
RANK = 128
HALF = RANK // 2
QUARTER = PROBES // 4
SPAN = 128
WIDTH = 512
TRANSFER = 80
LANES = 1024
BLOCK = 256
ROOT = math.sqrt(math.log2(math.e))
TWO_LN2 = 2.0 * math.log(2.0)
F32 = jnp.float32
BF16 = jnp.bfloat16
I16 = jnp.int16
FINE = 2.0**26
OCTAVES = 44.0
VMEM = pl.BlockSpec(memory_space=pltpu.VMEM)
ROOM = pltpu.CompilerParams(vmem_limit_bytes=16 * 2**20)
SMEM = pl.BlockSpec(memory_space=pltpu.SMEM)


def cost(flops, moved):
    return pl.CostEstimate(flops=flops, bytes_accessed=moved, transcendentals=0)


def row_index():
    z = lax.axis_index("zh") * 2 + lax.axis_index("zl")
    return lax.axis_index("x") * 32 + z * 4 + lax.axis_index("y")


def split3(value):
    first = value.astype(BF16).astype(F32)
    rest = value - first
    second = rest.astype(BF16).astype(F32)
    third = (rest - second).astype(BF16).astype(F32)
    return first, second, third


def norms(value):
    return -0.5 * jnp.sum(value * value, axis=0, keepdims=True)


def stacked(parts, rows):
    width = parts[0].shape[1]
    index = lax.broadcasted_iota(jnp.int32, (8, width), 0)
    held = jnp.zeros((8, width), F32)
    for k, row in enumerate(rows):
        held = jnp.where(index == k, row, held)
    zeros = jnp.zeros((SPAN - 56, width), F32)
    return jnp.concatenate(list(parts) + [held, zeros], axis=0)


def left_form(value, extra):
    one, two, three = split3(value)
    n1, n2, n3 = split3(norms(value) + extra)
    return stacked((one, one, two, one, three, two), (1.0, 1.0, 1.0, n1, n2, n3))


def right_form(value, extra):
    one, two, three = split3(value)
    n1, n2, n3 = split3(norms(value) + extra)
    return stacked((one, two, one, three, one, two), (n1, n2, n3, 1.0, 1.0, 1.0))


def points_of(message, inverse):
    high = message[PROBES : PROBES + 8, :].astype(F32)
    low = message[PROBES + 8 : PROBES + 16, :].astype(F32)
    return ((high * 64.0 + low) * (1.0 / 4096.0) - 0.5) * inverse


def kernel_pair(exponent, log_strength):
    kern = jnp.exp2(exponent)
    return kern, kern * (TWO_LN2 * log_strength - TWO_LN2 * exponent)


def halved(value):
    top = value.astype(BF16)
    return top, (value - top.astype(F32)).astype(BF16)


def encode(value):
    grade = jnp.log(1.0 + jnp.abs(value) * FINE) * (32767.0 / (OCTAVES * math.log(2.0))) + 0.5
    return jnp.where(value < 0.0, -grade, grade).astype(jnp.int32).astype(jnp.int16)


def decode(code):
    grade = code.astype(jnp.int32).astype(F32)
    size = (jnp.exp2(jnp.abs(grade) * (OCTAVES / 32767.0)) - 1.0) * (1.0 / FINE)
    return jnp.where(grade < 0.0, -size, size)


def prepare_kernel(
    coords_ref, probes_ref, marks_ref, scales_ref, strength_ref,
    out_ref, picked_ref, facts_ref, coords_buf, probes_buf, scales_buf, sem,
):
    row = row_index()
    copies = [
        pltpu.make_async_copy(probes_ref, probes_buf, sem.at[0]),
        pltpu.make_async_copy(coords_ref, coords_buf, sem.at[1]),
        pltpu.make_async_copy(scales_ref, scales_buf, sem.at[2 + LEVELS]),
    ]
    for level in range(LEVELS):
        node = 2 ** (LEVELS - level) - 2 + jnp.right_shift(row, level)
        copies.append(pltpu.make_async_copy(marks_ref.at[node], picked_ref.at[level], sem.at[2 + level]))
    for copy in copies:
        copy.start()
    for copy in copies:
        copy.wait()
    coords = coords_buf[...]
    high = jnp.right_shift(coords, 6)
    low = coords - high * 64
    out_ref[0:PROBES, :] = probes_buf[...].astype(BF16)
    both = jnp.concatenate([high.astype(F32), low.astype(F32)], axis=0)
    out_ref[PROBES:TRANSFER, :] = both.astype(BF16)
    place = lax.broadcasted_iota(jnp.int32, (8, 128), 0)
    held = jnp.full((8, 128), scales_buf[0], F32)
    for k in range(1, 8):
        held = jnp.where(place == k, scales_buf[k], held)
    facts_ref[0:8, :] = ROOT / held
    facts_ref[8:16, :] = jnp.log(jnp.full((8, 128), strength_ref[0], F32)) * math.log2(math.e)


def accumulate(message_ref, inverse, right, log_strength, held_k, held_s, fresh):
    message = message_ref[...]
    left = left_form(points_of(message, inverse), 0.0).T.astype(BF16)
    for block in range(WIDTH // BLOCK):
        rows = left[block * BLOCK : (block + 1) * BLOCK, :]
        signs = message[0:PROBES, block * BLOCK : (block + 1) * BLOCK]
        for at in range(0, LANES, BLOCK):
            exponent = jnp.dot(rows, right[:, at : at + BLOCK], preferred_element_type=F32)
            kern, slope = kernel_pair(exponent, log_strength)
            add_k = jnp.dot(signs, kern.astype(BF16), preferred_element_type=F32)
            add_s = jnp.dot(signs, slope.astype(BF16), preferred_element_type=F32)
            if fresh and block == 0:
                held_k[:, at : at + BLOCK] = add_k
                held_s[:, at : at + BLOCK] = add_s
            else:
                held_k[:, at : at + BLOCK] += add_k
                held_s[:, at : at + BLOCK] += add_s


def near_kernel(
    own_ref, other_ref, facts_ref, marks_ref,
    held_ref, right_ref, factor_ref,
):
    core = lax.axis_index("c")
    inverse = facts_ref[0:8, 0:1]
    log_strength = facts_ref[8:9, 0:1]
    own = points_of(own_ref[...], inverse)
    marks = [(marks_ref[level] - 0.5) * inverse for level in range(LEVELS)]
    halves = [jnp.where(core == 0, mark[:, :HALF], mark[:, HALF:]) for mark in marks]
    halves.append(jnp.zeros((8, HALF), F32))
    columns = jnp.concatenate([own] + halves, axis=1)
    right = right_form(columns, log_strength).astype(BF16)
    right_ref[...] = right
    accumulate(own_ref, inverse, right, log_strength, held_ref.at[0], held_ref.at[1], True)
    accumulate(other_ref, inverse, right, log_strength, held_ref.at[0], held_ref.at[1], False)
    own_right = right[:, :WIDTH]
    for level in range(LEVELS):
        turned = left_form(marks[level], 0.0).T.astype(BF16)
        exponent = jnp.dot(turned, own_right, preferred_element_type=F32)
        kern, slope = kernel_pair(exponent, log_strength)
        for which, value in enumerate((kern, slope)):
            top, rest = halved(value)
            factor_ref[2 * which, level * RANK : (level + 1) * RANK, :] = top
            factor_ref[2 * which + 1, level * RANK : (level + 1) * RANK, :] = rest


def far_kernel(far_ref, facts_ref, held_ref, right_ref, out_ref):
    inverse = facts_ref[0:8, 0:1]
    log_strength = facts_ref[8:9, 0:1]
    out_ref[...] = held_ref[...]
    accumulate(far_ref, inverse, right_ref[...], log_strength, out_ref.at[0], out_ref.at[1], False)


def cross_kernel(
    cross_ref, facts_ref, held_ref, right_ref,
    diagonal_ref, line_ref, low_ref, sums,
):
    y = lax.axis_index("y")
    zl = lax.axis_index("zl")
    inverse = facts_ref[0:8, 0:1]
    log_strength = facts_ref[8:9, 0:1]
    sums[...] = held_ref[...]
    accumulate(cross_ref, inverse, right_ref[...], log_strength, sums.at[0], sums.at[1], False)
    diagonal_ref[...] = sums[:, :, :WIDTH]
    units = []
    for level in range(LEVELS):
        at = WIDTH + level * HALF
        pair = [sums[0, :, at : at + HALF], sums[1, :, at : at + HALF]]
        units.append(encode(jnp.concatenate(pair, axis=1)))
    blank = jnp.zeros((QUARTER, 128), I16)
    for at in range(4):
        part = slice(at * QUARTER, (at + 1) * QUARTER)
        higher = [units[level][part] for level in range(3, LEVELS)]
        line_ref[zl * 4 + at] = jnp.concatenate([blank] + higher, axis=0)
        line_ref[(1 - zl) * 4 + at] = jnp.concatenate([units[2][part]] + higher, axis=0)
    low_ref[y] = jnp.zeros((PROBES, 128), I16)
    for apart, level in ((1, 0), (2, 1), (3, 1)):
        low_ref[jnp.bitwise_xor(y, apart)] = units[level]


def added(parts):
    while len(parts) > 1:
        parts = [a + b for a, b in zip(parts[::2], parts[1::2])]
    return parts[0]


def line_kernel(got_ref, out_ref, two_ref):
    x = lax.axis_index("x")
    zh = lax.axis_index("zh")
    zl = lax.axis_index("zl")
    two_ref[...] = encode(added([decode(got_ref[(1 - zl) * 4 + at, 0:QUARTER]) for at in range(4)]))
    packed = encode(added([decode(got_ref[at, QUARTER:]) for at in range(8)]))
    parts = [packed[at * QUARTER : (at + 1) * QUARTER] for at in range(4)]
    for aside in range(4):
        for apart in range(4):
            place = jnp.bitwise_xor(x, aside) * 4 + jnp.bitwise_xor(zh, apart)
            if aside > 0:
                out_ref[place] = parts[1 + aside.bit_length()]
            elif apart > 0:
                out_ref[place] = parts[apart.bit_length() - 1]
            else:
                out_ref[place] = jnp.zeros((QUARTER, 128), I16)


def depth_kernel(got_ref, two_ref, low_ref, out_ref):
    x = lax.axis_index("x")
    zh = lax.axis_index("zh")

    def total(asides, aparts):
        return added([
            decode(got_ref[jnp.bitwise_xor(x, aside) * 4 + jnp.bitwise_xor(zh, apart)])
            for aside in asides for apart in aparts
        ])

    found = [total((0,), (1,)), total((0,), (2, 3)), total((1,), range(4)), total((2, 3), range(4))]
    packed = jnp.concatenate([two_ref[...], encode(jnp.concatenate(found, axis=0))], axis=0)
    for at in range(4):
        for core in range(2):
            out_ref[2 * at + core, 0:PROBES] = low_ref[at]
            out_ref[2 * at + core, PROBES:] = packed


def final_kernel(got_ref, factor_ref, coupling_ref, diagonal_ref, out_ref, sibling):
    y = lax.axis_index("y")
    row = row_index()
    for core in range(2):
        lanes = slice(core * 128, core * 128 + 128)
        sibling[0:PROBES, lanes] = decode(got_ref[jnp.bitwise_xor(y, 1) * 2 + core, 0:PROBES])
        pair = decode(got_ref[jnp.bitwise_xor(y, 2) * 2 + core, 0:PROBES])
        pair = pair + decode(got_ref[jnp.bitwise_xor(y, 3) * 2 + core, 0:PROBES])
        sibling[PROBES : 2 * PROBES, lanes] = pair
        for level in range(2, LEVELS):
            for at in range(4):
                start = level * PROBES + at * QUARTER
                source = PROBES + (level - 2) * QUARTER
                sibling[start : start + QUARTER, lanes] = decode(got_ref[2 * at + core, source : source + QUARTER])
    coupling = coupling_ref[...]
    blank = jnp.zeros((HALF, RANK), F32)

    def spread(core_matrix):
        rows = []
        for core in range(2):
            part = core_matrix[core * HALF : (core + 1) * HALF, :]
            rows.append(jnp.concatenate([part, blank], axis=1))
            rows.append(jnp.concatenate([blank, part], axis=1))
        whole = jnp.concatenate(rows, axis=0)
        return halved(whole)

    values, remainders = halved(sibling[...])
    results = []
    for matrix in (coupling.T, coupling):
        top, rest = spread(matrix)
        results.append(
            jnp.dot(values, top, preferred_element_type=F32)
            + jnp.dot(values, rest, preferred_element_type=F32)
            + jnp.dot(remainders, top, preferred_element_type=F32)
        )
    heads = []
    for level in range(LEVELS):
        rows = slice(level * PROBES, (level + 1) * PROBES)
        left = jnp.bitwise_and(jnp.right_shift(row, level), 1) == 0
        heads.append(jnp.where(left, results[0][rows], results[1][rows]))
    firsts = jnp.concatenate([head[:, :RANK] for head in heads], axis=1)
    seconds = jnp.concatenate([head[:, RANK:] for head in heads], axis=1)
    top, rest = halved(jnp.concatenate([firsts, seconds], axis=0))
    stack = jnp.concatenate([top, rest], axis=0)
    on_kern = jnp.dot(stack, factor_ref[0], preferred_element_type=F32)
    pair = jnp.concatenate([top[:PROBES], rest[:PROBES]], axis=0)
    on_slope = jnp.dot(pair, factor_ref[2], preferred_element_type=F32)
    on_kern = on_kern[: 2 * PROBES] + on_kern[2 * PROBES :] + jnp.dot(top, factor_ref[1], preferred_element_type=F32)
    on_slope = on_slope[:PROBES] + on_slope[PROBES:] + jnp.dot(top[:PROBES], factor_ref[3], preferred_element_type=F32)
    out_ref[0] = diagonal_ref[0] + on_kern[:PROBES]
    out_ref[1] = diagonal_ref[1] + (on_kern[PROBES:] + on_slope)


def stay(array):
    return pltpu.with_memory_space_constraint(array, pltpu.HBM)


def swap(value, axis):
    return lax.ppermute(value, axis, [(0, 1), (1, 0)])


def exchange(value, axes):
    return lax.all_to_all(value, axes, 0, 0, tiled=True)


def on_device(coords, probes, lengthscales, amplitude, landmarks, coupling):
    message, marks, facts = pl.pallas_call(
        prepare_kernel,
        out_shape=(
            jax.ShapeDtypeStruct((TRANSFER, WIDTH), BF16),
            jax.ShapeDtypeStruct((LEVELS, 8, RANK), F32),
            jax.ShapeDtypeStruct((16, 128), F32),
        ),
        in_specs=[pl.BlockSpec(memory_space=pltpu.HBM)] * 4 + [SMEM],
        out_specs=(VMEM, VMEM, VMEM),
        scratch_shapes=[
            pltpu.VMEM((8, WIDTH), jnp.int32),
            pltpu.VMEM((PROBES, WIDTH), F32),
            pltpu.SMEM((8,), F32),
            pltpu.SemaphoreType.DMA((3 + LEVELS,)),
        ],
        compiler_params=ROOM,
        cost_estimate=cost(10**5, 2 * 10**5),
        name="prepare",
    )(*[stay(array) for array in (coords, probes, landmarks, lengthscales)], amplitude)
    far = swap(message, "h")
    other = swap(message, "c")
    held, right, factor = pl.pallas_call(
        near_kernel,
        out_shape=(
            jax.ShapeDtypeStruct((2, PROBES, LANES), F32),
            jax.ShapeDtypeStruct((SPAN, LANES), BF16),
            jax.ShapeDtypeStruct((4, LEVELS * RANK, WIDTH), BF16),
        ),
        in_specs=[VMEM] * 4,
        out_specs=(VMEM, VMEM, VMEM),
        compiler_params=ROOM,
        cost_estimate=cost(2 * 10**9, 3 * 10**6),
        name="near",
    )(message, other, facts, marks)
    far, held, right = lax.optimization_barrier((far, held, right))
    cross = swap(far, "c")
    held = pl.pallas_call(
        far_kernel,
        out_shape=jax.ShapeDtypeStruct((2, PROBES, LANES), F32),
        in_specs=[VMEM] * 4,
        out_specs=VMEM,
        compiler_params=ROOM,
        cost_estimate=cost(10**9, 2 * 10**6),
        name="far",
    )(far, facts, held, right)
    diagonal, line, low = pl.pallas_call(
        cross_kernel,
        out_shape=(
            jax.ShapeDtypeStruct((2, PROBES, WIDTH), F32),
            jax.ShapeDtypeStruct((8, 5 * QUARTER, 128), I16),
            jax.ShapeDtypeStruct((4, PROBES, 128), I16),
        ),
        in_specs=[VMEM] * 4,
        out_specs=(VMEM, VMEM, VMEM),
        scratch_shapes=[pltpu.VMEM((2, PROBES, LANES), F32)],
        compiler_params=ROOM,
        cost_estimate=cost(10**9, 2 * 10**6),
        name="cross",
    )(cross, facts, held, right)
    line = exchange(line, ("zl", "y"))
    deep, two = pl.pallas_call(
        line_kernel,
        out_shape=(
            jax.ShapeDtypeStruct((16, QUARTER, 128), I16),
            jax.ShapeDtypeStruct((QUARTER, 128), I16),
        ),
        in_specs=[VMEM],
        out_specs=(VMEM, VMEM),
        compiler_params=ROOM,
        cost_estimate=cost(10**5, 3 * 10**5),
        name="line",
    )(line)
    deep = exchange(deep, ("x", "zh"))
    wide = pl.pallas_call(
        depth_kernel,
        out_shape=jax.ShapeDtypeStruct((8, PROBES + 5 * QUARTER, 128), I16),
        in_specs=[VMEM] * 3,
        out_specs=VMEM,
        compiler_params=ROOM,
        cost_estimate=cost(10**5, 5 * 10**5),
        name="depth",
    )(deep, two, low)
    wide = exchange(wide, ("y", "c"))
    return pl.pallas_call(
        final_kernel,
        out_shape=jax.ShapeDtypeStruct((2, PROBES, WIDTH), F32),
        in_specs=[VMEM] * 4,
        out_specs=VMEM,
        scratch_shapes=[pltpu.VMEM((LEVELS * PROBES, 2 * RANK), F32)],
        compiler_params=ROOM,
        cost_estimate=cost(10**9, 3 * 10**6),
        name="final",
    )(wide, factor, coupling, diagonal)


def solution(mesh):
    fine = Mesh(mesh.devices.reshape(4, 4, 2, 4, 2, 2), ("x", "zh", "zl", "y", "h", "c"))
    every = ("x", "zh", "zl", "y", "h", "c")
    in_specs = (P(None, every), P(None, every), P(), P(), P(), P())
    return jax.shard_map(
        on_device, mesh=fine, in_specs=in_specs, out_specs=P(None, None, every), check_vma=False
    )
```

```python
import math

import jax
import jax.numpy as jnp
from jax import lax
from jax.experimental import pallas as pl
from jax.experimental.pallas import tpu as pltpu
from jax.sharding import Mesh, PartitionSpec as P


LEVELS = 7
PROBES = 64
RANK = 128
HALF = RANK // 2
QUARTER = PROBES // 4
SPAN = 128
WIDTH = 512
TRANSFER = 80
LANES = 1024
BLOCK = 256
KEPT = WIDTH + RANK
ALL_SPANS = ((0, 256), (256, 512), (512, 768), (768, 1024))
LATE_SPANS = ((0, 256), (256, 512), (512, 640))
ROOT = math.sqrt(math.log2(math.e))
TWO_LN2 = 2.0 * math.log(2.0)
F32 = jnp.float32
BF16 = jnp.bfloat16
I16 = jnp.int16
FINE = 2.0**26
OCTAVES = 44.0
VMEM = pl.BlockSpec(memory_space=pltpu.VMEM)
ROOM = pltpu.CompilerParams(vmem_limit_bytes=16 * 2**20)
SMEM = pl.BlockSpec(memory_space=pltpu.SMEM)


def cost(flops, moved):
    return pl.CostEstimate(flops=flops, bytes_accessed=moved, transcendentals=0)


def row_index():
    z = lax.axis_index("zh") * 2 + lax.axis_index("zl")
    return lax.axis_index("x") * 32 + z * 4 + lax.axis_index("y")


def split3(value):
    first = value.astype(BF16).astype(F32)
    rest = value - first
    second = rest.astype(BF16).astype(F32)
    third = (rest - second).astype(BF16).astype(F32)
    return first, second, third


def norms(value):
    return -0.5 * jnp.sum(value * value, axis=0, keepdims=True)


def stacked(parts, rows):
    width = parts[0].shape[1]
    index = lax.broadcasted_iota(jnp.int32, (8, width), 0)
    held = jnp.zeros((8, width), F32)
    for k, row in enumerate(rows):
        held = jnp.where(index == k, row, held)
    zeros = jnp.zeros((SPAN - 56, width), F32)
    return jnp.concatenate(list(parts) + [held, zeros], axis=0)


def left_form(value, extra):
    one, two, three = split3(value)
    n1, n2, n3 = split3(norms(value) + extra)
    return stacked((one, one, two, one, three, two), (1.0, 1.0, 1.0, n1, n2, n3))


def right_form(value, extra):
    one, two, three = split3(value)
    n1, n2, n3 = split3(norms(value) + extra)
    return stacked((one, two, one, three, one, two), (n1, n2, n3, 1.0, 1.0, 1.0))


def points_of(message, inverse):
    high = message[PROBES : PROBES + 8, :].astype(F32)
    low = message[PROBES + 8 : PROBES + 16, :].astype(F32)
    return ((high * 64.0 + low) * (1.0 / 4096.0) - 0.5) * inverse


def kernel_pair(exponent, log_strength):
    kern = jnp.exp2(exponent)
    return kern, kern * (TWO_LN2 * log_strength - TWO_LN2 * exponent)


def halved(value):
    top = value.astype(BF16)
    return top, (value - top.astype(F32)).astype(BF16)


def encode(value):
    grade = jnp.log(1.0 + jnp.abs(value) * FINE) * (32767.0 / (OCTAVES * math.log(2.0))) + 0.5
    return jnp.where(value < 0.0, -grade, grade).astype(jnp.int32).astype(jnp.int16)


def decode(code):
    grade = code.astype(jnp.int32).astype(F32)
    size = (jnp.exp2(jnp.abs(grade) * (OCTAVES / 32767.0)) - 1.0) * (1.0 / FINE)
    return jnp.where(grade < 0.0, -size, size)


def prepare_kernel(
    coords_ref, probes_ref, marks_ref, scales_ref, strength_ref,
    out_ref, picked_ref, facts_ref, coords_buf, probes_buf, scales_buf, sem,
):
    row = row_index()
    copies = [
        pltpu.make_async_copy(probes_ref, probes_buf, sem.at[0]),
        pltpu.make_async_copy(coords_ref, coords_buf, sem.at[1]),
        pltpu.make_async_copy(scales_ref, scales_buf, sem.at[2 + LEVELS]),
    ]
    for level in range(LEVELS):
        node = 2 ** (LEVELS - level) - 2 + jnp.right_shift(row, level)
        copies.append(pltpu.make_async_copy(marks_ref.at[node], picked_ref.at[level], sem.at[2 + level]))
    for copy in copies:
        copy.start()
    for copy in copies:
        copy.wait()
    coords = coords_buf[...]
    high = jnp.right_shift(coords, 6)
    low = coords - high * 64
    out_ref[0:PROBES, :] = probes_buf[...].astype(BF16)
    both = jnp.concatenate([high.astype(F32), low.astype(F32)], axis=0)
    out_ref[PROBES:TRANSFER, :] = both.astype(BF16)
    place = lax.broadcasted_iota(jnp.int32, (8, 128), 0)
    held = jnp.full((8, 128), scales_buf[0], F32)
    for k in range(1, 8):
        held = jnp.where(place == k, scales_buf[k], held)
    facts_ref[0:8, :] = ROOT / held
    facts_ref[8:16, :] = jnp.log(jnp.full((8, 128), strength_ref[0], F32)) * math.log2(math.e)


def accumulate(message_ref, facts_ref, right_ref, sums, spans, fresh):
    message = message_ref[...]
    left = left_form(points_of(message, facts_ref[0:8, 0:1]), 0.0).T.astype(BF16)
    for block in range(WIDTH // BLOCK):
        rows = left[block * BLOCK : (block + 1) * BLOCK, :]
        signs = message[0:PROBES, block * BLOCK : (block + 1) * BLOCK]
        for start, stop in spans:
            exponent = jnp.dot(rows, right_ref[:, start:stop], preferred_element_type=F32)
            for which, value in enumerate(kernel_pair(exponent, facts_ref[8:9, 0:1])):
                top, rest = halved(value)
                total = jnp.dot(signs, top, preferred_element_type=F32)
                if start >= WIDTH:
                    total = total + jnp.dot(signs, rest, preferred_element_type=F32)
                if fresh and block == 0:
                    sums[which, :, start:stop] = total
                else:
                    sums[which, :, start:stop] += total


def unit_of(sums, level):
    at = WIDTH + level * HALF
    return encode(jnp.concatenate([sums[0, :, at : at + HALF], sums[1, :, at : at + HALF]], axis=1))


def own_kernel(own_ref, facts_ref, marks_ref, held_ref, right_ref):
    core = lax.axis_index("c")
    inverse = facts_ref[0:8, 0:1]
    own = points_of(own_ref[...], inverse)
    halves = []
    for level in range(LEVELS):
        mark = (marks_ref[level] - 0.5) * inverse
        halves.append(jnp.where(core == 0, mark[:, :HALF], mark[:, HALF:]))
    halves.append(jnp.zeros((8, HALF), F32))
    columns = jnp.concatenate([own] + halves, axis=1)
    right_ref[...] = right_form(columns, facts_ref[8:9, 0:1]).astype(BF16)
    accumulate(own_ref, facts_ref, right_ref, held_ref, ALL_SPANS, True)


def factor_kernel(facts_ref, marks_ref, right_ref, factor_ref):
    inverse = facts_ref[0:8, 0:1]
    right = right_ref[:, :WIDTH]
    for level in range(LEVELS):
        turned = left_form((marks_ref[level] - 0.5) * inverse, 0.0).T.astype(BF16)
        exponent = jnp.dot(turned, right, preferred_element_type=F32)
        for which, value in enumerate(kernel_pair(exponent, facts_ref[8:9, 0:1])):
            factor_ref[which, level * RANK : (level + 1) * RANK, :] = value.astype(BF16)


def near_kernel(other_ref, facts_ref, held_ref, right_ref, kept_ref, line_ref, sums):
    zl = lax.axis_index("zl")
    sums[...] = held_ref[...]
    accumulate(other_ref, facts_ref, right_ref, sums, ALL_SPANS, False)
    kept_ref[...] = sums[:, :, :KEPT]
    units = [unit_of(sums, level) for level in range(2, LEVELS)]
    blank = jnp.zeros((QUARTER, 128), I16)
    for at in range(4):
        part = slice(at * QUARTER, (at + 1) * QUARTER)
        higher = [unit[part] for unit in units[1:]]
        line_ref[zl * 4 + at] = jnp.concatenate([blank] + higher, axis=0)
        line_ref[(1 - zl) * 4 + at] = jnp.concatenate([units[0][part]] + higher, axis=0)


def added(parts):
    while len(parts) > 1:
        parts = [a + b for a, b in zip(parts[::2], parts[1::2])]
    return parts[0]


def line_kernel(got_ref, out_ref):
    x = lax.axis_index("x")
    zh = lax.axis_index("zh")
    zl = lax.axis_index("zl")
    two = encode(added([decode(got_ref[(1 - zl) * 4 + at, 0:QUARTER]) for at in range(4)]))
    packed = encode(added([decode(got_ref[at, QUARTER:]) for at in range(8)]))
    parts = [packed[at * QUARTER : (at + 1) * QUARTER] for at in range(4)]
    for aside in range(4):
        for apart in range(4):
            place = jnp.bitwise_xor(x, aside) * 8 + jnp.bitwise_xor(zh, apart) * 2
            if aside > 0:
                piece = parts[1 + aside.bit_length()]
            elif apart > 0:
                piece = parts[apart.bit_length() - 1]
            else:
                piece = two
            for half in range(2):
                out_ref[place + half] = piece


def far_kernel(far_ref, facts_ref, kept_ref, right_ref, out_ref):
    out_ref[...] = kept_ref[...]
    accumulate(far_ref, facts_ref, right_ref, out_ref, LATE_SPANS, False)


def cross_kernel(cross_ref, facts_ref, kept_ref, right_ref, diagonal_ref, low_ref, sums):
    y = lax.axis_index("y")
    sums[...] = kept_ref[...]
    accumulate(cross_ref, facts_ref, right_ref, sums, LATE_SPANS, False)
    diagonal_ref[...] = sums[:, :, :WIDTH]
    units = [unit_of(sums, level) for level in range(2)]
    low_ref[y] = jnp.zeros((PROBES, 128), I16)
    for apart, level in ((1, 0), (2, 1), (3, 1)):
        low_ref[jnp.bitwise_xor(y, apart)] = units[level]


def depth_kernel(got_ref, low_ref, out_ref):
    x = lax.axis_index("x")
    zh = lax.axis_index("zh")

    def total(asides, aparts):
        return added([
            decode(got_ref[jnp.bitwise_xor(x, aside) * 8 + jnp.bitwise_xor(zh, apart) * 2 + half])
            for aside in asides for apart in aparts for half in range(2)
        ])

    found = [
        total((0,), (0,)),
        total((0,), (1,)),
        total((0,), (2, 3)),
        total((1,), range(4)),
        total((2, 3), range(4)),
    ]
    packed = encode(jnp.concatenate(found, axis=0))
    for at in range(4):
        for core in range(2):
            out_ref[2 * at + core, 0:PROBES] = low_ref[at]
            out_ref[2 * at + core, PROBES:] = packed


def final_kernel(got_ref, factor_ref, coupling_ref, diagonal_ref, out_ref, sibling):
    y = lax.axis_index("y")
    row = row_index()
    for core in range(2):
        lanes = slice(core * 128, core * 128 + 128)
        sibling[0:PROBES, lanes] = decode(got_ref[jnp.bitwise_xor(y, 1) * 2 + core, 0:PROBES])
        pair = decode(got_ref[jnp.bitwise_xor(y, 2) * 2 + core, 0:PROBES])
        pair = pair + decode(got_ref[jnp.bitwise_xor(y, 3) * 2 + core, 0:PROBES])
        sibling[PROBES : 2 * PROBES, lanes] = pair
        for level in range(2, LEVELS):
            for at in range(4):
                start = level * PROBES + at * QUARTER
                source = PROBES + (level - 2) * QUARTER
                sibling[start : start + QUARTER, lanes] = decode(got_ref[2 * at + core, source : source + QUARTER])
    coupling = coupling_ref[...]
    blank = jnp.zeros((HALF, RANK), F32)

    def spread(core_matrix):
        rows = []
        for core in range(2):
            part = core_matrix[core * HALF : (core + 1) * HALF, :]
            rows.append(jnp.concatenate([part, blank], axis=1))
            rows.append(jnp.concatenate([blank, part], axis=1))
        whole = jnp.concatenate(rows, axis=0)
        return halved(whole)

    values, remainders = halved(sibling[...])
    results = []
    for matrix in (coupling.T, coupling):
        top, rest = spread(matrix)
        results.append(
            jnp.dot(values, top, preferred_element_type=F32)
            + jnp.dot(values, rest, preferred_element_type=F32)
            + jnp.dot(remainders, top, preferred_element_type=F32)
        )
    heads = []
    for level in range(LEVELS):
        rows = slice(level * PROBES, (level + 1) * PROBES)
        left = jnp.bitwise_and(jnp.right_shift(row, level), 1) == 0
        heads.append(jnp.where(left, results[0][rows], results[1][rows]))
    firsts = jnp.concatenate([head[:, :RANK] for head in heads], axis=1)
    seconds = jnp.concatenate([head[:, RANK:] for head in heads], axis=1)
    top, rest = halved(jnp.concatenate([firsts, seconds], axis=0))
    stack = jnp.concatenate([top, rest], axis=0)
    on_kern = jnp.dot(stack, factor_ref[0], preferred_element_type=F32)
    pair = jnp.concatenate([top[:PROBES], rest[:PROBES]], axis=0)
    on_slope = jnp.dot(pair, factor_ref[1], preferred_element_type=F32)
    on_kern = on_kern[: 2 * PROBES] + on_kern[2 * PROBES :]
    on_slope = on_slope[:PROBES] + on_slope[PROBES:]
    out_ref[0] = diagonal_ref[0] + on_kern[:PROBES]
    out_ref[1] = diagonal_ref[1] + (on_kern[PROBES:] + on_slope)


def stay(array):
    return pltpu.with_memory_space_constraint(array, pltpu.HBM)


def swap(value, axis):
    return lax.ppermute(value, axis, [(0, 1), (1, 0)])


def exchange(value, axes):
    return lax.all_to_all(value, axes, 0, 0, tiled=True)


def on_device(coords, probes, lengthscales, amplitude, landmarks, coupling):
    message, marks, facts = pl.pallas_call(
        prepare_kernel,
        out_shape=(
            jax.ShapeDtypeStruct((TRANSFER, WIDTH), BF16),
            jax.ShapeDtypeStruct((LEVELS, 8, RANK), F32),
            jax.ShapeDtypeStruct((16, 128), F32),
        ),
        in_specs=[pl.BlockSpec(memory_space=pltpu.HBM)] * 4 + [SMEM],
        out_specs=(VMEM, VMEM, VMEM),
        scratch_shapes=[
            pltpu.VMEM((8, WIDTH), jnp.int32),
            pltpu.VMEM((PROBES, WIDTH), F32),
            pltpu.SMEM((8,), F32),
            pltpu.SemaphoreType.DMA((3 + LEVELS,)),
        ],
        compiler_params=ROOM,
        cost_estimate=cost(10**5, 2 * 10**5),
        name="prepare",
    )(*[stay(array) for array in (coords, probes, landmarks, lengthscales)], amplitude)
    far = swap(message, "h")
    other = swap(message, "c")
    held, right = pl.pallas_call(
        own_kernel,
        out_shape=(
            jax.ShapeDtypeStruct((2, PROBES, LANES), F32),
            jax.ShapeDtypeStruct((SPAN, LANES), BF16),
        ),
        in_specs=[VMEM] * 3,
        out_specs=(VMEM, VMEM),
        compiler_params=ROOM,
        cost_estimate=cost(10**9, 2 * 10**6),
        name="own",
    )(message, facts, marks)
    kept, line = pl.pallas_call(
        near_kernel,
        out_shape=(
            jax.ShapeDtypeStruct((2, PROBES, KEPT), F32),
            jax.ShapeDtypeStruct((8, 5 * QUARTER, 128), I16),
        ),
        in_specs=[VMEM] * 4,
        out_specs=(VMEM, VMEM),
        scratch_shapes=[pltpu.VMEM((2, PROBES, LANES), F32)],
        compiler_params=ROOM,
        cost_estimate=cost(10**9, 2 * 10**6),
        name="near",
    )(other, facts, held, right)
    line = exchange(line, ("zl", "y"))
    deep = pl.pallas_call(
        line_kernel,
        out_shape=jax.ShapeDtypeStruct((32, QUARTER, 128), I16),
        in_specs=[VMEM],
        out_specs=VMEM,
        compiler_params=ROOM,
        cost_estimate=cost(10**5, 3 * 10**5),
        name="line",
    )(line)
    deep = exchange(deep, ("x", "zh", "h"))
    cross = swap(far, "c")
    kept = pl.pallas_call(
        far_kernel,
        out_shape=jax.ShapeDtypeStruct((2, PROBES, KEPT), F32),
        in_specs=[VMEM] * 4,
        out_specs=VMEM,
        compiler_params=ROOM,
        cost_estimate=cost(10**9, 2 * 10**6),
        name="far",
    )(far, facts, kept, right)
    diagonal, low = pl.pallas_call(
        cross_kernel,
        out_shape=(
            jax.ShapeDtypeStruct((2, PROBES, WIDTH), F32),
            jax.ShapeDtypeStruct((4, PROBES, 128), I16),
        ),
        in_specs=[VMEM] * 4,
        out_specs=(VMEM, VMEM),
        scratch_shapes=[pltpu.VMEM((2, PROBES, KEPT), F32)],
        compiler_params=ROOM,
        cost_estimate=cost(10**9, 2 * 10**6),
        name="cross",
    )(cross, facts, kept, right)
    factor = pl.pallas_call(
        factor_kernel,
        out_shape=jax.ShapeDtypeStruct((2, LEVELS * RANK, WIDTH), BF16),
        in_specs=[VMEM] * 3,
        out_specs=VMEM,
        compiler_params=ROOM,
        cost_estimate=cost(10**9, 3 * 10**6),
        name="factor",
    )(facts, marks, right)
    wide = pl.pallas_call(
        depth_kernel,
        out_shape=jax.ShapeDtypeStruct((8, PROBES + 5 * QUARTER, 128), I16),
        in_specs=[VMEM] * 2,
        out_specs=VMEM,
        compiler_params=ROOM,
        cost_estimate=cost(10**5, 5 * 10**5),
        name="depth",
    )(deep, low)
    wide = exchange(wide, ("y", "c"))
    return pl.pallas_call(
        final_kernel,
        out_shape=jax.ShapeDtypeStruct((2, PROBES, WIDTH), F32),
        in_specs=[VMEM] * 4,
        out_specs=VMEM,
        scratch_shapes=[pltpu.VMEM((LEVELS * PROBES, 2 * RANK), F32)],
        compiler_params=ROOM,
        cost_estimate=cost(10**9, 3 * 10**6),
        name="final",
    )(wide, factor, coupling, diagonal)


def solution(mesh):
    fine = Mesh(mesh.devices.reshape(4, 4, 2, 4, 2, 2), ("x", "zh", "zl", "y", "h", "c"))
    every = ("x", "zh", "zl", "y", "h", "c")
    in_specs = (P(None, every), P(None, every), P(), P(), P(), P())
    return jax.shard_map(
        on_device, mesh=fine, in_specs=in_specs, out_specs=P(None, None, every), check_vma=False
    )
```

```python
import math

import jax
import jax.numpy as jnp
from jax import lax
from jax.experimental import pallas as pl
from jax.experimental.pallas import tpu as pltpu
from jax.sharding import Mesh, PartitionSpec as P


LEVELS = 7
PROBES = 64
RANK = 128
HALF = RANK // 2
QUARTER = PROBES // 4
SPAN = 128
WIDTH = 512
TRANSFER = 80
LANES = 1024
BLOCK = 256
PASSED = TRANSFER + 32
ALL_SPANS = ((0, 256), (256, 512), (512, 768), (768, 1024))
LATE_SPANS = ((0, 256), (256, 512))
ROOT = math.sqrt(math.log2(math.e))
TWO_LN2 = 2.0 * math.log(2.0)
F32 = jnp.float32
BF16 = jnp.bfloat16
I16 = jnp.int16
FINE = 2.0**26
OCTAVES = 44.0
VMEM = pl.BlockSpec(memory_space=pltpu.VMEM)
ROOM = pltpu.CompilerParams(vmem_limit_bytes=16 * 2**20)
SMEM = pl.BlockSpec(memory_space=pltpu.SMEM)


def cost(flops, moved):
    return pl.CostEstimate(flops=flops, bytes_accessed=moved, transcendentals=0)


def row_index():
    z = lax.axis_index("zh") * 2 + lax.axis_index("zl")
    return lax.axis_index("x") * 32 + z * 4 + lax.axis_index("y")


def split3(value):
    first = value.astype(BF16).astype(F32)
    rest = value - first
    second = rest.astype(BF16).astype(F32)
    third = (rest - second).astype(BF16).astype(F32)
    return first, second, third


def norms(value):
    return -0.5 * jnp.sum(value * value, axis=0, keepdims=True)


def stacked(parts, rows):
    width = parts[0].shape[1]
    index = lax.broadcasted_iota(jnp.int32, (8, width), 0)
    held = jnp.zeros((8, width), F32)
    for k, row in enumerate(rows):
        held = jnp.where(index == k, row, held)
    zeros = jnp.zeros((SPAN - 56, width), F32)
    return jnp.concatenate(list(parts) + [held, zeros], axis=0)


def left_form(value, extra):
    one, two, three = split3(value)
    n1, n2, n3 = split3(norms(value) + extra)
    return stacked((one, one, two, one, three, two), (1.0, 1.0, 1.0, n1, n2, n3))


def right_form(value, extra):
    one, two, three = split3(value)
    n1, n2, n3 = split3(norms(value) + extra)
    return stacked((one, two, one, three, one, two), (n1, n2, n3, 1.0, 1.0, 1.0))


def points_of(message, inverse):
    high = message[PROBES : PROBES + 8, :].astype(F32)
    low = message[PROBES + 8 : PROBES + 16, :].astype(F32)
    return ((high * 64.0 + low) * (1.0 / 4096.0) - 0.5) * inverse


def kernel_pair(exponent, log_strength):
    kern = jnp.exp2(exponent)
    return kern, kern * (TWO_LN2 * log_strength - TWO_LN2 * exponent)


def halved(value):
    top = value.astype(BF16)
    return top, (value - top.astype(F32)).astype(BF16)


def encode(value):
    grade = jnp.log(1.0 + jnp.abs(value) * FINE) * (32767.0 / (OCTAVES * math.log(2.0))) + 0.5
    return jnp.where(value < 0.0, -grade, grade).astype(jnp.int32).astype(jnp.int16)


def decode(code):
    grade = code.astype(jnp.int32).astype(F32)
    size = (jnp.exp2(jnp.abs(grade) * (OCTAVES / 32767.0)) - 1.0) * (1.0 / FINE)
    return jnp.where(grade < 0.0, -size, size)


def prepare_kernel(
    coords_ref, probes_ref, marks_ref, scales_ref, strength_ref,
    out_ref, picked_ref, facts_ref, coords_buf, probes_buf, scales_buf, sem,
):
    row = row_index()
    copies = [
        pltpu.make_async_copy(probes_ref, probes_buf, sem.at[0]),
        pltpu.make_async_copy(coords_ref, coords_buf, sem.at[1]),
        pltpu.make_async_copy(scales_ref, scales_buf, sem.at[2 + LEVELS]),
    ]
    for level in range(LEVELS):
        node = 2 ** (LEVELS - level) - 2 + jnp.right_shift(row, level)
        copies.append(pltpu.make_async_copy(marks_ref.at[node], picked_ref.at[level], sem.at[2 + level]))
    for copy in copies:
        copy.start()
    for copy in copies:
        copy.wait()
    coords = coords_buf[...]
    high = jnp.right_shift(coords, 6)
    low = coords - high * 64
    out_ref[0:PROBES, :] = probes_buf[...].astype(BF16)
    both = jnp.concatenate([high.astype(F32), low.astype(F32)], axis=0)
    out_ref[PROBES:TRANSFER, :] = both.astype(BF16)
    place = lax.broadcasted_iota(jnp.int32, (8, 128), 0)
    held = jnp.full((8, 128), scales_buf[0], F32)
    for k in range(1, 8):
        held = jnp.where(place == k, scales_buf[k], held)
    facts_ref[0:8, :] = ROOT / held
    facts_ref[8:16, :] = jnp.log(jnp.full((8, 128), strength_ref[0], F32)) * math.log2(math.e)


def accumulate(message_ref, facts_ref, right_ref, sums, spans, fresh):
    message = message_ref[...]
    left = left_form(points_of(message, facts_ref[0:8, 0:1]), 0.0).T.astype(BF16)
    for block in range(WIDTH // BLOCK):
        rows = left[block * BLOCK : (block + 1) * BLOCK, :]
        signs = message[0:PROBES, block * BLOCK : (block + 1) * BLOCK]
        for start, stop in spans:
            exponent = jnp.dot(rows, right_ref[:, start:stop], preferred_element_type=F32)
            for which, value in enumerate(kernel_pair(exponent, facts_ref[8:9, 0:1])):
                top, rest = halved(value)
                total = jnp.dot(signs, top, preferred_element_type=F32)
                if start >= WIDTH:
                    total = total + jnp.dot(signs, rest, preferred_element_type=F32)
                if fresh and block == 0:
                    sums[which, :, start:stop] = total
                else:
                    sums[which, :, start:stop] += total


def unit_of(sums, level):
    at = WIDTH + level * HALF
    return encode(jnp.concatenate([sums[0, :, at : at + HALF], sums[1, :, at : at + HALF]], axis=1))


def own_kernel(own_ref, facts_ref, marks_ref, held_ref, right_ref):
    core = lax.axis_index("c")
    inverse = facts_ref[0:8, 0:1]
    own = points_of(own_ref[...], inverse)
    halves = []
    for level in range(LEVELS):
        mark = (marks_ref[level] - 0.5) * inverse
        halves.append(jnp.where(core == 0, mark[:, :HALF], mark[:, HALF:]))
    halves.append(jnp.zeros((8, HALF), F32))
    columns = jnp.concatenate([own] + halves, axis=1)
    right_ref[...] = right_form(columns, facts_ref[8:9, 0:1]).astype(BF16)
    accumulate(own_ref, facts_ref, right_ref, held_ref, ALL_SPANS, True)


def factor_kernel(facts_ref, marks_ref, right_ref, factor_ref):
    inverse = facts_ref[0:8, 0:1]
    right = right_ref[:, :WIDTH]
    for level in range(LEVELS):
        turned = left_form((marks_ref[level] - 0.5) * inverse, 0.0).T.astype(BF16)
        exponent = jnp.dot(turned, right, preferred_element_type=F32)
        for which, value in enumerate(kernel_pair(exponent, facts_ref[8:9, 0:1])):
            factor_ref[which, level * RANK : (level + 1) * RANK, :] = value.astype(BF16)


def near_kernel(other_ref, facts_ref, held_ref, right_ref, kept_ref, line_ref, sums):
    y = lax.axis_index("y")
    zl = lax.axis_index("zl")
    sums[...] = held_ref[...]
    accumulate(other_ref, facts_ref, right_ref, sums, ALL_SPANS, False)
    kept_ref[...] = sums[:, :, :WIDTH]
    units = [unit_of(sums, level) for level in range(LEVELS)]
    blank = jnp.zeros((QUARTER, 128), I16)
    whole = jnp.zeros((PROBES, 128), I16)
    for at in range(4):
        part = slice(at * QUARTER, (at + 1) * QUARTER)
        higher = [unit[part] for unit in units[3:]]
        line_ref[zl * 4 + at, 0 : 5 * QUARTER] = jnp.concatenate([blank] + higher, axis=0)
        line_ref[(1 - zl) * 4 + at, 0 : 5 * QUARTER] = jnp.concatenate([units[2][part]] + higher, axis=0)
        line_ref[(1 - zl) * 4 + at, 5 * QUARTER :] = whole
    for apart, unit in ((0, whole), (1, units[0]), (2, units[1]), (3, units[1])):
        line_ref[zl * 4 + jnp.bitwise_xor(y, apart), 5 * QUARTER :] = unit


def added(parts):
    while len(parts) > 1:
        parts = [a + b for a, b in zip(parts[::2], parts[1::2])]
    return parts[0]


def line_kernel(got_ref, message_ref, out_ref, passed_ref):
    x = lax.axis_index("x")
    y = lax.axis_index("y")
    zh = lax.axis_index("zh")
    zl = lax.axis_index("zl")
    two = encode(added([decode(got_ref[(1 - zl) * 4 + at, 0:QUARTER]) for at in range(4)]))
    packed = encode(added([decode(got_ref[at, QUARTER : 5 * QUARTER]) for at in range(8)]))
    parts = [packed[at * QUARTER : (at + 1) * QUARTER] for at in range(4)]
    for aside in range(4):
        for apart in range(4):
            place = jnp.bitwise_xor(x, aside) * 8 + jnp.bitwise_xor(zh, apart) * 2
            if aside > 0:
                piece = parts[1 + aside.bit_length()]
            elif apart > 0:
                piece = parts[apart.bit_length() - 1]
            else:
                piece = two
            for half in range(2):
                out_ref[place + half] = piece
    passed_ref[0:TRANSFER, :] = message_ref[...]
    first, second, third = [
        decode(got_ref[zl * 4 + jnp.bitwise_xor(y, apart), 5 * QUARTER :]) for apart in (1, 2, 3)
    ]
    low = jnp.concatenate([first, second + third], axis=0).astype(BF16)
    for at in range(4):
        passed_ref[TRANSFER:, at * 128 : (at + 1) * 128] = low[at * 32 : (at + 1) * 32]


def relay_kernel(far_ref, own_ref, out_ref):
    out_ref[0:TRANSFER, :] = far_ref[0:TRANSFER, :]
    total = far_ref[TRANSFER:, :].astype(F32) + own_ref[TRANSFER:, :].astype(F32)
    out_ref[TRANSFER:, :] = total.astype(BF16)


def late_kernel(far_ref, facts_ref, kept_ref, right_ref, out_ref):
    out_ref[...] = kept_ref[...]
    accumulate(far_ref, facts_ref, right_ref, out_ref, LATE_SPANS, False)


def depth_kernel(got_ref, out_ref):
    x = lax.axis_index("x")
    zh = lax.axis_index("zh")

    def total(asides, aparts):
        return added([
            decode(got_ref[jnp.bitwise_xor(x, aside) * 8 + jnp.bitwise_xor(zh, apart) * 2 + half])
            for aside in asides for apart in aparts for half in range(2)
        ])

    found = [
        total((0,), (0,)),
        total((0,), (1,)),
        total((0,), (2, 3)),
        total((1,), range(4)),
        total((2, 3), range(4)),
    ]
    packed = encode(jnp.concatenate(found, axis=0))
    for place in range(8):
        out_ref[place] = packed


def final_kernel(got_ref, factor_ref, coupling_ref, diagonal_ref, relay_ref, cross_ref, out_ref, sibling):
    row = row_index()
    mine = lax.axis_index("c")
    for core in range(2):
        lanes = slice(core * 128, core * 128 + 128)
        for at in range(4):
            parts = [ref[TRANSFER:, at * 128 : (at + 1) * 128].astype(F32) for ref in (relay_ref, cross_ref)]
            sibling[at * 32 : (at + 1) * 32, lanes] = jnp.where(mine == core, parts[0], parts[1])
        for level in range(2, LEVELS):
            for at in range(4):
                start = level * PROBES + at * QUARTER
                source = (level - 2) * QUARTER
                sibling[start : start + QUARTER, lanes] = decode(got_ref[2 * at + core, source : source + QUARTER])
    coupling = coupling_ref[...]
    blank = jnp.zeros((HALF, RANK), F32)

    def spread(core_matrix):
        rows = []
        for core in range(2):
            part = core_matrix[core * HALF : (core + 1) * HALF, :]
            rows.append(jnp.concatenate([part, blank], axis=1))
            rows.append(jnp.concatenate([blank, part], axis=1))
        whole = jnp.concatenate(rows, axis=0)
        return halved(whole)

    values, remainders = halved(sibling[...])
    results = []
    for matrix in (coupling.T, coupling):
        top, rest = spread(matrix)
        results.append(
            jnp.dot(values, top, preferred_element_type=F32)
            + jnp.dot(values, rest, preferred_element_type=F32)
            + jnp.dot(remainders, top, preferred_element_type=F32)
        )
    heads = []
    for level in range(LEVELS):
        rows = slice(level * PROBES, (level + 1) * PROBES)
        left = jnp.bitwise_and(jnp.right_shift(row, level), 1) == 0
        heads.append(jnp.where(left, results[0][rows], results[1][rows]))
    firsts = jnp.concatenate([head[:, :RANK] for head in heads], axis=1)
    seconds = jnp.concatenate([head[:, RANK:] for head in heads], axis=1)
    top, rest = halved(jnp.concatenate([firsts, seconds], axis=0))
    stack = jnp.concatenate([top, rest], axis=0)
    on_kern = jnp.dot(stack, factor_ref[0], preferred_element_type=F32)
    pair = jnp.concatenate([top[:PROBES], rest[:PROBES]], axis=0)
    on_slope = jnp.dot(pair, factor_ref[1], preferred_element_type=F32)
    on_kern = on_kern[: 2 * PROBES] + on_kern[2 * PROBES :]
    on_slope = on_slope[:PROBES] + on_slope[PROBES:]
    out_ref[0] = diagonal_ref[0] + on_kern[:PROBES]
    out_ref[1] = diagonal_ref[1] + (on_kern[PROBES:] + on_slope)


def stay(array):
    return pltpu.with_memory_space_constraint(array, pltpu.HBM)


def swap(value, axis):
    return lax.ppermute(value, axis, [(0, 1), (1, 0)])


def exchange(value, axes):
    return lax.all_to_all(value, axes, 0, 0, tiled=True)


def on_device(coords, probes, lengthscales, amplitude, landmarks, coupling):
    message, marks, facts = pl.pallas_call(
        prepare_kernel,
        out_shape=(
            jax.ShapeDtypeStruct((TRANSFER, WIDTH), BF16),
            jax.ShapeDtypeStruct((LEVELS, 8, RANK), F32),
            jax.ShapeDtypeStruct((16, 128), F32),
        ),
        in_specs=[pl.BlockSpec(memory_space=pltpu.HBM)] * 4 + [SMEM],
        out_specs=(VMEM, VMEM, VMEM),
        scratch_shapes=[
            pltpu.VMEM((8, WIDTH), jnp.int32),
            pltpu.VMEM((PROBES, WIDTH), F32),
            pltpu.SMEM((8,), F32),
            pltpu.SemaphoreType.DMA((3 + LEVELS,)),
        ],
        compiler_params=ROOM,
        cost_estimate=cost(10**5, 2 * 10**5),
        name="prepare",
    )(*[stay(array) for array in (coords, probes, landmarks, lengthscales)], amplitude)
    far = swap(message, "h")
    other = swap(message, "c")
    held, right = pl.pallas_call(
        own_kernel,
        out_shape=(
            jax.ShapeDtypeStruct((2, PROBES, LANES), F32),
            jax.ShapeDtypeStruct((SPAN, LANES), BF16),
        ),
        in_specs=[VMEM] * 3,
        out_specs=(VMEM, VMEM),
        compiler_params=ROOM,
        cost_estimate=cost(10**9, 2 * 10**6),
        name="own",
    )(message, facts, marks)
    kept, line = pl.pallas_call(
        near_kernel,
        out_shape=(
            jax.ShapeDtypeStruct((2, PROBES, WIDTH), F32),
            jax.ShapeDtypeStruct((8, 5 * QUARTER + PROBES, 128), I16),
        ),
        in_specs=[VMEM] * 4,
        out_specs=(VMEM, VMEM),
        scratch_shapes=[pltpu.VMEM((2, PROBES, LANES), F32)],
        compiler_params=ROOM,
        cost_estimate=cost(10**9, 2 * 10**6),
        name="near",
    )(other, facts, held, right)
    line = exchange(line, ("zl", "y"))
    deep, passed = pl.pallas_call(
        line_kernel,
        out_shape=(
            jax.ShapeDtypeStruct((32, QUARTER, 128), I16),
            jax.ShapeDtypeStruct((PASSED, WIDTH), BF16),
        ),
        in_specs=[VMEM] * 2,
        out_specs=(VMEM, VMEM),
        compiler_params=ROOM,
        cost_estimate=cost(10**5, 3 * 10**5),
        name="line",
    )(line, message)
    deep = exchange(deep, ("x", "zh", "h"))
    far = swap(passed, "h")
    factor = pl.pallas_call(
        factor_kernel,
        out_shape=jax.ShapeDtypeStruct((2, LEVELS * RANK, WIDTH), BF16),
        in_specs=[VMEM] * 3,
        out_specs=VMEM,
        compiler_params=ROOM,
        cost_estimate=cost(10**9, 3 * 10**6),
        name="factor",
    )(facts, marks, right)
    wide = pl.pallas_call(
        depth_kernel,
        out_shape=jax.ShapeDtypeStruct((8, 5 * QUARTER, 128), I16),
        in_specs=[VMEM],
        out_specs=VMEM,
        compiler_params=ROOM,
        cost_estimate=cost(10**5, 5 * 10**5),
        name="depth",
    )(deep)
    wide = exchange(wide, ("y", "c"))
    relay = pl.pallas_call(
        relay_kernel,
        out_shape=jax.ShapeDtypeStruct((PASSED, WIDTH), BF16),
        in_specs=[VMEM] * 2,
        out_specs=VMEM,
        compiler_params=ROOM,
        cost_estimate=cost(10**5, 5 * 10**5),
        name="relay",
    )(far, passed)
    cross = swap(relay, "c")

    def late(points, sums):
        return pl.pallas_call(
            late_kernel,
            out_shape=jax.ShapeDtypeStruct((2, PROBES, WIDTH), F32),
            in_specs=[VMEM] * 4,
            out_specs=VMEM,
            compiler_params=ROOM,
            cost_estimate=cost(10**9, 2 * 10**6),
        )(points, facts, sums, right)

    kept = late(relay, kept)
    diagonal = late(cross, kept)
    return pl.pallas_call(
        final_kernel,
        out_shape=jax.ShapeDtypeStruct((2, PROBES, WIDTH), F32),
        in_specs=[VMEM] * 6,
        out_specs=VMEM,
        scratch_shapes=[pltpu.VMEM((LEVELS * PROBES, 2 * RANK), F32)],
        compiler_params=ROOM,
        cost_estimate=cost(10**9, 3 * 10**6),
        name="final",
    )(wide, factor, coupling, diagonal, relay, cross)


def solution(mesh):
    fine = Mesh(mesh.devices.reshape(4, 4, 2, 4, 2, 2), ("x", "zh", "zl", "y", "h", "c"))
    every = ("x", "zh", "zl", "y", "h", "c")
    in_specs = (P(None, every), P(None, every), P(), P(), P(), P())
    return jax.shard_map(
        on_device, mesh=fine, in_specs=in_specs, out_specs=P(None, None, every), check_vma=False
    )
```

```python
import math

import jax
import jax.numpy as jnp
from jax import lax
from jax.experimental import pallas as pl
from jax.experimental.pallas import tpu as pltpu
from jax.sharding import Mesh, PartitionSpec as P


LEVELS = 7
PROBES = 64
RANK = 128
HALF = RANK // 2
QUARTER = PROBES // 4
SPAN = 128
WIDTH = 512
TRANSFER = 80
LANES = 1024
BLOCK = 256
KEPT = WIDTH + RANK
NEAR_SPANS = ((512, 768), (768, 1024))
SELF_SPANS = ((0, 256), (256, 512))
LATE_SPANS = ((0, 256), (256, 512), (512, 640))
ROOT = math.sqrt(math.log2(math.e))
TWO_LN2 = 2.0 * math.log(2.0)
F32 = jnp.float32
BF16 = jnp.bfloat16
I16 = jnp.int16
FINE = 2.0**26
OCTAVES = 44.0
VMEM = pl.BlockSpec(memory_space=pltpu.VMEM)
ROOM = pltpu.CompilerParams(vmem_limit_bytes=16 * 2**20)
SMEM = pl.BlockSpec(memory_space=pltpu.SMEM)


def cost(flops, moved):
    return pl.CostEstimate(flops=flops, bytes_accessed=moved, transcendentals=0)


def row_index():
    z = lax.axis_index("zh") * 2 + lax.axis_index("zl")
    return lax.axis_index("x") * 32 + z * 4 + lax.axis_index("y")


def split3(value):
    first = value.astype(BF16).astype(F32)
    rest = value - first
    second = rest.astype(BF16).astype(F32)
    third = (rest - second).astype(BF16).astype(F32)
    return first, second, third


def norms(value):
    return -0.5 * jnp.sum(value * value, axis=0, keepdims=True)


def stacked(parts, rows):
    width = parts[0].shape[1]
    index = lax.broadcasted_iota(jnp.int32, (8, width), 0)
    held = jnp.zeros((8, width), F32)
    for k, row in enumerate(rows):
        held = jnp.where(index == k, row, held)
    zeros = jnp.zeros((SPAN - 56, width), F32)
    return jnp.concatenate(list(parts) + [held, zeros], axis=0)


def left_form(value, extra):
    one, two, three = split3(value)
    n1, n2, n3 = split3(norms(value) + extra)
    return stacked((one, one, two, one, three, two), (1.0, 1.0, 1.0, n1, n2, n3))


def right_form(value, extra):
    one, two, three = split3(value)
    n1, n2, n3 = split3(norms(value) + extra)
    return stacked((one, two, one, three, one, two), (n1, n2, n3, 1.0, 1.0, 1.0))


def points_of(message, inverse):
    high = message[PROBES : PROBES + 8, :].astype(F32)
    low = message[PROBES + 8 : PROBES + 16, :].astype(F32)
    return ((high * 64.0 + low) * (1.0 / 4096.0) - 0.5) * inverse


def kernel_pair(exponent, log_strength):
    kern = jnp.exp2(exponent)
    return kern, kern * (TWO_LN2 * log_strength - TWO_LN2 * exponent)


def halved(value):
    top = value.astype(BF16)
    return top, (value - top.astype(F32)).astype(BF16)


def encode(value):
    grade = jnp.log(1.0 + jnp.abs(value) * FINE) * (32767.0 / (OCTAVES * math.log(2.0))) + 0.5
    return jnp.where(value < 0.0, -grade, grade).astype(jnp.int32).astype(jnp.int16)


def decode(code):
    grade = code.astype(jnp.int32).astype(F32)
    size = (jnp.exp2(jnp.abs(grade) * (OCTAVES / 32767.0)) - 1.0) * (1.0 / FINE)
    return jnp.where(grade < 0.0, -size, size)


def prepare_kernel(
    coords_ref, probes_ref, marks_ref, scales_ref, strength_ref,
    out_ref, picked_ref, facts_ref, coords_buf, probes_buf, scales_buf, sem,
):
    row = row_index()
    copies = [
        pltpu.make_async_copy(probes_ref, probes_buf, sem.at[0]),
        pltpu.make_async_copy(coords_ref, coords_buf, sem.at[1]),
        pltpu.make_async_copy(scales_ref, scales_buf, sem.at[2 + LEVELS]),
    ]
    for level in range(LEVELS):
        node = 2 ** (LEVELS - level) - 2 + jnp.right_shift(row, level)
        copies.append(pltpu.make_async_copy(marks_ref.at[node], picked_ref.at[level], sem.at[2 + level]))
    for copy in copies:
        copy.start()
    for copy in copies:
        copy.wait()
    coords = coords_buf[...]
    high = jnp.right_shift(coords, 6)
    low = coords - high * 64
    out_ref[0:PROBES, :] = probes_buf[...].astype(BF16)
    both = jnp.concatenate([high.astype(F32), low.astype(F32)], axis=0)
    out_ref[PROBES:TRANSFER, :] = both.astype(BF16)
    place = lax.broadcasted_iota(jnp.int32, (8, 128), 0)
    held = jnp.full((8, 128), scales_buf[0], F32)
    for k in range(1, 8):
        held = jnp.where(place == k, scales_buf[k], held)
    facts_ref[0:8, :] = ROOT / held
    facts_ref[8:16, :] = jnp.log(jnp.full((8, 128), strength_ref[0], F32)) * math.log2(math.e)


def accumulate(message_ref, facts_ref, right_ref, sums, spans, fresh):
    message = message_ref[...]
    left = left_form(points_of(message, facts_ref[0:8, 0:1]), 0.0).T.astype(BF16)
    for block in range(WIDTH // BLOCK):
        rows = left[block * BLOCK : (block + 1) * BLOCK, :]
        signs = message[0:PROBES, block * BLOCK : (block + 1) * BLOCK]
        for start, stop in spans:
            exponent = jnp.dot(rows, right_ref[:, start:stop], preferred_element_type=F32)
            for which, value in enumerate(kernel_pair(exponent, facts_ref[8:9, 0:1])):
                top, rest = halved(value)
                total = jnp.dot(signs, top, preferred_element_type=F32)
                if start >= WIDTH:
                    total = total + jnp.dot(signs, rest, preferred_element_type=F32)
                if fresh and block == 0:
                    sums[which, :, start:stop] = total
                else:
                    sums[which, :, start:stop] += total


def unit_of(sums, level):
    at = WIDTH + level * HALF
    return encode(jnp.concatenate([sums[0, :, at : at + HALF], sums[1, :, at : at + HALF]], axis=1))


def own_kernel(own_ref, facts_ref, marks_ref, held_ref, right_ref):
    core = lax.axis_index("c")
    inverse = facts_ref[0:8, 0:1]
    own = points_of(own_ref[...], inverse)
    halves = []
    for level in range(LEVELS):
        mark = (marks_ref[level] - 0.5) * inverse
        halves.append(jnp.where(core == 0, mark[:, :HALF], mark[:, HALF:]))
    halves.append(jnp.zeros((8, HALF), F32))
    columns = jnp.concatenate([own] + halves, axis=1)
    right_ref[...] = right_form(columns, facts_ref[8:9, 0:1]).astype(BF16)
    accumulate(own_ref, facts_ref, right_ref, held_ref, NEAR_SPANS, True)


def factor_kernel(facts_ref, marks_ref, right_ref, factor_ref):
    inverse = facts_ref[0:8, 0:1]
    right = right_ref[:, :WIDTH]
    for level in range(LEVELS):
        turned = left_form((marks_ref[level] - 0.5) * inverse, 0.0).T.astype(BF16)
        exponent = jnp.dot(turned, right, preferred_element_type=F32)
        for which, value in enumerate(kernel_pair(exponent, facts_ref[8:9, 0:1])):
            factor_ref[which, level * RANK : (level + 1) * RANK, :] = value.astype(BF16)


def near_kernel(other_ref, facts_ref, held_ref, right_ref, kept_ref, line_ref, sums):
    zl = lax.axis_index("zl")
    sums[:, :, WIDTH:] = held_ref[:, :, WIDTH:]
    accumulate(other_ref, facts_ref, right_ref, sums, NEAR_SPANS, False)
    kept_ref[...] = sums[:, :, WIDTH:KEPT]
    units = [unit_of(sums, level) for level in range(2, LEVELS)]
    blank = jnp.zeros((QUARTER, 128), I16)
    for at in range(4):
        part = slice(at * QUARTER, (at + 1) * QUARTER)
        higher = [unit[part] for unit in units[1:]]
        line_ref[zl * 4 + at] = jnp.concatenate([blank] + higher, axis=0)
        line_ref[(1 - zl) * 4 + at] = jnp.concatenate([units[0][part]] + higher, axis=0)


def added(parts):
    while len(parts) > 1:
        parts = [a + b for a, b in zip(parts[::2], parts[1::2])]
    return parts[0]


def line_kernel(got_ref, out_ref):
    x = lax.axis_index("x")
    zh = lax.axis_index("zh")
    zl = lax.axis_index("zl")
    two = encode(added([decode(got_ref[(1 - zl) * 4 + at, 0:QUARTER]) for at in range(4)]))
    packed = encode(added([decode(got_ref[at, QUARTER:]) for at in range(8)]))
    parts = [packed[at * QUARTER : (at + 1) * QUARTER] for at in range(4)]
    for aside in range(4):
        for apart in range(4):
            place = jnp.bitwise_xor(x, aside) * 8 + jnp.bitwise_xor(zh, apart) * 2
            if aside > 0:
                piece = parts[1 + aside.bit_length()]
            elif apart > 0:
                piece = parts[apart.bit_length() - 1]
            else:
                piece = two
            for half in range(2):
                out_ref[place + half] = piece


def far_kernel(far_ref, own_ref, other_ref, facts_ref, kept_ref, right_ref, out_ref):
    out_ref[:, :, WIDTH:] = kept_ref[...]
    accumulate(own_ref, facts_ref, right_ref, out_ref, SELF_SPANS, True)
    accumulate(other_ref, facts_ref, right_ref, out_ref, SELF_SPANS, False)
    accumulate(far_ref, facts_ref, right_ref, out_ref, LATE_SPANS, False)


def cross_kernel(cross_ref, facts_ref, kept_ref, right_ref, diagonal_ref, low_ref, sums):
    y = lax.axis_index("y")
    sums[...] = kept_ref[...]
    accumulate(cross_ref, facts_ref, right_ref, sums, LATE_SPANS, False)
    diagonal_ref[...] = sums[:, :, :WIDTH]
    units = [unit_of(sums, level) for level in range(2)]
    low_ref[y] = jnp.zeros((PROBES, 128), I16)
    for apart, level in ((1, 0), (2, 1), (3, 1)):
        low_ref[jnp.bitwise_xor(y, apart)] = units[level]


def depth_kernel(got_ref, low_ref, out_ref):
    x = lax.axis_index("x")
    zh = lax.axis_index("zh")

    def total(asides, aparts):
        return added([
            decode(got_ref[jnp.bitwise_xor(x, aside) * 8 + jnp.bitwise_xor(zh, apart) * 2 + half])
            for aside in asides for apart in aparts for half in range(2)
        ])

    found = [
        total((0,), (0,)),
        total((0,), (1,)),
        total((0,), (2, 3)),
        total((1,), range(4)),
        total((2, 3), range(4)),
    ]
    packed = encode(jnp.concatenate(found, axis=0))
    for at in range(4):
        for core in range(2):
            out_ref[2 * at + core, 0:PROBES] = low_ref[at]
            out_ref[2 * at + core, PROBES:] = packed


def final_kernel(got_ref, factor_ref, coupling_ref, diagonal_ref, out_ref, sibling):
    y = lax.axis_index("y")
    row = row_index()
    for core in range(2):
        lanes = slice(core * 128, core * 128 + 128)
        sibling[0:PROBES, lanes] = decode(got_ref[jnp.bitwise_xor(y, 1) * 2 + core, 0:PROBES])
        pair = decode(got_ref[jnp.bitwise_xor(y, 2) * 2 + core, 0:PROBES])
        pair = pair + decode(got_ref[jnp.bitwise_xor(y, 3) * 2 + core, 0:PROBES])
        sibling[PROBES : 2 * PROBES, lanes] = pair
        for level in range(2, LEVELS):
            for at in range(4):
                start = level * PROBES + at * QUARTER
                source = PROBES + (level - 2) * QUARTER
                sibling[start : start + QUARTER, lanes] = decode(got_ref[2 * at + core, source : source + QUARTER])
    coupling = coupling_ref[...]
    blank = jnp.zeros((HALF, RANK), F32)

    def spread(core_matrix):
        rows = []
        for core in range(2):
            part = core_matrix[core * HALF : (core + 1) * HALF, :]
            rows.append(jnp.concatenate([part, blank], axis=1))
            rows.append(jnp.concatenate([blank, part], axis=1))
        whole = jnp.concatenate(rows, axis=0)
        return halved(whole)

    values, remainders = halved(sibling[...])
    results = []
    for matrix in (coupling.T, coupling):
        top, rest = spread(matrix)
        results.append(
            jnp.dot(values, top, preferred_element_type=F32)
            + jnp.dot(values, rest, preferred_element_type=F32)
            + jnp.dot(remainders, top, preferred_element_type=F32)
        )
    heads = []
    for level in range(LEVELS):
        rows = slice(level * PROBES, (level + 1) * PROBES)
        left = jnp.bitwise_and(jnp.right_shift(row, level), 1) == 0
        heads.append(jnp.where(left, results[0][rows], results[1][rows]))
    firsts = jnp.concatenate([head[:, :RANK] for head in heads], axis=1)
    seconds = jnp.concatenate([head[:, RANK:] for head in heads], axis=1)
    top, rest = halved(jnp.concatenate([firsts, seconds], axis=0))
    stack = jnp.concatenate([top, rest], axis=0)
    on_kern = jnp.dot(stack, factor_ref[0], preferred_element_type=F32)
    pair = jnp.concatenate([top[:PROBES], rest[:PROBES]], axis=0)
    on_slope = jnp.dot(pair, factor_ref[1], preferred_element_type=F32)
    on_kern = on_kern[: 2 * PROBES] + on_kern[2 * PROBES :]
    on_slope = on_slope[:PROBES] + on_slope[PROBES:]
    out_ref[0] = diagonal_ref[0] + on_kern[:PROBES]
    out_ref[1] = diagonal_ref[1] + (on_kern[PROBES:] + on_slope)


def stay(array):
    return pltpu.with_memory_space_constraint(array, pltpu.HBM)


def swap(value, axis):
    return lax.ppermute(value, axis, [(0, 1), (1, 0)])


def exchange(value, axes):
    return lax.all_to_all(value, axes, 0, 0, tiled=True)


def on_device(coords, probes, lengthscales, amplitude, landmarks, coupling):
    message, marks, facts = pl.pallas_call(
        prepare_kernel,
        out_shape=(
            jax.ShapeDtypeStruct((TRANSFER, WIDTH), BF16),
            jax.ShapeDtypeStruct((LEVELS, 8, RANK), F32),
            jax.ShapeDtypeStruct((16, 128), F32),
        ),
        in_specs=[pl.BlockSpec(memory_space=pltpu.HBM)] * 4 + [SMEM],
        out_specs=(VMEM, VMEM, VMEM),
        scratch_shapes=[
            pltpu.VMEM((8, WIDTH), jnp.int32),
            pltpu.VMEM((PROBES, WIDTH), F32),
            pltpu.SMEM((8,), F32),
            pltpu.SemaphoreType.DMA((3 + LEVELS,)),
        ],
        compiler_params=ROOM,
        cost_estimate=cost(10**5, 2 * 10**5),
        name="prepare",
    )(*[stay(array) for array in (coords, probes, landmarks, lengthscales)], amplitude)
    far = swap(message, "h")
    other = swap(message, "c")
    held, right = pl.pallas_call(
        own_kernel,
        out_shape=(
            jax.ShapeDtypeStruct((2, PROBES, LANES), F32),
            jax.ShapeDtypeStruct((SPAN, LANES), BF16),
        ),
        in_specs=[VMEM] * 3,
        out_specs=(VMEM, VMEM),
        compiler_params=ROOM,
        cost_estimate=cost(10**9, 2 * 10**6),
        name="own",
    )(message, facts, marks)
    kept, line = pl.pallas_call(
        near_kernel,
        out_shape=(
            jax.ShapeDtypeStruct((2, PROBES, RANK), F32),
            jax.ShapeDtypeStruct((8, 5 * QUARTER, 128), I16),
        ),
        in_specs=[VMEM] * 4,
        out_specs=(VMEM, VMEM),
        scratch_shapes=[pltpu.VMEM((2, PROBES, LANES), F32)],
        compiler_params=ROOM,
        cost_estimate=cost(10**9, 2 * 10**6),
        name="near",
    )(other, facts, held, right)
    line = exchange(line, ("zl", "y"))
    deep = pl.pallas_call(
        line_kernel,
        out_shape=jax.ShapeDtypeStruct((32, QUARTER, 128), I16),
        in_specs=[VMEM],
        out_specs=VMEM,
        compiler_params=ROOM,
        cost_estimate=cost(10**5, 3 * 10**5),
        name="line",
    )(line)
    deep = exchange(deep, ("x", "zh", "h"))
    cross = swap(far, "c")
    kept = pl.pallas_call(
        far_kernel,
        out_shape=jax.ShapeDtypeStruct((2, PROBES, KEPT), F32),
        in_specs=[VMEM] * 6,
        out_specs=VMEM,
        compiler_params=ROOM,
        cost_estimate=cost(10**9, 2 * 10**6),
        name="far",
    )(far, message, other, facts, kept, right)
    diagonal, low = pl.pallas_call(
        cross_kernel,
        out_shape=(
            jax.ShapeDtypeStruct((2, PROBES, WIDTH), F32),
            jax.ShapeDtypeStruct((4, PROBES, 128), I16),
        ),
        in_specs=[VMEM] * 4,
        out_specs=(VMEM, VMEM),
        scratch_shapes=[pltpu.VMEM((2, PROBES, KEPT), F32)],
        compiler_params=ROOM,
        cost_estimate=cost(10**9, 2 * 10**6),
        name="cross",
    )(cross, facts, kept, right)
    factor = pl.pallas_call(
        factor_kernel,
        out_shape=jax.ShapeDtypeStruct((2, LEVELS * RANK, WIDTH), BF16),
        in_specs=[VMEM] * 3,
        out_specs=VMEM,
        compiler_params=ROOM,
        cost_estimate=cost(10**9, 3 * 10**6),
        name="factor",
    )(facts, marks, right)
    wide = pl.pallas_call(
        depth_kernel,
        out_shape=jax.ShapeDtypeStruct((8, PROBES + 5 * QUARTER, 128), I16),
        in_specs=[VMEM] * 2,
        out_specs=VMEM,
        compiler_params=ROOM,
        cost_estimate=cost(10**5, 5 * 10**5),
        name="depth",
    )(deep, low)
    wide = exchange(wide, ("y", "c"))
    return pl.pallas_call(
        final_kernel,
        out_shape=jax.ShapeDtypeStruct((2, PROBES, WIDTH), F32),
        in_specs=[VMEM] * 4,
        out_specs=VMEM,
        scratch_shapes=[pltpu.VMEM((LEVELS * PROBES, 2 * RANK), F32)],
        compiler_params=ROOM,
        cost_estimate=cost(10**9, 3 * 10**6),
        name="final",
    )(wide, factor, coupling, diagonal)


def solution(mesh):
    fine = Mesh(mesh.devices.reshape(4, 4, 2, 4, 2, 2), ("x", "zh", "zl", "y", "h", "c"))
    every = ("x", "zh", "zl", "y", "h", "c")
    in_specs = (P(None, every), P(None, every), P(), P(), P(), P())
    return jax.shard_map(
        on_device, mesh=fine, in_specs=in_specs, out_specs=P(None, None, every), check_vma=False
    )
```

```python
import math

import jax
import jax.numpy as jnp
from jax import lax
from jax.experimental import pallas as pl
from jax.experimental.pallas import tpu as pltpu
from jax.sharding import Mesh, PartitionSpec as P


LEVELS = 7
PROBES = 64
RANK = 128
HALF = RANK // 2
QUARTER = PROBES // 4
SPAN = 128
WIDTH = 512
TRANSFER = 80
LANES = 1024
BLOCK = 256
KEPT = WIDTH + RANK
NEAR_SPANS = ((512, 768), (768, 1024))
SELF_SPANS = ((0, 256), (256, 512))
LATE_SPANS = ((0, 256), (256, 512), (512, 640))
ROOT = math.sqrt(math.log2(math.e))
TWO_LN2 = 2.0 * math.log(2.0)
F32 = jnp.float32
BF16 = jnp.bfloat16
I16 = jnp.int16
FINE = 2.0**26
OCTAVES = 44.0
VMEM = pl.BlockSpec(memory_space=pltpu.VMEM)
ROOM = pltpu.CompilerParams(vmem_limit_bytes=16 * 2**20)
SMEM = pl.BlockSpec(memory_space=pltpu.SMEM)


def cost(flops, moved):
    return pl.CostEstimate(flops=flops, bytes_accessed=moved, transcendentals=0)


def row_index():
    z = lax.axis_index("zh") * 2 + lax.axis_index("zl")
    return lax.axis_index("x") * 32 + z * 4 + lax.axis_index("y")


def split3(value):
    first = value.astype(BF16).astype(F32)
    rest = value - first
    second = rest.astype(BF16).astype(F32)
    third = (rest - second).astype(BF16).astype(F32)
    return first, second, third


def norms(value):
    return -0.5 * jnp.sum(value * value, axis=0, keepdims=True)


def stacked(parts, rows):
    width = parts[0].shape[1]
    index = lax.broadcasted_iota(jnp.int32, (8, width), 0)
    held = jnp.zeros((8, width), F32)
    for k, row in enumerate(rows):
        held = jnp.where(index == k, row, held)
    zeros = jnp.zeros((SPAN - 56, width), F32)
    return jnp.concatenate(list(parts) + [held, zeros], axis=0)


def left_form(value, extra):
    one, two, three = split3(value)
    n1, n2, n3 = split3(norms(value) + extra)
    return stacked((one, one, two, one, three, two), (1.0, 1.0, 1.0, n1, n2, n3))


def right_form(value, extra):
    one, two, three = split3(value)
    n1, n2, n3 = split3(norms(value) + extra)
    return stacked((one, two, one, three, one, two), (n1, n2, n3, 1.0, 1.0, 1.0))


def points_of(message, inverse):
    high = message[PROBES : PROBES + 8, :].astype(F32)
    low = message[PROBES + 8 : PROBES + 16, :].astype(F32)
    return ((high * 64.0 + low) * (1.0 / 4096.0) - 0.5) * inverse


def kernel_pair(exponent, log_strength):
    kern = jnp.exp2(exponent)
    return kern, kern * (TWO_LN2 * log_strength - TWO_LN2 * exponent)


def halved(value):
    top = value.astype(BF16)
    return top, (value - top.astype(F32)).astype(BF16)


def encode(value):
    grade = jnp.log(1.0 + jnp.abs(value) * FINE) * (32767.0 / (OCTAVES * math.log(2.0))) + 0.5
    return jnp.where(value < 0.0, -grade, grade).astype(jnp.int32).astype(jnp.int16)


def decode(code):
    grade = code.astype(jnp.int32).astype(F32)
    size = (jnp.exp2(jnp.abs(grade) * (OCTAVES / 32767.0)) - 1.0) * (1.0 / FINE)
    return jnp.where(grade < 0.0, -size, size)


def prepare_kernel(
    coords_ref, probes_ref, marks_ref, scales_ref, strength_ref,
    out_ref, picked_ref, facts_ref, coords_buf, probes_buf, scales_buf, sem,
):
    row = row_index()
    copies = [
        pltpu.make_async_copy(probes_ref, probes_buf, sem.at[0]),
        pltpu.make_async_copy(coords_ref, coords_buf, sem.at[1]),
        pltpu.make_async_copy(scales_ref, scales_buf, sem.at[2 + LEVELS]),
    ]
    for level in range(LEVELS):
        node = 2 ** (LEVELS - level) - 2 + jnp.right_shift(row, level)
        copies.append(pltpu.make_async_copy(marks_ref.at[node], picked_ref.at[level], sem.at[2 + level]))
    for copy in copies:
        copy.start()
    for copy in copies:
        copy.wait()
    coords = coords_buf[...]
    high = jnp.right_shift(coords, 6)
    low = coords - high * 64
    out_ref[0:PROBES, :] = probes_buf[...].astype(BF16)
    both = jnp.concatenate([high.astype(F32), low.astype(F32)], axis=0)
    out_ref[PROBES:TRANSFER, :] = both.astype(BF16)
    place = lax.broadcasted_iota(jnp.int32, (8, 128), 0)
    held = jnp.full((8, 128), scales_buf[0], F32)
    for k in range(1, 8):
        held = jnp.where(place == k, scales_buf[k], held)
    facts_ref[0:8, :] = ROOT / held
    facts_ref[8:16, :] = jnp.log(jnp.full((8, 128), strength_ref[0], F32)) * math.log2(math.e)


def accumulate(message_ref, facts_ref, right_ref, sums, spans, fresh):
    message = message_ref[...]
    left = left_form(points_of(message, facts_ref[0:8, 0:1]), 0.0).T.astype(BF16)
    for block in range(WIDTH // BLOCK):
        rows = left[block * BLOCK : (block + 1) * BLOCK, :]
        signs = message[0:PROBES, block * BLOCK : (block + 1) * BLOCK]
        for start, stop in spans:
            exponent = jnp.dot(rows, right_ref[:, start:stop], preferred_element_type=F32)
            for which, value in enumerate(kernel_pair(exponent, facts_ref[8:9, 0:1])):
                top, rest = halved(value)
                total = jnp.dot(signs, top, preferred_element_type=F32)
                if start >= WIDTH:
                    total = total + jnp.dot(signs, rest, preferred_element_type=F32)
                if fresh and block == 0:
                    sums[which, :, start:stop] = total
                else:
                    sums[which, :, start:stop] += total


def unit_of(sums, level):
    at = WIDTH + level * HALF
    return encode(jnp.concatenate([sums[0, :, at : at + HALF], sums[1, :, at : at + HALF]], axis=1))


def own_kernel(own_ref, facts_ref, marks_ref, held_ref, right_ref):
    core = lax.axis_index("c")
    inverse = facts_ref[0:8, 0:1]
    own = points_of(own_ref[...], inverse)
    halves = []
    for level in range(LEVELS):
        mark = (marks_ref[level] - 0.5) * inverse
        halves.append(jnp.where(core == 0, mark[:, :HALF], mark[:, HALF:]))
    halves.append(jnp.zeros((8, HALF), F32))
    columns = jnp.concatenate([own] + halves, axis=1)
    right_ref[...] = right_form(columns, facts_ref[8:9, 0:1]).astype(BF16)
    accumulate(own_ref, facts_ref, right_ref, held_ref, NEAR_SPANS, True)


def scale_kernel(facts_ref, marks_ref, out_ref):
    for level in range(LEVELS):
        out_ref[level] = (marks_ref[level] - 0.5) * facts_ref[0:8, 0:1]


def factor_kernel(facts_ref, marks_ref, right_ref, factor_ref):
    right = right_ref[:, :WIDTH]
    for level in range(LEVELS):
        turned = left_form(marks_ref[level], 0.0).T.astype(BF16)
        exponent = jnp.dot(turned, right, preferred_element_type=F32)
        for which, value in enumerate(kernel_pair(exponent, facts_ref[8:9, 0:1])):
            factor_ref[which, level * RANK : (level + 1) * RANK, :] = value.astype(BF16)


def near_kernel(other_ref, facts_ref, held_ref, right_ref, kept_ref, line_ref, sums):
    zl = lax.axis_index("zl")
    sums[:, :, WIDTH:] = held_ref[:, :, WIDTH:]
    accumulate(other_ref, facts_ref, right_ref, sums, NEAR_SPANS, False)
    kept_ref[...] = sums[:, :, WIDTH:KEPT]
    units = [unit_of(sums, level) for level in range(2, LEVELS)]
    blank = jnp.zeros((QUARTER, 128), I16)
    for at in range(4):
        part = slice(at * QUARTER, (at + 1) * QUARTER)
        higher = [unit[part] for unit in units[1:]]
        line_ref[zl * 4 + at] = jnp.concatenate([blank] + higher, axis=0)
        line_ref[(1 - zl) * 4 + at] = jnp.concatenate([units[0][part]] + higher, axis=0)


def added(parts):
    while len(parts) > 1:
        parts = [a + b for a, b in zip(parts[::2], parts[1::2])]
    return parts[0]


def line_kernel(got_ref, out_ref):
    x = lax.axis_index("x")
    zh = lax.axis_index("zh")
    zl = lax.axis_index("zl")
    two = encode(added([decode(got_ref[(1 - zl) * 4 + at, 0:QUARTER]) for at in range(4)]))
    packed = encode(added([decode(got_ref[at, QUARTER:]) for at in range(8)]))
    parts = [packed[at * QUARTER : (at + 1) * QUARTER] for at in range(4)]
    for aside in range(4):
        for apart in range(4):
            place = jnp.bitwise_xor(x, aside) * 8 + jnp.bitwise_xor(zh, apart) * 2
            if aside > 0:
                piece = parts[1 + aside.bit_length()]
            elif apart > 0:
                piece = parts[apart.bit_length() - 1]
            else:
                piece = two
            for half in range(2):
                out_ref[place + half] = piece


def far_kernel(far_ref, own_ref, other_ref, facts_ref, kept_ref, right_ref, out_ref):
    out_ref[:, :, WIDTH:] = kept_ref[...]
    accumulate(own_ref, facts_ref, right_ref, out_ref, SELF_SPANS, True)
    accumulate(other_ref, facts_ref, right_ref, out_ref, SELF_SPANS, False)
    accumulate(far_ref, facts_ref, right_ref, out_ref, LATE_SPANS, False)


def cross_kernel(cross_ref, facts_ref, kept_ref, right_ref, diagonal_ref, low_ref, sums):
    y = lax.axis_index("y")
    sums[...] = kept_ref[...]
    accumulate(cross_ref, facts_ref, right_ref, sums, LATE_SPANS, False)
    diagonal_ref[...] = sums[:, :, :WIDTH]
    units = [unit_of(sums, level) for level in range(2)]
    low_ref[y] = jnp.zeros((PROBES, 128), I16)
    for apart, level in ((1, 0), (2, 1), (3, 1)):
        low_ref[jnp.bitwise_xor(y, apart)] = units[level]


def depth_kernel(got_ref, low_ref, out_ref):
    x = lax.axis_index("x")
    zh = lax.axis_index("zh")

    def total(asides, aparts):
        return added([
            decode(got_ref[jnp.bitwise_xor(x, aside) * 8 + jnp.bitwise_xor(zh, apart) * 2 + half])
            for aside in asides for apart in aparts for half in range(2)
        ])

    found = [
        total((0,), (0,)),
        total((0,), (1,)),
        total((0,), (2, 3)),
        total((1,), range(4)),
        total((2, 3), range(4)),
    ]
    packed = encode(jnp.concatenate(found, axis=0))
    for at in range(4):
        for core in range(2):
            out_ref[2 * at + core, 0:PROBES] = low_ref[at]
            out_ref[2 * at + core, PROBES:] = packed


def final_kernel(got_ref, factor_ref, coupling_ref, diagonal_ref, out_ref, sibling):
    y = lax.axis_index("y")
    row = row_index()
    for core in range(2):
        lanes = slice(core * 128, core * 128 + 128)
        sibling[0:PROBES, lanes] = decode(got_ref[jnp.bitwise_xor(y, 1) * 2 + core, 0:PROBES])
        pair = decode(got_ref[jnp.bitwise_xor(y, 2) * 2 + core, 0:PROBES])
        pair = pair + decode(got_ref[jnp.bitwise_xor(y, 3) * 2 + core, 0:PROBES])
        sibling[PROBES : 2 * PROBES, lanes] = pair
        for level in range(2, LEVELS):
            for at in range(4):
                start = level * PROBES + at * QUARTER
                source = PROBES + (level - 2) * QUARTER
                sibling[start : start + QUARTER, lanes] = decode(got_ref[2 * at + core, source : source + QUARTER])
    coupling = coupling_ref[...]
    blank = jnp.zeros((HALF, RANK), F32)

    def spread(core_matrix):
        rows = []
        for core in range(2):
            part = core_matrix[core * HALF : (core + 1) * HALF, :]
            rows.append(jnp.concatenate([part, blank], axis=1))
            rows.append(jnp.concatenate([blank, part], axis=1))
        whole = jnp.concatenate(rows, axis=0)
        return halved(whole)

    values, remainders = halved(sibling[...])
    results = []
    for matrix in (coupling.T, coupling):
        top, rest = spread(matrix)
        results.append(
            jnp.dot(values, top, preferred_element_type=F32)
            + jnp.dot(values, rest, preferred_element_type=F32)
            + jnp.dot(remainders, top, preferred_element_type=F32)
        )
    heads = []
    for level in range(LEVELS):
        rows = slice(level * PROBES, (level + 1) * PROBES)
        left = jnp.bitwise_and(jnp.right_shift(row, level), 1) == 0
        heads.append(jnp.where(left, results[0][rows], results[1][rows]))
    firsts = jnp.concatenate([head[:, :RANK] for head in heads], axis=1)
    seconds = jnp.concatenate([head[:, RANK:] for head in heads], axis=1)
    top, rest = halved(jnp.concatenate([firsts, seconds], axis=0))
    stack = jnp.concatenate([top, rest], axis=0)
    on_kern = jnp.dot(stack, factor_ref[0], preferred_element_type=F32)
    pair = jnp.concatenate([top[:PROBES], rest[:PROBES]], axis=0)
    on_slope = jnp.dot(pair, factor_ref[1], preferred_element_type=F32)
    on_kern = on_kern[: 2 * PROBES] + on_kern[2 * PROBES :]
    on_slope = on_slope[:PROBES] + on_slope[PROBES:]
    out_ref[0] = diagonal_ref[0] + on_kern[:PROBES]
    out_ref[1] = diagonal_ref[1] + (on_kern[PROBES:] + on_slope)


def stay(array):
    return pltpu.with_memory_space_constraint(array, pltpu.HBM)


def swap(value, axis):
    return lax.ppermute(value, axis, [(0, 1), (1, 0)])


def exchange(value, axes):
    return lax.all_to_all(value, axes, 0, 0, tiled=True)


def on_device(coords, probes, lengthscales, amplitude, landmarks, coupling):
    message, marks, facts = pl.pallas_call(
        prepare_kernel,
        out_shape=(
            jax.ShapeDtypeStruct((TRANSFER, WIDTH), BF16),
            jax.ShapeDtypeStruct((LEVELS, 8, RANK), F32),
            jax.ShapeDtypeStruct((16, 128), F32),
        ),
        in_specs=[pl.BlockSpec(memory_space=pltpu.HBM)] * 4 + [SMEM],
        out_specs=(VMEM, VMEM, VMEM),
        scratch_shapes=[
            pltpu.VMEM((8, WIDTH), jnp.int32),
            pltpu.VMEM((PROBES, WIDTH), F32),
            pltpu.SMEM((8,), F32),
            pltpu.SemaphoreType.DMA((3 + LEVELS,)),
        ],
        compiler_params=ROOM,
        cost_estimate=cost(10**5, 2 * 10**5),
        name="prepare",
    )(*[stay(array) for array in (coords, probes, landmarks, lengthscales)], amplitude)
    far = swap(message, "h")
    other = swap(message, "c")
    held, right = pl.pallas_call(
        own_kernel,
        out_shape=(
            jax.ShapeDtypeStruct((2, PROBES, LANES), F32),
            jax.ShapeDtypeStruct((SPAN, LANES), BF16),
        ),
        in_specs=[VMEM] * 3,
        out_specs=(VMEM, VMEM),
        compiler_params=ROOM,
        cost_estimate=cost(10**9, 2 * 10**6),
        name="own",
    )(message, facts, marks)
    kept, line = pl.pallas_call(
        near_kernel,
        out_shape=(
            jax.ShapeDtypeStruct((2, PROBES, RANK), F32),
            jax.ShapeDtypeStruct((8, 5 * QUARTER, 128), I16),
        ),
        in_specs=[VMEM] * 4,
        out_specs=(VMEM, VMEM),
        scratch_shapes=[pltpu.VMEM((2, PROBES, LANES), F32)],
        compiler_params=ROOM,
        cost_estimate=cost(10**9, 2 * 10**6),
        name="near",
    )(other, facts, held, right)
    line = exchange(line, ("zl", "y"))
    deep = pl.pallas_call(
        line_kernel,
        out_shape=jax.ShapeDtypeStruct((32, QUARTER, 128), I16),
        in_specs=[VMEM],
        out_specs=VMEM,
        compiler_params=ROOM,
        cost_estimate=cost(10**5, 3 * 10**5),
        name="line",
    )(line)
    deep = exchange(deep, ("x", "zh", "h"))
    cross = swap(far, "c")
    kept = pl.pallas_call(
        far_kernel,
        out_shape=jax.ShapeDtypeStruct((2, PROBES, KEPT), F32),
        in_specs=[VMEM] * 6,
        out_specs=VMEM,
        compiler_params=ROOM,
        cost_estimate=cost(10**9, 2 * 10**6),
        name="far",
    )(far, message, other, facts, kept, right)
    diagonal, low = pl.pallas_call(
        cross_kernel,
        out_shape=(
            jax.ShapeDtypeStruct((2, PROBES, WIDTH), F32),
            jax.ShapeDtypeStruct((4, PROBES, 128), I16),
        ),
        in_specs=[VMEM] * 4,
        out_specs=(VMEM, VMEM),
        scratch_shapes=[pltpu.VMEM((2, PROBES, KEPT), F32)],
        compiler_params=ROOM,
        cost_estimate=cost(10**9, 2 * 10**6),
        name="cross",
    )(cross, facts, kept, right)
    anchors = pl.pallas_call(
        scale_kernel,
        out_shape=jax.ShapeDtypeStruct((LEVELS, 8, RANK), F32),
        in_specs=[VMEM] * 2,
        out_specs=VMEM,
        compiler_params=ROOM,
        cost_estimate=cost(10**5, 10**5),
        name="scale",
    )(facts, marks)
    factor = pl.pallas_call(
        factor_kernel,
        out_shape=jax.ShapeDtypeStruct((2, LEVELS * RANK, WIDTH), BF16),
        in_specs=[VMEM] * 3,
        out_specs=VMEM,
        compiler_params=ROOM,
        cost_estimate=cost(10**9, 3 * 10**6),
        name="factor",
    )(facts, anchors, right)
    wide = pl.pallas_call(
        depth_kernel,
        out_shape=jax.ShapeDtypeStruct((8, PROBES + 5 * QUARTER, 128), I16),
        in_specs=[VMEM] * 2,
        out_specs=VMEM,
        compiler_params=ROOM,
        cost_estimate=cost(10**5, 5 * 10**5),
        name="depth",
    )(deep, low)
    wide = exchange(wide, ("y", "c"))
    return pl.pallas_call(
        final_kernel,
        out_shape=jax.ShapeDtypeStruct((2, PROBES, WIDTH), F32),
        in_specs=[VMEM] * 4,
        out_specs=VMEM,
        scratch_shapes=[pltpu.VMEM((LEVELS * PROBES, 2 * RANK), F32)],
        compiler_params=ROOM,
        cost_estimate=cost(10**9, 3 * 10**6),
        name="final",
    )(wide, factor, coupling, diagonal)


def solution(mesh):
    fine = Mesh(mesh.devices.reshape(4, 4, 2, 4, 2, 2), ("x", "zh", "zl", "y", "h", "c"))
    every = ("x", "zh", "zl", "y", "h", "c")
    in_specs = (P(None, every), P(None, every), P(), P(), P(), P())
    return jax.shard_map(
        on_device, mesh=fine, in_specs=in_specs, out_specs=P(None, None, every), check_vma=False
    )
```

```python
import math

import jax
import jax.numpy as jnp
from jax import lax
from jax.experimental import pallas as pl
from jax.experimental.pallas import tpu as pltpu
from jax.sharding import Mesh, PartitionSpec as P


LEVELS = 7
PROBES = 64
RANK = 128
HALF = RANK // 2
QUARTER = PROBES // 4
SPAN = 128
WIDTH = 512
TRANSFER = 80
LANES = 1024
BLOCK = 256
KEPT = WIDTH + RANK
USED = WIDTH + LEVELS * HALF
NEAR_SPANS = ((512, 768), (768, USED))
SELF_SPANS = ((0, 256), (256, 512))
LATE_SPANS = ((0, 256), (256, 512), (512, 640))
ROOT = math.sqrt(math.log2(math.e))
TWO_LN2 = 2.0 * math.log(2.0)
F32 = jnp.float32
BF16 = jnp.bfloat16
I16 = jnp.int16
FINE = 2.0**26
OCTAVES = 44.0
VMEM = pl.BlockSpec(memory_space=pltpu.VMEM)
ROOM = pltpu.CompilerParams(vmem_limit_bytes=16 * 2**20)
SMEM = pl.BlockSpec(memory_space=pltpu.SMEM)


def cost(flops, moved):
    return pl.CostEstimate(flops=flops, bytes_accessed=moved, transcendentals=0)


def row_index():
    z = lax.axis_index("zh") * 2 + lax.axis_index("zl")
    return lax.axis_index("x") * 32 + z * 4 + lax.axis_index("y")


def split3(value):
    first = value.astype(BF16).astype(F32)
    rest = value - first
    second = rest.astype(BF16).astype(F32)
    third = (rest - second).astype(BF16).astype(F32)
    return first, second, third


def norms(value):
    return -0.5 * jnp.sum(value * value, axis=0, keepdims=True)


def stacked(parts, rows):
    width = parts[0].shape[1]
    index = lax.broadcasted_iota(jnp.int32, (8, width), 0)
    held = jnp.zeros((8, width), F32)
    for k, row in enumerate(rows):
        held = jnp.where(index == k, row, held)
    zeros = jnp.zeros((SPAN - 56, width), F32)
    return jnp.concatenate(list(parts) + [held, zeros], axis=0)


def left_form(value, extra):
    one, two, three = split3(value)
    n1, n2, n3 = split3(norms(value) + extra)
    return stacked((one, one, two, one, three, two), (1.0, 1.0, 1.0, n1, n2, n3))


def right_form(value, extra):
    one, two, three = split3(value)
    n1, n2, n3 = split3(norms(value) + extra)
    return stacked((one, two, one, three, one, two), (n1, n2, n3, 1.0, 1.0, 1.0))


def points_of(message, inverse):
    high = message[PROBES : PROBES + 8, :].astype(F32)
    low = message[PROBES + 8 : PROBES + 16, :].astype(F32)
    return ((high * 64.0 + low) * (1.0 / 4096.0) - 0.5) * inverse


def kernel_pair(exponent, log_strength):
    kern = jnp.exp2(exponent)
    return kern, kern * (TWO_LN2 * log_strength - TWO_LN2 * exponent)


def halved(value):
    top = value.astype(BF16)
    return top, (value - top.astype(F32)).astype(BF16)


def encode(value):
    grade = jnp.log(1.0 + jnp.abs(value) * FINE) * (32767.0 / (OCTAVES * math.log(2.0))) + 0.5
    return jnp.where(value < 0.0, -grade, grade).astype(jnp.int32).astype(jnp.int16)


def decode(code):
    grade = code.astype(jnp.int32).astype(F32)
    size = (jnp.exp2(jnp.abs(grade) * (OCTAVES / 32767.0)) - 1.0) * (1.0 / FINE)
    return jnp.where(grade < 0.0, -size, size)


def prepare_kernel(
    coords_ref, probes_ref, marks_ref, scales_ref, strength_ref,
    out_ref, picked_ref, facts_ref, coords_buf, probes_buf, scales_buf, sem,
):
    row = row_index()
    copies = [
        pltpu.make_async_copy(probes_ref, probes_buf, sem.at[0]),
        pltpu.make_async_copy(coords_ref, coords_buf, sem.at[1]),
        pltpu.make_async_copy(scales_ref, scales_buf, sem.at[2 + LEVELS]),
    ]
    for level in range(LEVELS):
        node = 2 ** (LEVELS - level) - 2 + jnp.right_shift(row, level)
        copies.append(pltpu.make_async_copy(marks_ref.at[node], picked_ref.at[level], sem.at[2 + level]))
    for copy in copies:
        copy.start()
    for copy in copies:
        copy.wait()
    coords = coords_buf[...]
    high = jnp.right_shift(coords, 6)
    low = coords - high * 64
    out_ref[0:PROBES, :] = probes_buf[...].astype(BF16)
    both = jnp.concatenate([high.astype(F32), low.astype(F32)], axis=0)
    out_ref[PROBES:TRANSFER, :] = both.astype(BF16)
    place = lax.broadcasted_iota(jnp.int32, (8, 128), 0)
    held = jnp.full((8, 128), scales_buf[0], F32)
    for k in range(1, 8):
        held = jnp.where(place == k, scales_buf[k], held)
    facts_ref[0:8, :] = ROOT / held
    facts_ref[8:16, :] = jnp.log(jnp.full((8, 128), strength_ref[0], F32)) * math.log2(math.e)


def accumulate(message_ref, facts_ref, right_ref, sums, spans, fresh):
    message = message_ref[...]
    left = left_form(points_of(message, facts_ref[0:8, 0:1]), 0.0).T.astype(BF16)
    for block in range(WIDTH // BLOCK):
        rows = left[block * BLOCK : (block + 1) * BLOCK, :]
        signs = message[0:PROBES, block * BLOCK : (block + 1) * BLOCK]
        for start, stop in spans:
            exponent = jnp.dot(rows, right_ref[:, start:stop], preferred_element_type=F32)
            for which, value in enumerate(kernel_pair(exponent, facts_ref[8:9, 0:1])):
                top, rest = halved(value)
                total = jnp.dot(signs, top, preferred_element_type=F32)
                if start >= WIDTH:
                    total = total + jnp.dot(signs, rest, preferred_element_type=F32)
                if fresh and block == 0:
                    sums[which, :, start:stop] = total
                else:
                    sums[which, :, start:stop] += total


def unit_of(sums, level):
    at = WIDTH + level * HALF
    return encode(jnp.concatenate([sums[0, :, at : at + HALF], sums[1, :, at : at + HALF]], axis=1))


def own_kernel(own_ref, facts_ref, marks_ref, held_ref, right_ref):
    core = lax.axis_index("c")
    inverse = facts_ref[0:8, 0:1]
    own = points_of(own_ref[...], inverse)
    halves = []
    for level in range(LEVELS):
        mark = (marks_ref[level] - 0.5) * inverse
        halves.append(jnp.where(core == 0, mark[:, :HALF], mark[:, HALF:]))
    halves.append(jnp.zeros((8, HALF), F32))
    columns = jnp.concatenate([own] + halves, axis=1)
    right_ref[...] = right_form(columns, facts_ref[8:9, 0:1]).astype(BF16)
    accumulate(own_ref, facts_ref, right_ref, held_ref, NEAR_SPANS, True)


def scale_kernel(facts_ref, marks_ref, out_ref):
    for level in range(LEVELS):
        out_ref[level] = (marks_ref[level] - 0.5) * facts_ref[0:8, 0:1]


def factor_kernel(facts_ref, marks_ref, right_ref, factor_ref):
    right = right_ref[:, :WIDTH]
    for level in range(LEVELS):
        turned = left_form(marks_ref[level], 0.0).T.astype(BF16)
        exponent = jnp.dot(turned, right, preferred_element_type=F32)
        for which, value in enumerate(kernel_pair(exponent, facts_ref[8:9, 0:1])):
            factor_ref[which, level * RANK : (level + 1) * RANK, :] = value.astype(BF16)


def near_kernel(other_ref, facts_ref, held_ref, right_ref, kept_ref, line_ref, sums):
    zl = lax.axis_index("zl")
    sums[:, :, WIDTH:USED] = held_ref[:, :, WIDTH:USED]
    accumulate(other_ref, facts_ref, right_ref, sums, NEAR_SPANS, False)
    kept_ref[...] = sums[:, :, WIDTH:KEPT]
    units = [unit_of(sums, level) for level in range(2, LEVELS)]
    blank = jnp.zeros((QUARTER, 128), I16)
    for at in range(4):
        part = slice(at * QUARTER, (at + 1) * QUARTER)
        higher = [unit[part] for unit in units[1:]]
        line_ref[zl * 4 + at] = jnp.concatenate([blank] + higher, axis=0)
        line_ref[(1 - zl) * 4 + at] = jnp.concatenate([units[0][part]] + higher, axis=0)


def added(parts):
    while len(parts) > 1:
        parts = [a + b for a, b in zip(parts[::2], parts[1::2])]
    return parts[0]


def line_kernel(got_ref, out_ref):
    x = lax.axis_index("x")
    zh = lax.axis_index("zh")
    zl = lax.axis_index("zl")
    two = encode(added([decode(got_ref[(1 - zl) * 4 + at, 0:QUARTER]) for at in range(4)]))
    packed = encode(added([decode(got_ref[at, QUARTER:]) for at in range(8)]))
    parts = [packed[at * QUARTER : (at + 1) * QUARTER] for at in range(4)]
    for aside in range(4):
        for apart in range(4):
            place = jnp.bitwise_xor(x, aside) * 8 + jnp.bitwise_xor(zh, apart) * 2
            if aside > 0:
                piece = parts[1 + aside.bit_length()]
            elif apart > 0:
                piece = parts[apart.bit_length() - 1]
            else:
                piece = two
            for half in range(2):
                out_ref[place + half] = piece


def far_kernel(far_ref, own_ref, other_ref, facts_ref, kept_ref, right_ref, out_ref):
    out_ref[:, :, WIDTH:] = kept_ref[...]
    accumulate(own_ref, facts_ref, right_ref, out_ref, SELF_SPANS, True)
    accumulate(other_ref, facts_ref, right_ref, out_ref, SELF_SPANS, False)
    accumulate(far_ref, facts_ref, right_ref, out_ref, LATE_SPANS, False)


def cross_kernel(cross_ref, facts_ref, kept_ref, right_ref, diagonal_ref, low_ref, sums):
    y = lax.axis_index("y")
    sums[...] = kept_ref[...]
    accumulate(cross_ref, facts_ref, right_ref, sums, LATE_SPANS, False)
    diagonal_ref[...] = sums[:, :, :WIDTH]
    units = [unit_of(sums, level) for level in range(2)]
    low_ref[y] = jnp.zeros((PROBES, 128), I16)
    for apart, level in ((1, 0), (2, 1), (3, 1)):
        low_ref[jnp.bitwise_xor(y, apart)] = units[level]


def depth_kernel(got_ref, low_ref, out_ref):
    x = lax.axis_index("x")
    zh = lax.axis_index("zh")

    def total(asides, aparts):
        return added([
            decode(got_ref[jnp.bitwise_xor(x, aside) * 8 + jnp.bitwise_xor(zh, apart) * 2 + half])
            for aside in asides for apart in aparts for half in range(2)
        ])

    found = [
        total((0,), (0,)),
        total((0,), (1,)),
        total((0,), (2, 3)),
        total((1,), range(4)),
        total((2, 3), range(4)),
    ]
    packed = encode(jnp.concatenate(found, axis=0))
    for at in range(4):
        for core in range(2):
            out_ref[2 * at + core, 0:PROBES] = low_ref[at]
            out_ref[2 * at + core, PROBES:] = packed


def final_kernel(got_ref, factor_ref, coupling_ref, diagonal_ref, out_ref, sibling):
    y = lax.axis_index("y")
    row = row_index()
    for core in range(2):
        lanes = slice(core * 128, core * 128 + 128)
        sibling[0:PROBES, lanes] = decode(got_ref[jnp.bitwise_xor(y, 1) * 2 + core, 0:PROBES])
        pair = decode(got_ref[jnp.bitwise_xor(y, 2) * 2 + core, 0:PROBES])
        pair = pair + decode(got_ref[jnp.bitwise_xor(y, 3) * 2 + core, 0:PROBES])
        sibling[PROBES : 2 * PROBES, lanes] = pair
        for level in range(2, LEVELS):
            for at in range(4):
                start = level * PROBES + at * QUARTER
                source = PROBES + (level - 2) * QUARTER
                sibling[start : start + QUARTER, lanes] = decode(got_ref[2 * at + core, source : source + QUARTER])
    coupling = coupling_ref[...]
    blank = jnp.zeros((HALF, RANK), F32)

    def spread(core_matrix):
        rows = []
        for core in range(2):
            part = core_matrix[core * HALF : (core + 1) * HALF, :]
            rows.append(jnp.concatenate([part, blank], axis=1))
            rows.append(jnp.concatenate([blank, part], axis=1))
        whole = jnp.concatenate(rows, axis=0)
        return halved(whole)

    values, remainders = halved(sibling[...])
    results = []
    for matrix in (coupling.T, coupling):
        top, rest = spread(matrix)
        results.append(
            jnp.dot(values, top, preferred_element_type=F32)
            + jnp.dot(values, rest, preferred_element_type=F32)
            + jnp.dot(remainders, top, preferred_element_type=F32)
        )
    heads = []
    for level in range(LEVELS):
        rows = slice(level * PROBES, (level + 1) * PROBES)
        left = jnp.bitwise_and(jnp.right_shift(row, level), 1) == 0
        heads.append(jnp.where(left, results[0][rows], results[1][rows]))
    firsts = jnp.concatenate([head[:, :RANK] for head in heads], axis=1)
    seconds = jnp.concatenate([head[:, RANK:] for head in heads], axis=1)
    top, rest = halved(jnp.concatenate([firsts, seconds], axis=0))
    stack = jnp.concatenate([top, rest], axis=0)
    on_kern = jnp.dot(stack, factor_ref[0], preferred_element_type=F32)
    pair = jnp.concatenate([top[:PROBES], rest[:PROBES]], axis=0)
    on_slope = jnp.dot(pair, factor_ref[1], preferred_element_type=F32)
    on_kern = on_kern[: 2 * PROBES] + on_kern[2 * PROBES :]
    on_slope = on_slope[:PROBES] + on_slope[PROBES:]
    out_ref[0] = diagonal_ref[0] + on_kern[:PROBES]
    out_ref[1] = diagonal_ref[1] + (on_kern[PROBES:] + on_slope)


def stay(array):
    return pltpu.with_memory_space_constraint(array, pltpu.HBM)


def swap(value, axis):
    return lax.ppermute(value, axis, [(0, 1), (1, 0)])


def exchange(value, axes):
    return lax.all_to_all(value, axes, 0, 0, tiled=True)


def on_device(coords, probes, lengthscales, amplitude, landmarks, coupling):
    message, marks, facts = pl.pallas_call(
        prepare_kernel,
        out_shape=(
            jax.ShapeDtypeStruct((TRANSFER, WIDTH), BF16),
            jax.ShapeDtypeStruct((LEVELS, 8, RANK), F32),
            jax.ShapeDtypeStruct((16, 128), F32),
        ),
        in_specs=[pl.BlockSpec(memory_space=pltpu.HBM)] * 4 + [SMEM],
        out_specs=(VMEM, VMEM, VMEM),
        scratch_shapes=[
            pltpu.VMEM((8, WIDTH), jnp.int32),
            pltpu.VMEM((PROBES, WIDTH), F32),
            pltpu.SMEM((8,), F32),
            pltpu.SemaphoreType.DMA((3 + LEVELS,)),
        ],
        compiler_params=ROOM,
        cost_estimate=cost(10**5, 2 * 10**5),
        name="prepare",
    )(*[stay(array) for array in (coords, probes, landmarks, lengthscales)], amplitude)
    far = swap(message, "h")
    other = swap(message, "c")
    held, right = pl.pallas_call(
        own_kernel,
        out_shape=(
            jax.ShapeDtypeStruct((2, PROBES, LANES), F32),
            jax.ShapeDtypeStruct((SPAN, LANES), BF16),
        ),
        in_specs=[VMEM] * 3,
        out_specs=(VMEM, VMEM),
        compiler_params=ROOM,
        cost_estimate=cost(10**9, 2 * 10**6),
        name="own",
    )(message, facts, marks)
    kept, line = pl.pallas_call(
        near_kernel,
        out_shape=(
            jax.ShapeDtypeStruct((2, PROBES, RANK), F32),
            jax.ShapeDtypeStruct((8, 5 * QUARTER, 128), I16),
        ),
        in_specs=[VMEM] * 4,
        out_specs=(VMEM, VMEM),
        scratch_shapes=[pltpu.VMEM((2, PROBES, LANES), F32)],
        compiler_params=ROOM,
        cost_estimate=cost(10**9, 2 * 10**6),
        name="near",
    )(other, facts, held, right)
    line = exchange(line, ("zl", "y"))
    deep = pl.pallas_call(
        line_kernel,
        out_shape=jax.ShapeDtypeStruct((32, QUARTER, 128), I16),
        in_specs=[VMEM],
        out_specs=VMEM,
        compiler_params=ROOM,
        cost_estimate=cost(10**5, 3 * 10**5),
        name="line",
    )(line)
    deep = exchange(deep, ("x", "zh", "h"))
    cross = swap(far, "c")
    kept = pl.pallas_call(
        far_kernel,
        out_shape=jax.ShapeDtypeStruct((2, PROBES, KEPT), F32),
        in_specs=[VMEM] * 6,
        out_specs=VMEM,
        compiler_params=ROOM,
        cost_estimate=cost(10**9, 2 * 10**6),
        name="far",
    )(far, message, other, facts, kept, right)
    diagonal, low = pl.pallas_call(
        cross_kernel,
        out_shape=(
            jax.ShapeDtypeStruct((2, PROBES, WIDTH), F32),
            jax.ShapeDtypeStruct((4, PROBES, 128), I16),
        ),
        in_specs=[VMEM] * 4,
        out_specs=(VMEM, VMEM),
        scratch_shapes=[pltpu.VMEM((2, PROBES, KEPT), F32)],
        compiler_params=ROOM,
        cost_estimate=cost(10**9, 2 * 10**6),
        name="cross",
    )(cross, facts, kept, right)
    anchors = pl.pallas_call(
        scale_kernel,
        out_shape=jax.ShapeDtypeStruct((LEVELS, 8, RANK), F32),
        in_specs=[VMEM] * 2,
        out_specs=VMEM,
        compiler_params=ROOM,
        cost_estimate=cost(10**5, 10**5),
        name="scale",
    )(facts, marks)
    factor = pl.pallas_call(
        factor_kernel,
        out_shape=jax.ShapeDtypeStruct((2, LEVELS * RANK, WIDTH), BF16),
        in_specs=[VMEM] * 3,
        out_specs=VMEM,
        compiler_params=ROOM,
        cost_estimate=cost(10**9, 3 * 10**6),
        name="factor",
    )(facts, anchors, right)
    wide = pl.pallas_call(
        depth_kernel,
        out_shape=jax.ShapeDtypeStruct((8, PROBES + 5 * QUARTER, 128), I16),
        in_specs=[VMEM] * 2,
        out_specs=VMEM,
        compiler_params=ROOM,
        cost_estimate=cost(10**5, 5 * 10**5),
        name="depth",
    )(deep, low)
    wide = exchange(wide, ("y", "c"))
    return pl.pallas_call(
        final_kernel,
        out_shape=jax.ShapeDtypeStruct((2, PROBES, WIDTH), F32),
        in_specs=[VMEM] * 4,
        out_specs=VMEM,
        scratch_shapes=[pltpu.VMEM((LEVELS * PROBES, 2 * RANK), F32)],
        compiler_params=ROOM,
        cost_estimate=cost(10**9, 3 * 10**6),
        name="final",
    )(wide, factor, coupling, diagonal)


def solution(mesh):
    fine = Mesh(mesh.devices.reshape(4, 4, 2, 4, 2, 2), ("x", "zh", "zl", "y", "h", "c"))
    every = ("x", "zh", "zl", "y", "h", "c")
    in_specs = (P(None, every), P(None, every), P(), P(), P(), P())
    return jax.shard_map(
        on_device, mesh=fine, in_specs=in_specs, out_specs=P(None, None, every), check_vma=False
    )
```
